256 devices in a mesh: seq: 16 (over y, z_hi, core), tp: 16 (over x, z_lo).
Axes of the slice: x: 4, y: 4, z: 8 (z_hi: 2, z_lo: 4; z = z_hi * 4 + z_lo), core: 2. Of those that a mesh axis runs over, the one named last changes fastest.
Arguments:
- tokens: bfloat16 [8192, 4608], P(('seq', 'tp')), may hold values from -6 to 6
- norm_gain: float32 [4608], replicated, may hold values from 0.1 to 1.9
- query_weight: bfloat16 [4608, 4096], P(None, 'tp'), may hold values from -6 to 6
- key_matrix: bfloat16 [4608, 2048], P(None, 'tp'), may hold values from -0.09375 to 0.09375
- value_matrix: bfloat16 [4608, 2048], P(None, 'tp'), may hold values from -0.09375 to 0.09375
- output_grad: bfloat16 [8192, 4096], P('seq', 'tp'), may hold values from -3 to 3
Outputs:
- input_gradient: bfloat16 [8192, 4608], P(('seq', 'tp'))
The draws below stay inside these ranges and needn't reach their ends.
All inputs are finite; a program needn't handle non-finite values.
Results may differ from the reference program's by a relative error of at most 0.014.
The reference program's roundings to bfloat16 on the way (of `normed` and `grad_query`) count: a program that leaves them out, or rounds other values in their place, can miss the bound.
Values may be sent and summed in bfloat16 or wider, within the bound.
A program may use at most 64 MiB of HBM per device.

```python
import math
import jax
import jax.numpy as jnp
from jax import lax

MODEL_WIDTH = 4608
HQ = 32
KEY_VALUE_HEADS = 16
HEAD_SIZE = 128
TOK_DEV = 512
WINDOW = 640
TOKENS = 8192


def draw_query_weight(key, part):
    head_scale = jnp.exp(jax.random.uniform(jax.random.fold_in(key, 11), (HQ,), jnp.float32, math.log(3.0), math.log(12.0)))
    column_scale = jnp.repeat(head_scale, HEAD_SIZE)
    entries = jax.random.truncated_normal(jax.random.fold_in(key, 12), -4.0, 4.0, (MODEL_WIDTH, HQ * HEAD_SIZE), jnp.float32)
    return (entries * column_scale[None, :] / math.sqrt(MODEL_WIDTH)).astype(jnp.bfloat16)


def strengthened(values, stream_key, source, target, blocks, factor):
    def block_of(axis_at):
        return (jnp.arange(values.shape[axis_at]) // (values.shape[axis_at] // blocks)).reshape((-1,) + (1,) * (values.ndim - 1 - axis_at))

    near = jax.random.permutation(stream_key, blocks)[block_of(target)]
    far = (block_of(target) + blocks // 2) % blocks
    return jnp.where((block_of(source) == near) | (block_of(source) == far), factor * values, values)


def block_scale(own_key, extent, pieces, smallest, top_value):
    gain = 1.0
    for axis_at, shards_of in pieces:
        steps = jax.random.uniform(jax.random.fold_in(jax.random.fold_in(own_key, 6), axis_at), (shards_of,), jnp.float32, smallest / len(pieces), top_value / len(pieces))
        gain = gain * jnp.repeat(jnp.exp(steps), extent[axis_at] // shards_of).reshape((-1,) + (1,) * (len(extent) - 1 - axis_at))
    return gain


def gaussian(own_key, shape, width, reach, split=(), kind=jnp.bfloat16):
    values = jax.random.normal(own_key, shape, jnp.float32) * width
    if len(split) > 0:
        values = block_scale(own_key, shape, split, -0.22, 0.18) * values
    return jnp.clip(values, min=-reach, max=reach).astype(kind)


def bell_draw_with(own_key, shape, width, bound, shards, heavy, held_as=jnp.bfloat16):
    result = width * jax.random.normal(own_key, shape, jnp.float32)
    if shards:
        result = result * block_scale(own_key, shape, shards, -0.22, 0.18)
    return jnp.clip(strengthened(result, jax.random.fold_in(own_key, 3), *heavy), -bound, bound).astype(held_as)


def setup_inputs(seed: int = 0) -> dict:
    key_of = jax.random.split(jax.random.key(seed), 7)
    tokens = gaussian(key_of[0], (TOKENS, MODEL_WIDTH), 1.0, 6.0, ((0, 256),))
    norm_gain = jnp.clip(1.0 + 0.18 * jax.random.normal(key_of[1], (MODEL_WIDTH,), jnp.float32), 0.1, 1.9)
    query_weight = draw_query_weight(jax.random.fold_in(key_of[6], 71), 0)
    key_matrix = gaussian(key_of[3], (MODEL_WIDTH, KEY_VALUE_HEADS * HEAD_SIZE), MODEL_WIDTH ** -0.5, 0.09375, ((1, 16),))
    value_matrix = gaussian(key_of[4], (MODEL_WIDTH, KEY_VALUE_HEADS * HEAD_SIZE), MODEL_WIDTH ** -0.5, 0.09375, ((1, 16),))
    output_grad = bell_draw_with(key_of[5], (TOKENS, HQ * HEAD_SIZE), 0.5, 3.0, ((0, 16), (1, 16)), (1, 0, 16, 2.0))
    return dict(tokens=tokens, norm_gain=norm_gain, query_weight=query_weight, key_matrix=key_matrix, value_matrix=value_matrix, output_grad=output_grad)


SCALE = 1.0 / 12.0
CAP = 50.0
EPS = 1e-06

def block_grads(query_blk, grad_blk, key_blk, value_blk, query_pos, key_pos):
    row_count = query_blk.shape[0]
    key_span = key_blk.shape[0]
    kv_heads = key_blk.shape[1] // HEAD_SIZE
    groups = query_blk.shape[1] // key_blk.shape[1]
    query_four = query_blk.reshape(row_count, kv_heads, groups, HEAD_SIZE).astype(jnp.float32)
    grad_four = grad_blk.reshape(row_count, kv_heads, groups, HEAD_SIZE).astype(jnp.float32)
    key_three = key_blk.reshape(key_span, kv_heads, HEAD_SIZE).astype(jnp.float32)
    value_three = value_blk.reshape(key_span, kv_heads, HEAD_SIZE).astype(jnp.float32)
    raw = jnp.einsum('qkgd,skd->kgqs', query_four, key_three)
    bent = jnp.tanh(raw * SCALE / CAP)
    capped = CAP * bent
    valid = (key_pos[None, :] <= query_pos[:, None]) & (key_pos[None, :] > query_pos[:, None] - WINDOW) & (key_pos[None, :] >= 0)
    expo = jnp.where(valid, jnp.exp(capped), 0.0)
    probs = expo / lax.optimization_barrier(jnp.sum(expo, axis=-1, keepdims=True))
    d_probs = jnp.einsum('qkgd,skd->kgqs', grad_four, value_three)
    delta = lax.optimization_barrier(jnp.sum(probs * d_probs, axis=-1, keepdims=True))
    d_raw = (probs * (d_probs - delta) * (1.0 - bent * bent) * SCALE).astype(jnp.bfloat16).astype(jnp.float32)
    probs_low = probs.astype(jnp.bfloat16).astype(jnp.float32)
    grad_query = jnp.einsum('kgqs,skd->qkgd', d_raw, key_three).reshape(row_count, kv_heads * groups * HEAD_SIZE)
    grad_key = jnp.einsum('kgqs,qkgd->skd', d_raw, query_four).reshape(key_span, kv_heads * HEAD_SIZE)
    grad_value = jnp.einsum('kgqs,qkgd->skd', probs_low, grad_four).reshape(key_span, kv_heads * HEAD_SIZE)
    return (grad_query, grad_key, grad_value)

def reference(tokens, norm_gain, query_weight, key_matrix, value_matrix, output_grad):
    total_rows = tokens.shape[0]
    key_cols = key_matrix.shape[1]
    block_rows = min(512, TOK_DEV)
    key_span = WINDOW + block_rows
    float_values = tokens.astype(jnp.float32)
    reciprocal_root_mean = lax.rsqrt(lax.optimization_barrier(jnp.mean(float_values * float_values, axis=1, keepdims=True)) + EPS)
    normed = (float_values * reciprocal_root_mean * norm_gain).astype(jnp.bfloat16)
    query_all = jnp.dot(normed, query_weight, preferred_element_type=jnp.float32).astype(jnp.bfloat16)
    key_all = jnp.dot(normed, key_matrix, preferred_element_type=jnp.float32).astype(jnp.bfloat16)
    value_all = jnp.dot(normed, value_matrix, preferred_element_type=jnp.float32).astype(jnp.bfloat16)
    pad_key = jnp.concatenate([jnp.zeros((WINDOW, key_cols), jnp.bfloat16), key_all], axis=0)
    pad_value = jnp.concatenate([jnp.zeros((WINDOW, key_cols), jnp.bfloat16), value_all], axis=0)

    def step_fn(carry, index_block):
        acc_key, acc_value = carry
        first_row = index_block * block_rows
        query_blk = lax.dynamic_slice_in_dim(query_all, first_row, block_rows, 0)
        grad_blk = lax.dynamic_slice_in_dim(output_grad, first_row, block_rows, 0)
        key_blk = lax.dynamic_slice_in_dim(pad_key, first_row, key_span, 0)
        value_blk = lax.dynamic_slice_in_dim(pad_value, first_row, key_span, 0)
        query_pos = first_row + jnp.arange(block_rows, dtype=jnp.int32)
        key_pos = first_row - WINDOW + jnp.arange(key_span, dtype=jnp.int32)
        grad_query, grad_key, grad_value = block_grads(query_blk, grad_blk, key_blk, value_blk, query_pos, key_pos)
        acc_key = lax.dynamic_update_slice_in_dim(acc_key, lax.dynamic_slice_in_dim(acc_key, first_row, key_span, 0) + grad_key, first_row, 0)
        acc_value = lax.dynamic_update_slice_in_dim(acc_value, lax.dynamic_slice_in_dim(acc_value, first_row, key_span, 0) + grad_value, first_row, 0)
        return ((acc_key, acc_value), grad_query.astype(jnp.bfloat16))
    zeros_acc = jnp.zeros((total_rows + WINDOW, key_cols), jnp.float32)
    (acc_key, acc_value), grad_blocks = lax.scan(step_fn, (zeros_acc, zeros_acc), jnp.arange(total_rows // block_rows, dtype=jnp.int32))
    grad_query = grad_blocks.reshape(total_rows, query_weight.shape[1])
    grad_key = acc_key[WINDOW:].astype(jnp.bfloat16)
    grad_value = acc_value[WINDOW:].astype(jnp.bfloat16)
    dims = (((1,), (1,)), ((), ()))
    d_norm = lax.dot_general(grad_query, query_weight, dims, preferred_element_type=jnp.float32)
    d_norm = d_norm + lax.dot_general(grad_key, key_matrix, dims, preferred_element_type=jnp.float32)
    d_norm = d_norm + lax.dot_general(grad_value, value_matrix, dims, preferred_element_type=jnp.float32)
    upper_limit = d_norm * norm_gain
    normalized_input = float_values * reciprocal_root_mean
    input_gradient = reciprocal_root_mean * (upper_limit - normalized_input * lax.optimization_barrier(jnp.mean(upper_limit * normalized_input, axis=1, keepdims=True)))
    return input_gradient.astype(jnp.bfloat16)
```

```python
import functools

import jax
import jax.numpy as jnp
from jax import lax
from jax.experimental import pallas as pl
from jax.experimental.pallas import tpu as pltpu
from jax.sharding import PartitionSpec as P

HEAD_SIZE = 128
WINDOW = 640
SCALE = 1.0 / 12.0
CAP = 50.0
EPS = 1e-06
MESH = pl.DeviceIdType.MESH
NX = 4
NZ = 4
A_TILES = 8


def place():
    t = lax.axis_index("tp")
    return t // NZ, t % NZ


def near_to_far(z):
    def high(q):
        return (q, 5 - q, jnp.int32(1), jnp.int32(0))

    up = high(z)
    low = high(3 - z)
    return [jnp.where(z >= 2, u, 3 - v) for u, v in zip(up, low)]


def send_to(src, dst, send_sem, recv_sem, tp):
    return pltpu.make_async_remote_copy(
        src_ref=src,
        dst_ref=dst,
        send_sem=send_sem,
        recv_sem=recv_sem,
        device_id={"tp": tp},
        device_id_type=MESH,
    )


def tp_of(x, z):
    return x * NZ + z


def greet_plane(x, z):
    barrier = pltpu.get_barrier_semaphore()

    def greet(tp):
        pl.semaphore_signal(barrier, inc=1, device_id={"tp": tp}, device_id_type=MESH)

    greet(tp_of((x + 1) % NX, z))
    greet(tp_of((x + 3) % NX, z))

    @pl.when(z > 0)
    def _():
        greet(tp_of(x, z - 1))

    @pl.when(z < NZ - 1)
    def _():
        greet(tp_of(x, z + 1))

    return barrier


def await_plane(barrier, z):
    edge = (z == 0) | (z == NZ - 1)
    pl.semaphore_wait(barrier, jnp.where(edge, 3, 4))


class Sends:
    def __init__(self):
        self.started = []

    def start(self, copy, when=None):
        self.started.append((copy, when))
        if when is None:
            copy.start()
        else:
            pl.when(when)(lambda: copy.start())

    def finish(self):
        for copy, when in self.started:
            if when is None:
                copy.wait_send()
            else:
                pl.when(when)(lambda copy=copy: copy.wait_send())


def gather_project(
    tokens_ref, gain_ref, wq_ref, wk_ref, wv_ref, out_ref,
    g, w, w_sem, sx, rx, szb, rzb, sza, rza,
):
    x, z = place()
    rows, width = tokens_ref.shape
    half = rows // 2
    a_cols = pl.ds(0, A_TILES * 128)
    b_cols = pl.ds(A_TILES * 128, width - A_TILES * 128)
    xp, xm, xo = (x + 1) % NX, (x + 3) % NX, (x + 2) % NX
    zs = near_to_far(z)
    q_cols, k_cols = wq_ref.shape[1], wk_ref.shape[1]
    barrier = greet_plane(x, z)
    loads = [
        pltpu.make_async_copy(wq_ref, w.at[:, pl.ds(0, q_cols)], w_sem.at[0]),
        pltpu.make_async_copy(wk_ref, w.at[:, pl.ds(q_cols, k_cols)], w_sem.at[1]),
        pltpu.make_async_copy(wv_ref, w.at[:, pl.ds(q_cols + k_cols, k_cols)], w_sem.at[2]),
    ]
    for load in loads:
        load.start()
    values = tokens_ref[...].astype(jnp.float32)
    inv = lax.rsqrt(jnp.mean(values * values, axis=1, keepdims=True) + EPS)
    g[z, pl.ds(x * rows, rows), :] = (values * inv * gain_ref[...]).astype(jnp.bfloat16)
    await_plane(barrier, z)
    sends = Sends()

    def part(zr, xr, h, cols):
        if h is None:
            return g.at[zr, pl.ds(pl.multiple_of(xr * rows, rows), rows), cols]
        return g.at[zr, pl.ds(pl.multiple_of(xr * rows + h * half, half), half), cols]

    def x_send(k, zr, xr, h, cols, to, direction, slot, when=None):
        piece = part(zr, xr, h, cols)
        p = 1 if k == NZ else 0
        sends.start(
            send_to(piece, piece, sx.at[direction, k, slot], rx.at[p, zr, xr, h], tp_of(to, z)), when
        )

    def x_wait(k, zr, xr, h, cols):
        piece = part(zr, xr, h, cols)
        p = 1 if k == NZ else 0
        send_to(piece, piece, sx.at[0, k, 0], rx.at[p, zr, xr, h], tp_of(xp, z)).wait_recv()

    def x_own(k, zr, cols, first):
        h_right, h_left = (0, 1) if first else (1, 0)
        slot = 0 if first else 1
        x_send(k, zr, x, h_right, cols, xp, 0, slot)
        x_send(k, zr, x, h_left, cols, xm, 1, slot)

    def x_forward(k, zr, cols):
        x_wait(k, zr, xm, 0, cols)
        x_send(k, zr, xm, 0, cols, xp, 0, 2)
        x_wait(k, zr, xp, 1, cols)
        x_send(k, zr, xp, 1, cols, xm, 1, 2)

    def x_rest(k, zr, cols):
        x_wait(k, zr, xm, 1, cols)
        x_wait(k, zr, xp, 0, cols)
        x_wait(k, zr, xo, 0, cols)
        x_wait(k, zr, xo, 1, cols)

    def z_piece(zr, is_a):
        return g.at[zr, :, a_cols] if is_a else part(zr, x, None, b_cols)

    def z_send(k, zr, is_a):
        piece = z_piece(zr, is_a)
        ss, rs = (sza, rza) if is_a else (szb, rzb)
        up = send_to(piece, piece, ss.at[0, k], rs.at[zr], tp_of(x, jnp.minimum(z + 1, NZ - 1)))
        down = send_to(piece, piece, ss.at[1, k], rs.at[zr], tp_of(x, jnp.maximum(z - 1, 0)))
        sends.start(up, (zr <= z) & (z < NZ - 1))
        sends.start(down, (zr >= z) & (z > 0))

    def z_wait(zr, is_a):
        piece = z_piece(zr, is_a)
        ss, rs = (sza, rza) if is_a else (szb, rzb)
        send_to(piece, piece, ss.at[0, 0], rs.at[zr], tp_of(xp, z)).wait_recv()

    def project(zr):
        for load in loads if not project.loaded else []:
            load.wait()
        project.loaded = True
        out = jnp.dot(g[zr], w[...], preferred_element_type=jnp.float32).astype(jnp.bfloat16)
        for i in range(NX):
            at = pl.multiple_of(i * NZ * rows + zr * rows, rows)
            out_ref[pl.ds(at, rows), :] = out[i * rows : (i + 1) * rows]

    project.loaded = False

    x_own(NZ, z, a_cols, True)
    x_own(NZ, z, a_cols, False)
    z_send(0, z, False)
    x_own(0, z, b_cols, True)
    x_forward(NZ, z, a_cols)
    x_own(0, z, b_cols, False)
    x_rest(NZ, z, a_cols)
    z_send(0, z, True)
    for k in range(1, NZ):
        zr, before = zs[k], zs[k - 1]
        x_forward(k - 1, before, b_cols)
        z_wait(zr, False)
        z_send(k, zr, False)
        x_own(k, zr, b_cols, True)
        x_own(k, zr, b_cols, False)
        z_wait(zr, True)
        z_send(k, zr, True)
        x_rest(k - 1, before, b_cols)
        project(before)
    x_forward(NZ - 1, zs[-1], b_cols)
    x_rest(NZ - 1, zs[-1], b_cols)
    project(zs[-1])
    sends.finish()


def gather_project_call(tokens, gain, wq, wk, wv):
    rows, width = tokens.shape
    cols = wq.shape[1] + 2 * wk.shape[1]
    vmem = pl.BlockSpec(memory_space=pltpu.VMEM)
    any_space = pl.BlockSpec(memory_space=pl.ANY)
    dma = pltpu.SemaphoreType.DMA
    return pl.pallas_call(
        gather_project,
        out_shape=jax.ShapeDtypeStruct((rows * NX * NZ, cols), jnp.bfloat16),
        in_specs=[vmem, vmem, any_space, any_space, any_space],
        out_specs=vmem,
        scratch_shapes=[
            pltpu.VMEM((NZ, NX * rows, width), jnp.bfloat16),
            pltpu.VMEM((width, cols), jnp.bfloat16),
            dma((3,)),
            dma((2, NZ + 1, 3)),
            dma((2, NZ, NX, 2)),
            dma((2, NZ)),
            dma((NZ,)),
            dma((2, NZ)),
            dma((NZ,)),
        ],
        compiler_params=pltpu.CompilerParams(
            collective_id=0, has_side_effects=True, vmem_limit_bytes=40 * 1024 * 1024
        ),
    )(tokens, gain, wq, wk, wv)


def product_scatter(
    tokens_ref, gain_ref, grads_ref, wq_ref, wk_ref, wv_ref, out_ref,
    p, w, total, got_opp, got_x, got_za, got_zb, w_sem, s1, r1, s2, r2, sza, rza, szb, rzb,
):
    x, z = place()
    rows, width = tokens_ref.shape
    half = rows // 2
    a_width = A_TILES * 128
    a_cols = pl.ds(0, a_width)
    b_cols = pl.ds(a_width, width - a_width)
    xp, xm, xo = (x + 1) % NX, (x + 3) % NX, (x + 2) % NX
    zs = near_to_far(z)[::-1]
    q_cols, k_cols = wq_ref.shape[1], wk_ref.shape[1]
    barrier = greet_plane(x, z)
    loads = [
        pltpu.make_async_copy(wq_ref, w.at[:, pl.ds(0, q_cols)], w_sem.at[0]),
        pltpu.make_async_copy(wk_ref, w.at[:, pl.ds(q_cols, k_cols)], w_sem.at[1]),
        pltpu.make_async_copy(wv_ref, w.at[:, pl.ds(q_cols + k_cols, k_cols)], w_sem.at[2]),
    ]
    for load in loads:
        load.start()
    await_plane(barrier, z)
    for load in loads:
        load.wait()
    sends = Sends()
    tile = 512

    def row_ds(xr, h=None):
        if h is None:
            return pl.ds(pl.multiple_of(xr * rows, rows), rows)
        return pl.ds(pl.multiple_of(xr * rows + h * half, half), half)

    def compute(zr):
        lhs = jnp.concatenate(
            [
                grads_ref[pl.ds(pl.multiple_of(i * NZ * rows + zr * rows, rows), rows), :]
                for i in range(NX)
            ],
            axis=0,
        )

        @pl.loop(0, width // tile)
        def _(j):
            at = pl.ds(pl.multiple_of(j * tile, tile), tile)
            p[zr, :, at] = lax.dot_general(
                lhs, w[at, :], (((1,), (1,)), ((), ())), preferred_element_type=jnp.float32
            ).astype(jnp.bfloat16)

    def far_exists(zr):
        return ((zr < z) & (z < NZ - 1)) | ((zr > z) & (z > 0))

    def way(zr):
        return jnp.where(zr > z, 1, 0)

    def nearer(zr):
        return tp_of(x, jnp.where(zr > z, z + 1, z - 1))

    def step1(k, zr, cols):
        for direction, to in ((0, xm), (1, xp)):
            sends.start(
                send_to(
                    p.at[zr, row_ds(xo, direction), cols],
                    got_opp.at[direction, zr, :, cols],
                    s1.at[direction, k],
                    r1.at[direction, k],
                    tp_of(to, z),
                )
            )

    def step2(k, zr, cols):
        for direction, to in ((0, xm), (1, xp)):
            land = got_opp.at[direction, zr, :, cols]
            send_to(land, land, s1.at[direction, k], r1.at[direction, k], tp_of(to, z)).wait_recv()
            at = row_ds(to, direction)
            p[zr, at, cols] = (
                p[zr, at, cols].astype(jnp.float32)
                + got_opp[direction, zr, :, cols].astype(jnp.float32)
            ).astype(jnp.bfloat16)
            sends.start(
                send_to(
                    p.at[zr, row_ds(to), cols],
                    got_x.at[direction, zr, :, cols],
                    s2.at[direction, k],
                    r2.at[direction, k],
                    tp_of(to, z),
                )
            )

    def x_sum(k, zr, cols):
        for direction, to in ((0, xm), (1, xp)):
            land = got_x.at[direction, zr, :, cols]
            send_to(land, land, s2.at[direction, k], r2.at[direction, k], tp_of(to, z)).wait_recv()
        return (
            p[zr, row_ds(x), cols].astype(jnp.float32)
            + got_x[0, zr, :, cols].astype(jnp.float32)
            + got_x[1, zr, :, cols].astype(jnp.float32)
        )

    def z_wait_b(d, zr):
        land = got_zb.at[d, zr]
        send_to(land, land, szb.at[0], rzb.at[d, zr], tp_of(xp, z)).wait_recv()

    def z_wait_a(d, zr):
        land = got_za.at[d, zr]
        send_to(land, land, sza.at[0], rza.at[d, zr], tp_of(xp, z)).wait_recv()

    def step3(k, zr, far):
        copy = send_to(
            p.at[zr, row_ds(x), b_cols], got_zb.at[way(zr), zr], szb.at[k],
            rzb.at[way(zr), zr], nearer(zr),
        )

        def run():
            value = x_sum(k, zr, b_cols)
            if far:
                z_wait_b(way(zr), zr)
                value = value + got_zb[way(zr), zr].astype(jnp.float32)
            p[zr, row_ds(x), b_cols] = value.astype(jnp.bfloat16)
            copy.start()

        if far:
            pl.when(far_exists(zr))(run)
            sends.started.append((copy, None))
        else:
            pl.when(jnp.logical_not(far_exists(zr)))(run)

    def line_a(k, zr, far):
        copy = send_to(
            p.at[zr, :, a_cols], got_za.at[way(zr), zr], sza.at[k],
            rza.at[way(zr), zr], nearer(zr),
        )

        def run():
            if far:
                z_wait_a(way(zr), zr)
                p[zr, :, a_cols] = (
                    p[zr, :, a_cols].astype(jnp.float32)
                    + got_za[way(zr), zr].astype(jnp.float32)
                ).astype(jnp.bfloat16)
            copy.start()

        if far:
            pl.when(far_exists(zr))(run)
            sends.started.append((copy, None))
        else:
            pl.when(jnp.logical_not(far_exists(zr)))(run)

    compute(zs[0])
    step1(0, zs[0], b_cols)
    line_a(0, zs[0], False)
    compute(zs[1])
    step1(1, zs[1], b_cols)
    line_a(1, zs[1], False)
    step2(0, zs[0], b_cols)
    line_a(0, zs[0], True)
    compute(zs[2])
    step1(2, zs[2], b_cols)
    line_a(2, zs[2], False)
    step2(1, zs[1], b_cols)
    line_a(1, zs[1], True)
    step3(0, zs[0], False)
    compute(z)
    step1(3, z, b_cols)
    step2(2, zs[2], b_cols)
    line_a(2, zs[2], True)
    step3(1, zs[1], False)
    step3(0, zs[0], True)
    step2(3, z, b_cols)
    step3(2, zs[2], False)

    for d, there in ((0, z < NZ - 1), (1, z > 0)):

        @pl.when(there)
        def _(d=d):
            z_wait_a(d, z)
            p[z, :, a_cols] = (
                p[z, :, a_cols].astype(jnp.float32) + got_za[d, z].astype(jnp.float32)
            ).astype(jnp.bfloat16)

    step1(4, z, a_cols)
    step3(1, zs[1], True)
    step2(4, z, a_cols)
    step3(2, zs[2], True)
    total[:, b_cols] = x_sum(3, z, b_cols)
    for d, there in ((0, z < NZ - 1), (1, z > 0)):

        @pl.when(there)
        def _(d=d):
            z_wait_b(d, z)
            total[:, b_cols] = total[:, b_cols] + got_zb[d, z].astype(jnp.float32)

    total[:, a_cols] = x_sum(4, z, a_cols)
    values = tokens_ref[...].astype(jnp.float32)
    inv = lax.rsqrt(jnp.mean(values * values, axis=1, keepdims=True) + EPS)
    upper = total[...] * gain_ref[...]
    xhat = values * inv
    out_ref[...] = (
        inv * (upper - xhat * jnp.mean(upper * xhat, axis=1, keepdims=True))
    ).astype(jnp.bfloat16)
    sends.finish()


def product_scatter_call(tokens, gain, grads, wq, wk, wv):
    rows, width = tokens.shape
    cols = wq.shape[1] + 2 * wk.shape[1]
    a_width = A_TILES * 128
    vmem = pl.BlockSpec(memory_space=pltpu.VMEM)
    any_space = pl.BlockSpec(memory_space=pl.ANY)
    dma = pltpu.SemaphoreType.DMA
    return pl.pallas_call(
        product_scatter,
        out_shape=jax.ShapeDtypeStruct((rows, width), jnp.bfloat16),
        in_specs=[vmem, vmem, vmem, any_space, any_space, any_space],
        out_specs=vmem,
        scratch_shapes=[
            pltpu.VMEM((NZ, NX * rows, width), jnp.bfloat16),
            pltpu.VMEM((width, cols), jnp.bfloat16),
            pltpu.VMEM((rows, width), jnp.float32),
            pltpu.VMEM((2, NZ, rows // 2, width), jnp.bfloat16),
            pltpu.VMEM((2, NZ, rows, width), jnp.bfloat16),
            pltpu.VMEM((2, NZ, NX * rows, a_width), jnp.bfloat16),
            pltpu.VMEM((2, NZ, rows, width - a_width), jnp.bfloat16),
            dma((3,)),
            dma((2, NZ + 1)),
            dma((2, NZ + 1)),
            dma((2, NZ + 1)),
            dma((2, NZ + 1)),
            dma((NZ,)),
            dma((2, NZ)),
            dma((NZ,)),
            dma((2, NZ)),
        ],
        compiler_params=pltpu.CompilerParams(
            collective_id=1, has_side_effects=True, vmem_limit_bytes=48 * 1024 * 1024
        ),
    )(tokens, gain, grads, wq, wk, wv)


def shifted(block, axis, distance):
    devices = range(lax.axis_size(axis))
    route = [(i - distance, i) for i in devices if i - distance in devices]
    return lax.ppermute(block, axis, route)


def block_grads(query_blk, grad_blk, key_blk, value_blk, query_pos, key_pos):
    row_count = query_blk.shape[0]
    key_span = key_blk.shape[0]
    kv_heads = key_blk.shape[1] // HEAD_SIZE
    groups = query_blk.shape[1] // key_blk.shape[1]
    query_four = query_blk.reshape(row_count, kv_heads, groups, HEAD_SIZE)
    grad_four = grad_blk.reshape(row_count, kv_heads, groups, HEAD_SIZE)
    key_three = key_blk.reshape(key_span, kv_heads, HEAD_SIZE)
    value_three = value_blk.reshape(key_span, kv_heads, HEAD_SIZE)
    raw = jnp.einsum("qkgd,skd->kgqs", query_four, key_three, preferred_element_type=jnp.float32)
    bent = jnp.tanh(raw * SCALE / CAP)
    capped = CAP * bent
    valid = (
        (key_pos[None, :] <= query_pos[:, None])
        & (key_pos[None, :] > query_pos[:, None] - WINDOW)
        & (key_pos[None, :] >= 0)
    )
    expo = jnp.where(valid, jnp.exp(capped), 0.0)
    probs = expo / jnp.sum(expo, axis=-1, keepdims=True)
    d_probs = jnp.einsum(
        "qkgd,skd->kgqs", grad_four, value_three, preferred_element_type=jnp.float32
    )
    delta = jnp.sum(probs * d_probs, axis=-1, keepdims=True)
    d_raw = (probs * (d_probs - delta) * (1.0 - bent * bent) * SCALE).astype(jnp.bfloat16)
    probs_low = probs.astype(jnp.bfloat16)
    grad_query = jnp.einsum(
        "kgqs,skd->qkgd", d_raw, key_three, preferred_element_type=jnp.float32
    ).reshape(row_count, kv_heads * groups * HEAD_SIZE)
    grad_key = jnp.einsum(
        "kgqs,qkgd->skd", d_raw, query_four, preferred_element_type=jnp.float32
    ).reshape(key_span, kv_heads * HEAD_SIZE)
    grad_value = jnp.einsum(
        "kgqs,qkgd->skd", probs_low, grad_four, preferred_element_type=jnp.float32
    ).reshape(key_span, kv_heads * HEAD_SIZE)
    return (grad_query, grad_key, grad_value)


def on_device(tokens, norm_gain, query_weight, key_matrix, value_matrix, output_grad):
    local_rows = output_grad.shape[0]
    query_cols = query_weight.shape[1]
    key_cols = key_matrix.shape[1]
    reach = WINDOW - local_rows
    key_span = WINDOW + local_rows
    gain = norm_gain.reshape(1, -1)
    joined = gather_project_call(tokens, gain, query_weight, key_matrix, value_matrix)
    query_own = joined[:, :query_cols]
    key_own = joined[:, query_cols : query_cols + key_cols]
    value_own = joined[:, query_cols + key_cols :]
    near_key, near_value = shifted((key_own, value_own), "seq", 1)
    far_key, far_value = shifted(
        (key_own[local_rows - reach :], value_own[local_rows - reach :]), "seq", 2
    )
    all_key = jnp.concatenate([far_key, near_key, key_own], axis=0)
    all_value = jnp.concatenate([far_value, near_value, value_own], axis=0)
    anchor = lax.axis_index("seq") * local_rows
    query_pos = anchor + jnp.arange(local_rows, dtype=jnp.int32)
    key_pos = anchor - WINDOW + jnp.arange(key_span, dtype=jnp.int32)
    grad_query, acc_key, acc_value = block_grads(
        query_own, output_grad, all_key, all_value, query_pos, key_pos
    )
    far_back_key, far_back_value = shifted((acc_key[:reach], acc_value[:reach]), "seq", -2)
    back_key, back_value = shifted(
        (acc_key[reach : reach + local_rows], acc_value[reach : reach + local_rows]), "seq", -1
    )
    own_gkey = acc_key[reach + local_rows :] + back_key
    own_gvalue = acc_value[reach + local_rows :] + back_value
    own_gkey = own_gkey.at[local_rows - reach :].add(far_back_key)
    own_gvalue = own_gvalue.at[local_rows - reach :].add(far_back_value)
    grads = jnp.concatenate([grad_query, own_gkey, own_gvalue], axis=1).astype(jnp.bfloat16)
    return product_scatter_call(tokens, gain, grads, query_weight, key_matrix, value_matrix)


def solution(mesh):
    tp, both = "tp", ("seq", "tp")
    in_specs = (P(both, None), P(), P(None, tp), P(None, tp), P(None, tp), P("seq", tp))
    return jax.shard_map(
        on_device, mesh=mesh, in_specs=in_specs, out_specs=P(both, None), check_vma=False
    )
```

```python
import jax
import jax.numpy as jnp
from jax import lax
from jax.experimental import pallas as pl
from jax.experimental.pallas import tpu as pltpu
from jax.sharding import PartitionSpec as P

HEAD_SIZE = 128
WINDOW = 640
SCALE = 1.0 / 12.0
CAP = 50.0
EPS = 1e-06
MESH = pl.DeviceIdType.MESH
NX = 4
NZ = 4
A_TILES = 8


def place():
    t = lax.axis_index("tp")
    return t // NZ, t % NZ


def near_to_far(z):
    def high(q):
        return (q, 5 - q, jnp.int32(1), jnp.int32(0))

    up = high(z)
    low = high(3 - z)
    return [jnp.where(z >= 2, u, 3 - v) for u, v in zip(up, low)]


def send_to(src, dst, send_sem, recv_sem, tp):
    return pltpu.make_async_remote_copy(
        src_ref=src,
        dst_ref=dst,
        send_sem=send_sem,
        recv_sem=recv_sem,
        device_id={"tp": tp},
        device_id_type=MESH,
    )


def tp_of(x, z):
    return x * NZ + z


def send_along(src, dst, send_sem, recv_sem, seq):
    return pltpu.make_async_remote_copy(
        src_ref=src,
        dst_ref=dst,
        send_sem=send_sem,
        recv_sem=recv_sem,
        device_id={"seq": seq},
        device_id_type=MESH,
    )


def greet_partners(x, z, s, blocks):
    barrier = pltpu.get_barrier_semaphore()

    def greet(device):
        pl.semaphore_signal(barrier, inc=1, device_id=device, device_id_type=MESH)

    greet({"tp": tp_of((x + 1) % NX, z)})
    greet({"tp": tp_of((x + 3) % NX, z)})
    pl.when(z > 0)(lambda: greet({"tp": tp_of(x, z - 1)}))
    pl.when(z < NZ - 1)(lambda: greet({"tp": tp_of(x, z + 1)}))
    count = jnp.where((z == 0) | (z == NZ - 1), 3, 4)
    for step in (-2, -1, 1, 2):
        there = (s + step >= 0) & (s + step < blocks)
        pl.when(there)(lambda step=step: greet({"seq": s + step}))
        count = count + jnp.where(there, 1, 0)
    return barrier, count


class Sends:
    def __init__(self):
        self.started = []

    def start(self, copy, when=None):
        self.started.append((copy, when))
        if when is None:
            copy.start()
        else:
            pl.when(when)(lambda: copy.start())

    def finish(self):
        for copy, when in self.started:
            if when is None:
                copy.wait_send()
            else:
                pl.when(when)(lambda copy=copy: copy.wait_send())


def whole(
    tokens_ref, gain_ref, grad_ref, wq_ref, wk_ref, wv_ref, out_ref,
    tok, gain, w, g, dout, qb, kv, kt, e_buf, dp_buf, b_buf, dr_buf, acc,
    back_out, back_near, back_far, grads, total, got_opp, got_x, got_za, got_zb,
    load_sem, sx, rx, szb, rzb, sza, rza, s_near, r_near, s_far, r_far,
    s_bn, r_bn, s_bf, r_bf, s1, r1, s2, r2, tza, uza, tzb, uzb,
):
    x, z = place()
    s = lax.axis_index("seq")
    blocks = lax.axis_size("seq")
    rows, width = tok.shape
    half = rows // 2
    a_width = A_TILES * 128
    a_cols = pl.ds(0, a_width)
    b_cols = pl.ds(a_width, width - a_width)
    xp, xm, xo = (x + 1) % NX, (x + 3) % NX, (x + 2) % NX
    zs = near_to_far(z)
    q_cols, k_cols = wq_ref.shape[1], wk_ref.shape[1]
    barrier, partners = greet_partners(x, z, s, blocks)
    loads = [
        pltpu.make_async_copy(tokens_ref, tok, load_sem.at[0]),
        pltpu.make_async_copy(gain_ref, gain, load_sem.at[1]),
        pltpu.make_async_copy(wq_ref, w.at[:, pl.ds(0, q_cols)], load_sem.at[2]),
        pltpu.make_async_copy(wk_ref, w.at[:, pl.ds(q_cols, k_cols)], load_sem.at[3]),
        pltpu.make_async_copy(wv_ref, w.at[:, pl.ds(q_cols + k_cols, k_cols)], load_sem.at[4]),
        pltpu.make_async_copy(grad_ref, dout, load_sem.at[5]),
    ]
    for load in loads:
        load.start()
    loads[0].wait()
    loads[1].wait()
    values = tok[...].astype(jnp.float32)
    inv_rms = lax.rsqrt(jnp.mean(values * values, axis=1, keepdims=True) + EPS)
    g[z, pl.ds(x * rows, rows), :] = (values * inv_rms * gain[...]).astype(jnp.bfloat16)
    pl.semaphore_wait(barrier, partners)
    sends = Sends()

    def part(zr, xr, h, cols):
        if h is None:
            return g.at[zr, pl.ds(pl.multiple_of(xr * rows, rows), rows), cols]
        return g.at[zr, pl.ds(pl.multiple_of(xr * rows + h * half, half), half), cols]

    def x_send(k, zr, xr, h, cols, to, direction, slot):
        piece = part(zr, xr, h, cols)
        p = 1 if k == NZ else 0
        sends.start(
            send_to(piece, piece, sx.at[direction, k, slot], rx.at[p, zr, xr, h], tp_of(to, z))
        )

    def x_wait(k, zr, xr, h, cols):
        piece = part(zr, xr, h, cols)
        p = 1 if k == NZ else 0
        send_to(piece, piece, sx.at[0, k, 0], rx.at[p, zr, xr, h], tp_of(xp, z)).wait_recv()

    def x_own(k, zr, cols, first):
        h_right, h_left = (0, 1) if first else (1, 0)
        slot = 0 if first else 1
        x_send(k, zr, x, h_right, cols, xp, 0, slot)
        x_send(k, zr, x, h_left, cols, xm, 1, slot)

    def x_forward(k, zr, cols):
        x_wait(k, zr, xm, 0, cols)
        x_send(k, zr, xm, 0, cols, xp, 0, 2)
        x_wait(k, zr, xp, 1, cols)
        x_send(k, zr, xp, 1, cols, xm, 1, 2)

    def x_rest(k, zr, cols):
        x_wait(k, zr, xm, 1, cols)
        x_wait(k, zr, xp, 0, cols)
        x_wait(k, zr, xo, 0, cols)
        x_wait(k, zr, xo, 1, cols)

    def z_piece(zr, is_a):
        return g.at[zr, :, a_cols] if is_a else part(zr, x, None, b_cols)

    def z_send(k, zr, is_a):
        piece = z_piece(zr, is_a)
        ss, rs = (sza, rza) if is_a else (szb, rzb)
        up = send_to(piece, piece, ss.at[0, k], rs.at[zr], tp_of(x, jnp.minimum(z + 1, NZ - 1)))
        down = send_to(piece, piece, ss.at[1, k], rs.at[zr], tp_of(x, jnp.maximum(z - 1, 0)))
        sends.start(up, (zr <= z) & (z < NZ - 1))
        sends.start(down, (zr >= z) & (z > 0))

    def z_wait(zr, is_a):
        piece = z_piece(zr, is_a)
        ss, rs = (sza, rza) if is_a else (szb, rzb)
        send_to(piece, piece, ss.at[0, 0], rs.at[zr], tp_of(xp, z)).wait_recv()

    def slab(first, count, zr):
        return kv.at[pl.ds(first, count), pl.ds(pl.multiple_of(zr * rows, rows), rows), :]

    def near_copy(k, zr):
        return send_along(
            slab(5, 4, zr), slab(1, 4, zr), s_near.at[k], r_near.at[k],
            jnp.minimum(s + 1, blocks - 1),
        )

    def far_copy(k, zr):
        return send_along(
            slab(8, 1, zr), slab(0, 1, zr), s_far.at[k], r_far.at[k],
            jnp.minimum(s + 2, blocks - 1),
        )

    def project(k):
        zr = zs[k]
        out = jnp.dot(g[zr], w[...], preferred_element_type=jnp.float32).astype(jnp.bfloat16)
        at = pl.ds(pl.multiple_of(zr * rows, rows), rows)
        for i in range(NX):
            kv[5 + i, at, :] = out[i * rows : (i + 1) * rows, q_cols:]
            qb[i, at, :] = out[i * rows : (i + 1) * rows, :q_cols]
        sends.start(near_copy(k, zr), s + 1 < blocks)
        sends.start(far_copy(k, zr), s + 2 < blocks)

    x_own(NZ, z, a_cols, True)
    x_own(NZ, z, a_cols, False)
    z_send(0, z, False)
    x_own(0, z, b_cols, True)
    x_forward(NZ, z, a_cols)
    x_own(0, z, b_cols, False)
    x_rest(NZ, z, a_cols)
    z_send(0, z, True)
    for load in loads[2:]:
        load.wait()
    acc[...] = jnp.zeros_like(acc)

    @pl.when(s == 0)
    def _():
        kv[0:5] = jnp.zeros_like(kv[0:5])

    @pl.when(s == 1)
    def _():
        kv[0] = jnp.zeros_like(kv[0])

    @pl.when(s == blocks - 1)
    def _():
        back_near[...] = jnp.zeros_like(back_near)

    @pl.when(s >= blocks - 2)
    def _():
        back_far[...] = jnp.zeros_like(back_far)

    for k in range(1, NZ):
        zr, before = zs[k], zs[k - 1]
        x_forward(k - 1, before, b_cols)
        z_wait(zr, False)
        z_send(k, zr, False)
        x_own(k, zr, b_cols, True)
        x_own(k, zr, b_cols, False)
        z_wait(zr, True)
        z_send(k, zr, True)
        x_rest(k - 1, before, b_cols)
        project(k - 1)
    x_forward(NZ - 1, zs[-1], b_cols)
    x_rest(NZ - 1, zs[-1], b_cols)
    project(NZ - 1)

    hd = HEAD_SIZE
    last = (((1,), (1,)), ((), ()))

    def two_heads(ref, qt):
        return jnp.concatenate([ref[qt, :, 0:hd], ref[qt, :, hd : 2 * hd]], axis=0)

    row_at = lax.broadcasted_iota(jnp.int32, (hd, 2 * hd), 0)
    col_at = lax.broadcasted_iota(jnp.int32, (hd, 2 * hd), 1) % hd

    def scores(qt, c, q2, do2):
        j = qt + c
        raw = lax.dot_general(kv[j, :, 0:hd], q2, last, preferred_element_type=jnp.float32)
        bent = jnp.tanh(raw * (SCALE / CAP))
        expo = jnp.exp(CAP * bent)
        if c == 0:
            expo = jnp.where(row_at > col_at, expo, 0.0)
        if c == 5:
            expo = jnp.where(row_at <= col_at, expo, 0.0)
        if j < 5:
            expo = expo * jnp.where(s >= (1 if j > 0 else 2), 1.0, 0.0)
        d_probs = lax.dot_general(
            kv[j, :, hd : 2 * hd], do2, last, preferred_element_type=jnp.float32
        )
        e_buf[qt, c] = expo
        dp_buf[qt, c] = d_probs
        b_buf[qt, c] = bent
        shape = (hd // 8, 8, 2 * hd)
        return (
            jnp.sum(expo.reshape(shape), axis=0),
            jnp.sum((expo * d_probs).reshape(shape), axis=0),
        )

    def transpose_keys(j):
        kt[:, pl.ds(j * hd, hd)] = kv[j, :, 0:hd].astype(jnp.float32).T.astype(jnp.bfloat16)

    sums = []
    for qt in range(NX):
        q2, do2 = two_heads(qb, qt), two_heads(dout, qt)
        parts = [scores(qt, c, q2, do2) for c in range(5 - qt, 6)]
        sums.append((sum(p[0] for p in parts), sum(p[1] for p in parts)))
    for j in range(5, 9):
        transpose_keys(j)

    @pl.when(s > 0)
    def _():
        for k in range(NZ):
            near_copy(k, zs[k]).wait_recv()

    @pl.when(s > 1)
    def _():
        for k in range(NZ):
            far_copy(k, zs[k]).wait_recv()

    for j in range(5):
        transpose_keys(j)

    gathering, sends = sends, Sends()

    def give_back(j):
        back_out[j] = acc[j].astype(jnp.bfloat16)
        if j == 0:
            far = send_along(
                back_out.at[0], back_far, s_bf.at[0], r_bf.at[0], jnp.maximum(s - 2, 0)
            )
            sends.start(far, s > 1)
        else:
            near = send_along(
                back_out.at[j], back_near.at[j - 1], s_bn.at[j - 1], r_bn.at[j - 1],
                jnp.maximum(s - 1, 0),
            )
            sends.start(near, s > 0)

    for qt in range(NX):
        q2, do2 = two_heads(qb, qt), two_heads(dout, qt)
        parts = [scores(qt, c, q2, do2) for c in range(0, 5 - qt)]
        norm = jnp.sum(sums[qt][0] + sum(p[0] for p in parts), axis=0, keepdims=True)
        inner = jnp.sum(sums[qt][1] + sum(p[1] for p in parts), axis=0, keepdims=True)
        inverse = 1.0 / norm
        delta = inner * inverse
        for c in range(6):
            probs = e_buf[qt, c] * inverse
            bent = b_buf[qt, c]
            d_raw = (
                probs * (dp_buf[qt, c] - delta) * (1.0 - bent * bent) * SCALE
            ).astype(jnp.bfloat16)
            dr_buf[pl.ds(c * hd, hd), :] = d_raw
            acc[qt + c, :, 0:hd] += jnp.dot(d_raw, q2, preferred_element_type=jnp.float32)
            acc[qt + c, :, hd : 2 * hd] += jnp.dot(
                probs.astype(jnp.bfloat16), do2, preferred_element_type=jnp.float32
            )
        d_query = jnp.dot(
            kt[:, pl.ds(qt * hd, 6 * hd)], dr_buf[...], preferred_element_type=jnp.float32
        )
        grads[qt, :, 0:hd] = d_query[:, 0:hd].T.astype(jnp.bfloat16)
        grads[qt, :, hd : 2 * hd] = d_query[:, hd : 2 * hd].T.astype(jnp.bfloat16)
        give_back(qt)
    give_back(4)

    @pl.when(s < blocks - 2)
    def _():
        send_along(back_out.at[0], back_far, s_bf.at[0], r_bf.at[0], s).wait_recv()

    @pl.when(s < blocks - 1)
    def _():
        for i in range(NX):
            send_along(
                back_out.at[i + 1], back_near.at[i], s_bn.at[i], r_bn.at[i], s
            ).wait_recv()

    for i in range(NX):
        own = acc[5 + i] + back_near[i].astype(jnp.float32)
        if i == NX - 1:
            own = own + back_far[...].astype(jnp.float32)
        grads[i, :, q_cols:] = own.astype(jnp.bfloat16)

    gathering.finish()
    zs = zs[::-1]
    p = g
    tile = 512

    def row_ds(xr, h=None):
        if h is None:
            return pl.ds(pl.multiple_of(xr * rows, rows), rows)
        return pl.ds(pl.multiple_of(xr * rows + h * half, half), half)

    def compute(zr):
        lhs = grads[:, pl.ds(pl.multiple_of(zr * rows, rows), rows), :].reshape(NX * rows, -1)

        @pl.loop(0, width // tile)
        def _(j):
            at = pl.ds(pl.multiple_of(j * tile, tile), tile)
            p[zr, :, at] = lax.dot_general(
                lhs, w[at, :], (((1,), (1,)), ((), ())), preferred_element_type=jnp.float32
            ).astype(jnp.bfloat16)

    def far_exists(zr):
        return ((zr < z) & (z < NZ - 1)) | ((zr > z) & (z > 0))

    def way(zr):
        return jnp.where(zr > z, 1, 0)

    def nearer(zr):
        return tp_of(x, jnp.where(zr > z, z + 1, z - 1))

    def step1(k, zr, cols):
        for direction, to in ((0, xm), (1, xp)):
            sends.start(
                send_to(
                    p.at[zr, row_ds(xo, direction), cols],
                    got_opp.at[direction, zr, :, cols],
                    s1.at[direction, k],
                    r1.at[direction, k],
                    tp_of(to, z),
                )
            )

    def step2(k, zr, cols):
        for direction, to in ((0, xm), (1, xp)):
            land = got_opp.at[direction, zr, :, cols]
            send_to(land, land, s1.at[direction, k], r1.at[direction, k], tp_of(to, z)).wait_recv()
            at = row_ds(to, direction)
            p[zr, at, cols] = (
                p[zr, at, cols].astype(jnp.float32)
                + got_opp[direction, zr, :, cols].astype(jnp.float32)
            ).astype(jnp.bfloat16)
            sends.start(
                send_to(
                    p.at[zr, row_ds(to), cols],
                    got_x.at[direction, zr, :, cols],
                    s2.at[direction, k],
                    r2.at[direction, k],
                    tp_of(to, z),
                )
            )

    def x_sum(k, zr, cols):
        for direction, to in ((0, xm), (1, xp)):
            land = got_x.at[direction, zr, :, cols]
            send_to(land, land, s2.at[direction, k], r2.at[direction, k], tp_of(to, z)).wait_recv()
        return (
            p[zr, row_ds(x), cols].astype(jnp.float32)
            + got_x[0, zr, :, cols].astype(jnp.float32)
            + got_x[1, zr, :, cols].astype(jnp.float32)
        )

    def z_wait_b(d, zr):
        land = got_zb.at[d, zr]
        send_to(land, land, tzb.at[0], uzb.at[d, zr], tp_of(xp, z)).wait_recv()

    def z_wait_a(d, zr):
        land = got_za.at[d, zr]
        send_to(land, land, tza.at[0], uza.at[d, zr], tp_of(xp, z)).wait_recv()

    def step3(k, zr, far):
        copy = send_to(
            p.at[zr, row_ds(x), b_cols], got_zb.at[way(zr), zr], tzb.at[k],
            uzb.at[way(zr), zr], nearer(zr),
        )

        def run():
            value = x_sum(k, zr, b_cols)
            if far:
                z_wait_b(way(zr), zr)
                value = value + got_zb[way(zr), zr].astype(jnp.float32)
            p[zr, row_ds(x), b_cols] = value.astype(jnp.bfloat16)
            copy.start()

        if far:
            pl.when(far_exists(zr))(run)
            sends.started.append((copy, None))
        else:
            pl.when(jnp.logical_not(far_exists(zr)))(run)

    def line_a(k, zr, far):
        copy = send_to(
            p.at[zr, :, a_cols], got_za.at[way(zr), zr], tza.at[k],
            uza.at[way(zr), zr], nearer(zr),
        )

        def run():
            if far:
                z_wait_a(way(zr), zr)
                p[zr, :, a_cols] = (
                    p[zr, :, a_cols].astype(jnp.float32)
                    + got_za[way(zr), zr].astype(jnp.float32)
                ).astype(jnp.bfloat16)
            copy.start()

        if far:
            pl.when(far_exists(zr))(run)
            sends.started.append((copy, None))
        else:
            pl.when(jnp.logical_not(far_exists(zr)))(run)

    compute(zs[0])
    step1(0, zs[0], b_cols)
    line_a(0, zs[0], False)
    compute(zs[1])
    step1(1, zs[1], b_cols)
    line_a(1, zs[1], False)
    step2(0, zs[0], b_cols)
    line_a(0, zs[0], True)
    compute(zs[2])
    step1(2, zs[2], b_cols)
    line_a(2, zs[2], False)
    step2(1, zs[1], b_cols)
    line_a(1, zs[1], True)
    step3(0, zs[0], False)
    compute(z)
    step1(3, z, b_cols)
    step2(2, zs[2], b_cols)
    line_a(2, zs[2], True)
    step3(1, zs[1], False)
    step3(0, zs[0], True)
    step2(3, z, b_cols)
    step3(2, zs[2], False)

    for d, there in ((0, z < NZ - 1), (1, z > 0)):

        @pl.when(there)
        def _(d=d):
            z_wait_a(d, z)
            p[z, :, a_cols] = (
                p[z, :, a_cols].astype(jnp.float32) + got_za[d, z].astype(jnp.float32)
            ).astype(jnp.bfloat16)

    step1(4, z, a_cols)
    step3(1, zs[1], True)
    step2(4, z, a_cols)
    step3(2, zs[2], True)
    total[:, b_cols] = x_sum(3, z, b_cols)
    for d, there in ((0, z < NZ - 1), (1, z > 0)):

        @pl.when(there)
        def _(d=d):
            z_wait_b(d, z)
            total[:, b_cols] = total[:, b_cols] + got_zb[d, z].astype(jnp.float32)

    total[:, a_cols] = x_sum(4, z, a_cols)
    values = tok[...].astype(jnp.float32)
    inv_rms = lax.rsqrt(jnp.mean(values * values, axis=1, keepdims=True) + EPS)
    upper = total[...] * gain[...]
    xhat = values * inv_rms
    out_ref[...] = (
        inv_rms * (upper - xhat * jnp.mean(upper * xhat, axis=1, keepdims=True))
    ).astype(jnp.bfloat16)
    sends.finish()


def on_device(tokens, norm_gain, query_weight, key_matrix, value_matrix, output_grad):
    rows, width = tokens.shape
    q_cols, k_cols = query_weight.shape[1], key_matrix.shape[1]
    cols = q_cols + 2 * k_cols
    a_width = A_TILES * 128
    hd = HEAD_SIZE
    any_space = pl.BlockSpec(memory_space=pl.ANY)
    dma = pltpu.SemaphoreType.DMA
    low, full = jnp.bfloat16, jnp.float32

    def vmem(kind, *shape):
        return pltpu.VMEM(shape, kind)

    return pl.pallas_call(
        whole,
        out_shape=jax.ShapeDtypeStruct((rows, width), low),
        in_specs=[any_space] * 6,
        out_specs=pl.BlockSpec(memory_space=pltpu.VMEM),
        scratch_shapes=[
            vmem(low, rows, width),
            vmem(full, 1, width),
            vmem(low, width, cols),
            vmem(low, NZ, NX * rows, width),
            vmem(low, NX, hd, q_cols),
            vmem(low, NX, hd, q_cols),
            vmem(low, 9, hd, 2 * k_cols),
            vmem(low, hd, 9 * hd),
            vmem(full, NX, 6, hd, 2 * hd),
            vmem(full, NX, 6, hd, 2 * hd),
            vmem(full, NX, 6, hd, 2 * hd),
            vmem(low, 6 * hd, 2 * hd),
            vmem(full, 9, hd, 2 * k_cols),
            vmem(low, 5, hd, 2 * k_cols),
            vmem(low, NX, hd, 2 * k_cols),
            vmem(low, hd, 2 * k_cols),
            vmem(low, NX, hd, cols),
            vmem(full, rows, width),
            vmem(low, 2, NZ, rows // 2, width),
            vmem(low, 2, NZ, rows, width),
            vmem(low, 2, NZ, NX * rows, a_width),
            vmem(low, 2, NZ, rows, width - a_width),
            dma((6,)),
            dma((2, NZ + 1, 3)),
            dma((2, NZ, NX, 2)),
            dma((2, NZ)),
            dma((NZ,)),
            dma((2, NZ)),
            dma((NZ,)),
            dma((NZ,)),
            dma((NZ,)),
            dma((NZ,)),
            dma((NZ,)),
            dma((NX,)),
            dma((NX,)),
            dma((1,)),
            dma((1,)),
            dma((2, NZ + 1)),
            dma((2, NZ + 1)),
            dma((2, NZ + 1)),
            dma((2, NZ + 1)),
            dma((NZ,)),
            dma((2, NZ)),
            dma((NZ,)),
            dma((2, NZ)),
        ],
        compiler_params=pltpu.CompilerParams(
            collective_id=0, has_side_effects=True, vmem_limit_bytes=62 * 1024 * 1024
        ),
    )(
        tokens,
        norm_gain.reshape(1, -1),
        output_grad.reshape(NX, hd, q_cols),
        query_weight,
        key_matrix,
        value_matrix,
    )


def solution(mesh):
    tp, both = "tp", ("seq", "tp")
    in_specs = (P(both, None), P(), P(None, tp), P(None, tp), P(None, tp), P("seq", tp))
    return jax.shard_map(
        on_device, mesh=mesh, in_specs=in_specs, out_specs=P(both, None), check_vma=False
    )
```

```python
import jax
import jax.numpy as jnp
from jax import lax
from jax.experimental import pallas as pl
from jax.experimental.pallas import tpu as pltpu
from jax.sharding import PartitionSpec as P

HEAD_SIZE = 128
WINDOW = 640
SCALE = 1.0 / 12.0
CAP = 50.0
EPS = 1e-06
MESH = pl.DeviceIdType.MESH
NX = 4
NZ = 4
A_TILES = 8
TURN = 512
TURNS = 9


def place():
    t = lax.axis_index("tp")
    return t // NZ, t % NZ


def near_to_far(z):
    def high(q):
        return (q, 5 - q, jnp.int32(1), jnp.int32(0))

    up = high(z)
    low = high(3 - z)
    return [jnp.where(z >= 2, u, 3 - v) for u, v in zip(up, low)]


def send_to(src, dst, send_sem, recv_sem, tp):
    return pltpu.make_async_remote_copy(
        src_ref=src,
        dst_ref=dst,
        send_sem=send_sem,
        recv_sem=recv_sem,
        device_id={"tp": tp},
        device_id_type=MESH,
    )


def tp_of(x, z):
    return x * NZ + z


def send_along(src, dst, send_sem, recv_sem, seq):
    return pltpu.make_async_remote_copy(
        src_ref=src,
        dst_ref=dst,
        send_sem=send_sem,
        recv_sem=recv_sem,
        device_id={"seq": seq},
        device_id_type=MESH,
    )


def greet_partners(x, z, s, blocks):
    barrier = pltpu.get_barrier_semaphore()

    def greet(device):
        pl.semaphore_signal(barrier, inc=1, device_id=device, device_id_type=MESH)

    greet({"tp": tp_of((x + 1) % NX, z)})
    greet({"tp": tp_of((x + 3) % NX, z)})
    pl.when(z > 0)(lambda: greet({"tp": tp_of(x, z - 1)}))
    pl.when(z < NZ - 1)(lambda: greet({"tp": tp_of(x, z + 1)}))
    count = jnp.where((z == 0) | (z == NZ - 1), 3, 4)
    for step in (-2, -1, 1, 2):
        there = (s + step >= 0) & (s + step < blocks)
        pl.when(there)(lambda step=step: greet({"seq": s + step}))
        count = count + jnp.where(there, 1, 0)
    return barrier, count


class Sends:
    def __init__(self):
        self.started = []

    def start(self, copy, when=None):
        self.started.append((copy, when))
        if when is None:
            copy.start()
        else:
            pl.when(when)(lambda: copy.start())

    def finish(self):
        for copy, when in self.started:
            if when is None:
                copy.wait_send()
            else:
                pl.when(when)(lambda copy=copy: copy.wait_send())


def whole(
    tokens_ref, gain_ref, grad_ref, wq_ref, wk_ref, wv_ref, out_ref,
    tok, gain, w, wt, g, dout, qb, kv, kt, e_buf, dp_buf, b_buf, dr_buf, acc,
    back_out, back_near, back_far, grads, total, got_opp, got_x, got_za, got_zb,
    load_sem, sx, rx, szb, rzb, sza, rza, s_near, r_near, s_far, r_far,
    s_bn, r_bn, s_bf, r_bf, s1, r1, s2, r2, tza, uza, tzb, uzb,
):
    x, z = place()
    s = lax.axis_index("seq")
    blocks = lax.axis_size("seq")
    rows, width = tok.shape
    half = rows // 2
    a_width = A_TILES * 128
    a_cols = pl.ds(0, a_width)
    b_cols = pl.ds(a_width, width - a_width)
    xp, xm, xo = (x + 1) % NX, (x + 3) % NX, (x + 2) % NX
    zs = near_to_far(z)
    q_cols, k_cols = wq_ref.shape[1], wk_ref.shape[1]
    barrier, partners = greet_partners(x, z, s, blocks)
    loads = [
        pltpu.make_async_copy(tokens_ref, tok, load_sem.at[0]),
        pltpu.make_async_copy(gain_ref, gain, load_sem.at[1]),
        pltpu.make_async_copy(wq_ref, w.at[:, pl.ds(0, q_cols)], load_sem.at[2]),
        pltpu.make_async_copy(wk_ref, w.at[:, pl.ds(q_cols, k_cols)], load_sem.at[3]),
        pltpu.make_async_copy(wv_ref, w.at[:, pl.ds(q_cols + k_cols, k_cols)], load_sem.at[4]),
        pltpu.make_async_copy(grad_ref, dout, load_sem.at[5]),
    ]
    for load in loads:
        load.start()
    loads[0].wait()
    loads[1].wait()
    values = tok[...].astype(jnp.float32)
    inv_rms = lax.rsqrt(jnp.mean(values * values, axis=1, keepdims=True) + EPS)
    g[z, pl.ds(x * rows, rows), :] = (values * inv_rms * gain[...]).astype(jnp.bfloat16)
    pl.semaphore_wait(barrier, partners)
    sends = Sends()

    def part(zr, xr, h, cols):
        if h is None:
            return g.at[zr, pl.ds(pl.multiple_of(xr * rows, rows), rows), cols]
        return g.at[zr, pl.ds(pl.multiple_of(xr * rows + h * half, half), half), cols]

    def x_send(k, zr, xr, h, cols, to, direction, slot):
        piece = part(zr, xr, h, cols)
        p = 1 if k == NZ else 0
        sends.start(
            send_to(piece, piece, sx.at[direction, k, slot], rx.at[p, zr, xr, h], tp_of(to, z))
        )

    def x_wait(k, zr, xr, h, cols):
        piece = part(zr, xr, h, cols)
        p = 1 if k == NZ else 0
        send_to(piece, piece, sx.at[0, k, 0], rx.at[p, zr, xr, h], tp_of(xp, z)).wait_recv()

    def x_own(k, zr, cols, first):
        h_right, h_left = (0, 1) if first else (1, 0)
        slot = 0 if first else 1
        x_send(k, zr, x, h_right, cols, xp, 0, slot)
        x_send(k, zr, x, h_left, cols, xm, 1, slot)

    def x_forward(k, zr, cols):
        x_wait(k, zr, xm, 0, cols)
        x_send(k, zr, xm, 0, cols, xp, 0, 2)
        x_wait(k, zr, xp, 1, cols)
        x_send(k, zr, xp, 1, cols, xm, 1, 2)

    def x_rest_near(k, zr, cols):
        x_wait(k, zr, xm, 1, cols)
        x_wait(k, zr, xp, 0, cols)

    def x_rest_opposite(k, zr, cols):
        x_wait(k, zr, xo, 0, cols)
        x_wait(k, zr, xo, 1, cols)

    def x_rest(k, zr, cols):
        x_rest_near(k, zr, cols)
        x_rest_opposite(k, zr, cols)

    def z_send_b(k, zr, way, to):
        piece = part(zr, x, None, b_cols)
        sends.start(send_to(piece, piece, szb.at[way, k], rzb.at[zr], tp_of(x, to)))

    def z_send_a(k, zr, xr, way, to):
        piece = part(zr, xr, None, a_cols)
        sends.start(
            send_to(piece, piece, sza.at[way, k, xr], rza.at[zr, xr], tp_of(x, to))
        )

    def z_wait_b(k):
        piece = part(zs[k], x, None, b_cols)
        send_to(piece, piece, szb.at[0, 0], rzb.at[zs[k]], tp_of(xp, z)).wait_recv()

    def z_wait_a(k):
        for i in range(NX):
            piece = part(zs[k], i, None, a_cols)
            send_to(piece, piece, sza.at[0, 0, i], rza.at[zs[k], i], tp_of(xp, z)).wait_recv()

    def turn(c):
        at = pl.ds(c * TURN, TURN)
        wt[:, at] = w[at, :].T

    def slab(first, count, zr):
        return kv.at[pl.ds(first, count), pl.ds(pl.multiple_of(zr * rows, rows), rows), :]

    def near_copy(k, zr):
        return send_along(
            slab(5, 4, zr), slab(1, 4, zr), s_near.at[k], r_near.at[k],
            jnp.minimum(s + 1, blocks - 1),
        )

    def far_copy(k, zr):
        return send_along(
            slab(8, 1, zr), slab(0, 1, zr), s_far.at[k], r_far.at[k],
            jnp.minimum(s + 2, blocks - 1),
        )

    def project(k):
        zr = zs[k]
        out = jnp.dot(g[zr], w[...], preferred_element_type=jnp.float32).astype(jnp.bfloat16)
        at = pl.ds(pl.multiple_of(zr * rows, rows), rows)
        for i in range(NX):
            kv[5 + i, at, :] = out[i * rows : (i + 1) * rows, q_cols:]
            qb[i, at, :] = out[i * rows : (i + 1) * rows, :q_cols]
        pl.when(s + 1 < blocks)(lambda: near_copy(k, zr).start())
        pl.when(s + 2 < blocks)(lambda: far_copy(k, zr).start())

    is_edge = (z == 0) | (z == NZ - 1)

    def start_gather(neighbours):
        x_own(NZ, z, a_cols, True)
        x_own(NZ, z, a_cols, False)
        for way, to in neighbours:
            z_send_b(0, z, way, to)
        x_own(0, z, b_cols, True)
        x_forward(NZ, z, a_cols)
        x_own(0, z, b_cols, False)
        way, to = neighbours[0]
        x_rest_near(NZ, z, a_cols)
        for i in (x, xm, xp):
            z_send_a(0, z, i, way, to)
        for load in loads[2:]:
            load.wait()
        clear_edges()
        turn(0)
        x_rest_opposite(NZ, z, a_cols)
        z_send_a(0, z, xo, way, to)
        x_forward(0, z, b_cols)

    def clear_edges():
        @pl.when(s == 0)
        def _():
            kv[0:5] = jnp.zeros_like(kv[0:5])

        @pl.when(s == 1)
        def _():
            kv[0] = jnp.zeros_like(kv[0])

        @pl.when(s == blocks - 1)
        def _():
            back_near[...] = jnp.zeros_like(back_near)

        @pl.when(s >= blocks - 2)
        def _():
            back_far[...] = jnp.zeros_like(back_far)

    @pl.when(is_edge)
    def _():
        start_gather([(0, jnp.where(z == 0, 1, NZ - 2))])
        z_wait_b(1)
        x_own(1, zs[1], b_cols, True)
        x_own(1, zs[1], b_cols, False)
        for c in range(1, 5):
            turn(c)
        x_rest(0, z, b_cols)
        project(0)
        x_forward(1, zs[1], b_cols)
        turn(5)
        z_wait_b(2)
        x_own(2, zs[2], b_cols, True)
        x_own(2, zs[2], b_cols, False)
        z_wait_a(1)
        x_rest(1, zs[1], b_cols)
        project(1)
        x_forward(2, zs[2], b_cols)
        z_wait_b(3)
        x_own(3, zs[3], b_cols, True)
        x_own(3, zs[3], b_cols, False)
        for c in range(6, TURNS):
            turn(c)
        z_wait_a(2)
        x_rest(2, zs[2], b_cols)
        project(2)
        x_forward(3, zs[3], b_cols)
        z_wait_a(3)
        x_rest(3, zs[3], b_cols)
        project(3)
        sends.finish()

    sends = Sends()

    @pl.when(jnp.logical_not(is_edge))
    def _():
        outer = jnp.where(z == 1, 0, NZ - 1)
        inner = NZ - 1 - z
        start_gather([(0, outer), (1, inner)])
        z_wait_b(1)
        z_send_b(1, zs[1], 1, inner)
        for i in (x, xm, xp, xo):
            z_send_a(0, z, i, 1, inner)
        x_own(1, zs[1], b_cols, True)
        x_own(1, zs[1], b_cols, False)
        z_wait_b(2)
        z_send_b(2, zs[2], 0, outer)
        x_own(2, zs[2], b_cols, True)
        x_own(2, zs[2], b_cols, False)
        for c in range(1, 4):
            turn(c)
        x_rest(0, z, b_cols)
        project(0)
        z_wait_a(1)
        for i in range(NX):
            z_send_a(1, zs[1], i, 1, inner)
        z_wait_b(3)
        z_send_b(3, zs[3], 0, outer)
        x_forward(1, zs[1], b_cols)
        x_own(3, zs[3], b_cols, True)
        x_own(3, zs[3], b_cols, False)
        for c in range(4, 7):
            turn(c)
        x_forward(2, zs[2], b_cols)
        z_wait_a(2)
        for i in range(NX):
            z_send_a(2, zs[2], i, 0, outer)
        for c in range(7, TURNS):
            turn(c)
        x_rest(1, zs[1], b_cols)
        project(1)
        z_wait_a(3)
        for i in range(NX):
            z_send_a(3, zs[3], i, 0, outer)
        x_forward(3, zs[3], b_cols)
        x_rest(2, zs[2], b_cols)
        project(2)
        x_rest(3, zs[3], b_cols)
        project(3)
        sends.finish()

    hd = HEAD_SIZE
    last = (((1,), (1,)), ((), ()))

    def two_heads(ref, qt):
        return jnp.concatenate([ref[qt, :, 0:hd], ref[qt, :, hd : 2 * hd]], axis=0)

    row_at = lax.broadcasted_iota(jnp.int32, (hd, 2 * hd), 0)
    col_at = lax.broadcasted_iota(jnp.int32, (hd, 2 * hd), 1) % hd

    def scores(qt, c, q2, do2):
        j = qt + c
        raw = lax.dot_general(kv[j, :, 0:hd], q2, last, preferred_element_type=jnp.float32)
        bent = jnp.tanh(raw * (SCALE / CAP))
        expo = jnp.exp(CAP * bent)
        if c == 0:
            expo = jnp.where(row_at > col_at, expo, 0.0)
        if c == 5:
            expo = jnp.where(row_at <= col_at, expo, 0.0)
        if j < 5:
            expo = expo * jnp.where(s >= (1 if j > 0 else 2), 1.0, 0.0)
        d_probs = lax.dot_general(
            kv[j, :, hd : 2 * hd], do2, last, preferred_element_type=jnp.float32
        )
        e_buf[qt, c] = expo
        dp_buf[qt, c] = d_probs
        b_buf[qt, c] = bent
        shape = (hd // 8, 8, 2 * hd)
        return (
            jnp.sum(expo.reshape(shape), axis=0),
            jnp.sum((expo * d_probs).reshape(shape), axis=0),
        )

    def transpose_keys(j):
        kt[:, pl.ds(j * hd, hd)] = kv[j, :, 0:hd].astype(jnp.float32).T.astype(jnp.bfloat16)

    sums = []
    for qt in range(NX):
        q2, do2 = two_heads(qb, qt), two_heads(dout, qt)
        parts = [scores(qt, c, q2, do2) for c in range(5 - qt, 6)]
        sums.append((sum(p[0] for p in parts), sum(p[1] for p in parts)))
    for j in range(5, 9):
        transpose_keys(j)

    @pl.when(s > 0)
    def _():
        for k in range(NZ):
            near_copy(k, zs[k]).wait_recv()

    @pl.when(s > 1)
    def _():
        for k in range(NZ):
            far_copy(k, zs[k]).wait_recv()

    for j in range(5):
        transpose_keys(j)

    rest = []
    for qt in range(NX):
        q2, do2 = two_heads(qb, qt), two_heads(dout, qt)
        parts = [scores(qt, c, q2, do2) for c in range(0, 5 - qt)]
        norm = jnp.sum(sums[qt][0] + sum(p[0] for p in parts), axis=0, keepdims=True)
        inner = jnp.sum(sums[qt][1] + sum(p[1] for p in parts), axis=0, keepdims=True)
        inverse = 1.0 / norm
        rest.append((inverse, inner * inverse))

    def tile_grads(j):
        d_key = d_value = 0.0
        for qt in range(max(0, j - 5), min(NX, j + 1)):
            c = j - qt
            inverse, delta = rest[qt]
            probs = e_buf[qt, c] * inverse
            bent = b_buf[qt, c]
            d_raw = (
                probs * (dp_buf[qt, c] - delta) * (1.0 - bent * bent) * SCALE
            ).astype(jnp.bfloat16)
            dr_buf[qt, pl.ds(c * hd, hd), :] = d_raw
            d_key += jnp.dot(d_raw, two_heads(qb, qt), preferred_element_type=jnp.float32)
            d_value += jnp.dot(
                probs.astype(jnp.bfloat16), two_heads(dout, qt), preferred_element_type=jnp.float32
            )
        return d_key, d_value

    far_back = send_along(
        back_out.at[0], back_far, s_bf.at[0], r_bf.at[0], jnp.maximum(s - 2, 0)
    )
    near_back = [
        send_along(
            back_out.at[j], back_near.at[j - 1], s_bn.at[j - 1], r_bn.at[j - 1],
            jnp.maximum(s - 1, 0),
        )
        for j in range(1, 5)
    ]
    for j in range(5):
        d_key, d_value = tile_grads(j)
        back_out[j, :, 0:hd] = d_key.astype(jnp.bfloat16)
        back_out[j, :, hd : 2 * hd] = d_value.astype(jnp.bfloat16)
        if j == 0:
            pl.when(s > 1)(lambda: far_back.start())
        else:
            pl.when(s > 0)(lambda j=j: near_back[j - 1].start())
    for j in range(5, 9):
        d_key, d_value = tile_grads(j)
        acc[j - 5, :, 0:hd] = d_key
        acc[j - 5, :, hd : 2 * hd] = d_value
    for qt in range(NX):
        d_query = jnp.dot(
            kt[:, pl.ds(qt * hd, 6 * hd)], dr_buf[qt], preferred_element_type=jnp.float32
        )
        grads[qt, :, 0:hd] = d_query[:, 0:hd].T.astype(jnp.bfloat16)
        grads[qt, :, hd : 2 * hd] = d_query[:, hd : 2 * hd].T.astype(jnp.bfloat16)

    @pl.when(s < blocks - 2)
    def _():
        send_along(back_out.at[0], back_far, s_bf.at[0], r_bf.at[0], s).wait_recv()

    @pl.when(s < blocks - 1)
    def _():
        for i in range(NX):
            send_along(
                back_out.at[i + 1], back_near.at[i], s_bn.at[i], r_bn.at[i], s
            ).wait_recv()

    for i in range(NX):
        own = acc[i] + back_near[i].astype(jnp.float32)
        if i == NX - 1:
            own = own + back_far[...].astype(jnp.float32)
        grads[i, :, q_cols:] = own.astype(jnp.bfloat16)

    zs = zs[::-1]
    p = g
    tile = 512

    def row_ds(xr, h=None):
        if h is None:
            return pl.ds(pl.multiple_of(xr * rows, rows), rows)
        return pl.ds(pl.multiple_of(xr * rows + h * half, half), half)

    def compute(zr):
        lhs = grads[:, pl.ds(pl.multiple_of(zr * rows, rows), rows), :].reshape(NX * rows, -1)

        @pl.loop(0, width // tile)
        def _(j):
            at = pl.ds(pl.multiple_of(j * tile, tile), tile)
            p[zr, :, at] = jnp.dot(
                lhs, wt[:, at], preferred_element_type=jnp.float32
            ).astype(jnp.bfloat16)

    def way(zr):
        return jnp.where(zr > z, 1, 0)

    def nearer(zr):
        return tp_of(x, jnp.where(zr > z, z + 1, z - 1))

    def step1(k, zr, cols):
        for direction, to in ((0, xm), (1, xp)):
            sends.start(
                send_to(
                    p.at[zr, row_ds(xo, direction), cols],
                    got_opp.at[direction, zr, :, cols],
                    s1.at[direction, k],
                    r1.at[direction, k],
                    tp_of(to, z),
                )
            )

    def step2(k, zr, cols):
        for direction, to in ((0, xm), (1, xp)):
            land = got_opp.at[direction, zr, :, cols]
            send_to(land, land, s1.at[direction, k], r1.at[direction, k], tp_of(to, z)).wait_recv()
            at = row_ds(to, direction)
            p[zr, at, cols] = (
                p[zr, at, cols].astype(jnp.float32)
                + got_opp[direction, zr, :, cols].astype(jnp.float32)
            ).astype(jnp.bfloat16)
            sends.start(
                send_to(
                    p.at[zr, row_ds(to), cols],
                    got_x.at[direction, zr, :, cols],
                    s2.at[direction, k],
                    r2.at[direction, k],
                    tp_of(to, z),
                )
            )

    def x_sum(k, zr, cols):
        for direction, to in ((0, xm), (1, xp)):
            land = got_x.at[direction, zr, :, cols]
            send_to(land, land, s2.at[direction, k], r2.at[direction, k], tp_of(to, z)).wait_recv()
        return (
            p[zr, row_ds(x), cols].astype(jnp.float32)
            + got_x[0, zr, :, cols].astype(jnp.float32)
            + got_x[1, zr, :, cols].astype(jnp.float32)
        )

    def line_wait_b(d, zr):
        land = got_zb.at[d, zr]
        send_to(land, land, tzb.at[0], uzb.at[d, zr], tp_of(xp, z)).wait_recv()

    def line_wait_a(d, zr):
        land = got_za.at[d, zr]
        send_to(land, land, tza.at[0], uza.at[d, zr], tp_of(xp, z)).wait_recv()

    def step3(k, far):
        zr = zs[k]
        value = x_sum(k, zr, b_cols)
        if far:
            line_wait_b(way(zr), zr)
            value = value + got_zb[way(zr), zr].astype(jnp.float32)
        p[zr, row_ds(x), b_cols] = value.astype(jnp.bfloat16)
        sends.start(
            send_to(
                p.at[zr, row_ds(x), b_cols], got_zb.at[way(zr), zr], tzb.at[k],
                uzb.at[way(zr), zr], nearer(zr),
            )
        )

    def add_a(d, zr):
        line_wait_a(d, zr)
        p[zr, :, a_cols] = (
            p[zr, :, a_cols].astype(jnp.float32) + got_za[d, zr].astype(jnp.float32)
        ).astype(jnp.bfloat16)

    def line_a(k, far):
        zr = zs[k]
        if far:
            add_a(way(zr), zr)
        sends.start(
            send_to(
                p.at[zr, :, a_cols], got_za.at[way(zr), zr], tza.at[k],
                uza.at[way(zr), zr], nearer(zr),
            )
        )

    def finish(sources):
        total[:, b_cols] = x_sum(3, z, b_cols)
        for d in sources:
            line_wait_b(d, z)
            total[:, b_cols] = total[:, b_cols] + got_zb[d, z].astype(jnp.float32)
        total[:, a_cols] = x_sum(4, z, a_cols)
        values = tok[...].astype(jnp.float32)
        inv_rms = lax.rsqrt(jnp.mean(values * values, axis=1, keepdims=True) + EPS)
        upper = total[...] * gain[...]
        xhat = values * inv_rms
        out_ref[...] = (
            inv_rms * (upper - xhat * jnp.mean(upper * xhat, axis=1, keepdims=True))
        ).astype(jnp.bfloat16)
        sends.finish()

    sends = Sends()

    @pl.when(is_edge)
    def _():
        source = jnp.where(z == 0, 0, 1)
        compute(zs[0])
        line_a(0, False)
        step1(0, zs[0], b_cols)
        compute(zs[1])
        line_a(1, False)
        step1(1, zs[1], b_cols)
        compute(zs[2])
        compute(z)
        step2(0, zs[0], b_cols)
        step1(2, zs[2], b_cols)
        step2(1, zs[1], b_cols)
        step3(0, False)
        line_a(2, False)
        step1(3, z, b_cols)
        step2(2, zs[2], b_cols)
        step3(1, False)
        add_a(source, z)
        step1(4, z, a_cols)
        step2(3, z, b_cols)
        step2(4, z, a_cols)
        step3(2, False)
        finish([source])

    sends = Sends()

    @pl.when(jnp.logical_not(is_edge))
    def _():
        compute(zs[0])
        step1(0, zs[0], b_cols)
        compute(zs[1])
        step1(1, zs[1], b_cols)
        compute(zs[2])
        compute(z)
        step2(0, zs[0], b_cols)
        step1(2, zs[2], b_cols)
        line_a(0, True)
        step2(1, zs[1], b_cols)
        step1(3, z, b_cols)
        line_a(1, True)
        step2(2, zs[2], b_cols)
        line_a(2, True)
        step3(0, True)
        step2(3, z, b_cols)
        add_a(0, z)
        add_a(1, z)
        step1(4, z, a_cols)
        step3(2, True)
        step3(1, True)
        step2(4, z, a_cols)
        finish([0, 1])

    @pl.when(s > 0)
    def _():
        for copy in near_back:
            copy.wait_send()

    @pl.when(s > 1)
    def _():
        far_back.wait_send()

    @pl.when(s + 1 < blocks)
    def _():
        for k in range(NZ):
            near_copy(k, zs[NZ - 1 - k]).wait_send()

    @pl.when(s + 2 < blocks)
    def _():
        for k in range(NZ):
            far_copy(k, zs[NZ - 1 - k]).wait_send()


def on_device(tokens, norm_gain, query_weight, key_matrix, value_matrix, output_grad):
    rows, width = tokens.shape
    q_cols, k_cols = query_weight.shape[1], key_matrix.shape[1]
    cols = q_cols + 2 * k_cols
    a_width = A_TILES * 128
    hd = HEAD_SIZE
    any_space = pl.BlockSpec(memory_space=pl.ANY)
    dma = pltpu.SemaphoreType.DMA
    low, full = jnp.bfloat16, jnp.float32

    def vmem(kind, *shape):
        return pltpu.VMEM(shape, kind)

    return pl.pallas_call(
        whole,
        out_shape=jax.ShapeDtypeStruct((rows, width), low),
        in_specs=[any_space] * 6,
        out_specs=pl.BlockSpec(memory_space=pltpu.VMEM),
        scratch_shapes=[
            vmem(low, rows, width),
            vmem(full, 1, width),
            vmem(low, width, cols),
            vmem(low, cols, width),
            vmem(low, NZ, NX * rows, width),
            vmem(low, NX, hd, q_cols),
            vmem(low, NX, hd, q_cols),
            vmem(low, 9, hd, 2 * k_cols),
            vmem(low, hd, 9 * hd),
            vmem(full, NX, 6, hd, 2 * hd),
            vmem(full, NX, 6, hd, 2 * hd),
            vmem(full, NX, 6, hd, 2 * hd),
            vmem(low, NX, 6 * hd, 2 * hd),
            vmem(full, NX, hd, 2 * k_cols),
            vmem(low, 5, hd, 2 * k_cols),
            vmem(low, NX, hd, 2 * k_cols),
            vmem(low, hd, 2 * k_cols),
            vmem(low, NX, hd, cols),
            vmem(full, rows, width),
            vmem(low, 2, NZ, rows // 2, width),
            vmem(low, 2, NZ, rows, width),
            vmem(low, 2, NZ, NX * rows, a_width),
            vmem(low, 2, NZ, rows, width - a_width),
            dma((6,)),
            dma((2, NZ + 1, 3)),
            dma((2, NZ, NX, 2)),
            dma((2, NZ)),
            dma((NZ,)),
            dma((2, NZ, NX)),
            dma((NZ, NX)),
            dma((NZ,)),
            dma((NZ,)),
            dma((NZ,)),
            dma((NZ,)),
            dma((NX,)),
            dma((NX,)),
            dma((1,)),
            dma((1,)),
            dma((2, NZ + 1)),
            dma((2, NZ + 1)),
            dma((2, NZ + 1)),
            dma((2, NZ + 1)),
            dma((NZ,)),
            dma((2, NZ)),
            dma((NZ,)),
            dma((2, NZ)),
        ],
        compiler_params=pltpu.CompilerParams(
            collective_id=0, has_side_effects=True, vmem_limit_bytes=62 * 1024 * 1024
        ),
    )(
        tokens,
        norm_gain.reshape(1, -1),
        output_grad.reshape(NX, hd, q_cols),
        query_weight,
        key_matrix,
        value_matrix,
    )


def solution(mesh):
    tp, both = "tp", ("seq", "tp")
    in_specs = (P(both, None), P(), P(None, tp), P(None, tp), P(None, tp), P("seq", tp))
    return jax.shard_map(
        on_device, mesh=mesh, in_specs=in_specs, out_specs=P(both, None), check_vma=False
    )
```

```python
import jax
import jax.numpy as jnp
from jax import lax
from jax.experimental import pallas as pl
from jax.experimental.pallas import tpu as pltpu
from jax.sharding import PartitionSpec as P

HEAD_SIZE = 128
WINDOW = 640
SCALE = 1.0 / 12.0
CAP = 50.0
EPS = 1e-06
MESH = pl.DeviceIdType.MESH
NX = 4
NZ = 4
A_TILES = 5
B_TILES = 8
TURN = 512
TURNS = 9


def place():
    t = lax.axis_index("tp")
    return t // NZ, t % NZ


def near_to_far(z):
    def high(q):
        return (q, 5 - q, jnp.int32(1), jnp.int32(0))

    up = high(z)
    low = high(3 - z)
    return [jnp.where(z >= 2, u, 3 - v) for u, v in zip(up, low)]


def send_to(src, dst, send_sem, recv_sem, tp):
    return pltpu.make_async_remote_copy(
        src_ref=src,
        dst_ref=dst,
        send_sem=send_sem,
        recv_sem=recv_sem,
        device_id={"tp": tp},
        device_id_type=MESH,
    )


def tp_of(x, z):
    return x * NZ + z


def send_along(src, dst, send_sem, recv_sem, seq):
    return pltpu.make_async_remote_copy(
        src_ref=src,
        dst_ref=dst,
        send_sem=send_sem,
        recv_sem=recv_sem,
        device_id={"seq": seq},
        device_id_type=MESH,
    )


def greet_partners(x, z, s, blocks):
    barrier = pltpu.get_barrier_semaphore()

    def greet(device):
        pl.semaphore_signal(barrier, inc=1, device_id=device, device_id_type=MESH)

    greet({"tp": tp_of((x + 1) % NX, z)})
    greet({"tp": tp_of((x + 3) % NX, z)})
    pl.when(z > 0)(lambda: greet({"tp": tp_of(x, z - 1)}))
    pl.when(z < NZ - 1)(lambda: greet({"tp": tp_of(x, z + 1)}))
    count = jnp.where((z == 0) | (z == NZ - 1), 3, 4)
    for step in (-2, -1, 1, 2):
        there = (s + step >= 0) & (s + step < blocks)
        pl.when(there)(lambda step=step: greet({"seq": s + step}))
        count = count + jnp.where(there, 1, 0)
    return barrier, count


class Sends:
    def __init__(self):
        self.started = []

    def start(self, copy, when=None):
        self.started.append((copy, when))
        if when is None:
            copy.start()
        else:
            pl.when(when)(lambda: copy.start())

    def finish(self):
        for copy, when in self.started:
            if when is None:
                copy.wait_send()
            else:
                pl.when(when)(lambda copy=copy: copy.wait_send())


def whole(
    tokens_ref, gain_ref, grad_ref, wq_ref, wk_ref, wv_ref, out_ref,
    tok, gain, w, wt, g, dout, qb, kv, kt, e_buf, dp_buf, b_buf, dr_buf, acc,
    back_out, back_near, back_far, grads, total, got_opp, got_x, got_za, got_zb,
    load_sem, sx, rx, szb, rzb, sza, rza, s_near, r_near, s_far, r_far,
    s_bn, r_bn, s_bf, r_bf, s1, r1, s2, r2, tza, uza, tzb, uzb,
):
    x, z = place()
    s = lax.axis_index("seq")
    blocks = lax.axis_size("seq")
    rows, width = tok.shape
    half = rows // 2
    a_width = A_TILES * 128
    a_cols = pl.ds(0, a_width)
    b_cols = pl.ds(a_width, width - a_width)
    xp, xm, xo = (x + 1) % NX, (x + 3) % NX, (x + 2) % NX
    zs = near_to_far(z)
    q_cols, k_cols = wq_ref.shape[1], wk_ref.shape[1]
    barrier, partners = greet_partners(x, z, s, blocks)
    loads = [
        pltpu.make_async_copy(tokens_ref, tok, load_sem.at[0]),
        pltpu.make_async_copy(gain_ref, gain, load_sem.at[1]),
        pltpu.make_async_copy(wq_ref, w.at[:, pl.ds(0, q_cols)], load_sem.at[2]),
        pltpu.make_async_copy(wk_ref, w.at[:, pl.ds(q_cols, k_cols)], load_sem.at[3]),
        pltpu.make_async_copy(wv_ref, w.at[:, pl.ds(q_cols + k_cols, k_cols)], load_sem.at[4]),
        pltpu.make_async_copy(grad_ref, dout, load_sem.at[5]),
    ]
    for load in loads:
        load.start()
    loads[0].wait()
    loads[1].wait()

    def gain_row():
        return jnp.concatenate([gain[i : i + 1, :] for i in range(gain.shape[0])], axis=1)

    values = tok[...].astype(jnp.float32)
    inv_rms = lax.rsqrt(jnp.mean(values * values, axis=1, keepdims=True) + EPS)
    g[z, pl.ds(x * rows, rows), :] = (values * inv_rms * gain_row()).astype(jnp.bfloat16)
    pl.semaphore_wait(barrier, partners)
    sends = Sends()

    def part(zr, xr, h, cols):
        if h is None:
            return g.at[zr, pl.ds(pl.multiple_of(xr * rows, rows), rows), cols]
        return g.at[zr, pl.ds(pl.multiple_of(xr * rows + h * half, half), half), cols]

    def x_send(k, zr, xr, h, cols, to, direction, slot):
        piece = part(zr, xr, h, cols)
        p = 1 if k == NZ else 0
        sends.start(
            send_to(piece, piece, sx.at[direction, k, slot], rx.at[p, zr, xr, h], tp_of(to, z))
        )

    def x_wait(k, zr, xr, h, cols):
        piece = part(zr, xr, h, cols)
        p = 1 if k == NZ else 0
        send_to(piece, piece, sx.at[0, k, 0], rx.at[p, zr, xr, h], tp_of(xp, z)).wait_recv()

    def x_own(k, zr, cols, first):
        h_right, h_left = (0, 1) if first else (1, 0)
        slot = 0 if first else 1
        x_send(k, zr, x, h_right, cols, xp, 0, slot)
        x_send(k, zr, x, h_left, cols, xm, 1, slot)

    def x_forward(k, zr, cols):
        x_wait(k, zr, xm, 0, cols)
        x_send(k, zr, xm, 0, cols, xp, 0, 2)
        x_wait(k, zr, xp, 1, cols)
        x_send(k, zr, xp, 1, cols, xm, 1, 2)

    def x_rest_near(k, zr, cols):
        x_wait(k, zr, xm, 1, cols)
        x_wait(k, zr, xp, 0, cols)

    def x_rest_opposite(k, zr, cols):
        x_wait(k, zr, xo, 0, cols)
        x_wait(k, zr, xo, 1, cols)

    def x_rest(k, zr, cols):
        x_rest_near(k, zr, cols)
        x_rest_opposite(k, zr, cols)

    def z_send_b(k, zr, way, to):
        piece = part(zr, x, None, b_cols)
        sends.start(send_to(piece, piece, szb.at[way, k], rzb.at[zr], tp_of(x, to)))

    def z_send_a(k, zr, xr, way, to):
        piece = part(zr, xr, None, a_cols)
        sends.start(
            send_to(piece, piece, sza.at[way, k, xr], rza.at[zr, xr], tp_of(x, to))
        )

    def z_wait_b(k):
        piece = part(zs[k], x, None, b_cols)
        send_to(piece, piece, szb.at[0, 0], rzb.at[zs[k]], tp_of(xp, z)).wait_recv()

    def z_wait_a(k):
        for i in range(NX):
            piece = part(zs[k], i, None, a_cols)
            send_to(piece, piece, sza.at[0, 0, i], rza.at[zs[k], i], tp_of(xp, z)).wait_recv()

    def turn(c):
        at = pl.ds(c * TURN, TURN)
        wt[:, at] = w[at, :].T

    def slab(first, count, zr):
        return kv.at[pl.ds(first, count), pl.ds(pl.multiple_of(zr * rows, rows), rows), :]

    def near_copy(k, zr):
        return send_along(
            slab(5, 4, zr), slab(1, 4, zr), s_near.at[k], r_near.at[k],
            jnp.minimum(s + 1, blocks - 1),
        )

    def far_copy(k, zr):
        return send_along(
            slab(8, 1, zr), slab(0, 1, zr), s_far.at[k], r_far.at[k],
            jnp.minimum(s + 2, blocks - 1),
        )

    def project(k):
        zr = zs[k]
        out = jnp.dot(g[zr], w[...], preferred_element_type=jnp.float32).astype(jnp.bfloat16)
        at = pl.ds(pl.multiple_of(zr * rows, rows), rows)
        for i in range(NX):
            kv[5 + i, at, :] = out[i * rows : (i + 1) * rows, q_cols:]
            qb[i, at, :] = out[i * rows : (i + 1) * rows, :q_cols]
        pl.when(s + 1 < blocks)(lambda: near_copy(k, zr).start())
        pl.when(s + 2 < blocks)(lambda: far_copy(k, zr).start())

    is_edge = (z == 0) | (z == NZ - 1)

    def start_gather(neighbours):
        x_own(NZ, z, a_cols, True)
        x_own(NZ, z, a_cols, False)
        for way, to in neighbours:
            z_send_b(0, z, way, to)
        x_own(0, z, b_cols, True)
        x_forward(NZ, z, a_cols)
        x_own(0, z, b_cols, False)
        way, to = neighbours[0]
        x_rest_near(NZ, z, a_cols)
        for i in (x, xm, xp):
            z_send_a(0, z, i, way, to)
        for load in loads[2:]:
            load.wait()
        clear_edges()
        turn(0)
        x_rest_opposite(NZ, z, a_cols)
        z_send_a(0, z, xo, way, to)
        x_forward(0, z, b_cols)

    def clear_edges():
        @pl.when(s == 0)
        def _():
            kv[0:5] = jnp.zeros_like(kv[0:5])

        @pl.when(s == 1)
        def _():
            kv[0] = jnp.zeros_like(kv[0])

        @pl.when(s == blocks - 1)
        def _():
            back_near[...] = jnp.zeros_like(back_near)

        @pl.when(s >= blocks - 2)
        def _():
            back_far[...] = jnp.zeros_like(back_far)

    @pl.when(is_edge)
    def _():
        start_gather([(0, jnp.where(z == 0, 1, NZ - 2))])
        z_wait_b(1)
        x_own(1, zs[1], b_cols, True)
        x_own(1, zs[1], b_cols, False)
        for c in range(1, 5):
            turn(c)
        x_rest(0, z, b_cols)
        project(0)
        x_forward(1, zs[1], b_cols)
        turn(5)
        z_wait_b(2)
        x_own(2, zs[2], b_cols, True)
        x_own(2, zs[2], b_cols, False)
        z_wait_a(1)
        x_rest(1, zs[1], b_cols)
        project(1)
        x_forward(2, zs[2], b_cols)
        z_wait_b(3)
        x_own(3, zs[3], b_cols, True)
        x_own(3, zs[3], b_cols, False)
        for c in range(6, TURNS):
            turn(c)
        z_wait_a(2)
        x_rest(2, zs[2], b_cols)
        project(2)
        x_forward(3, zs[3], b_cols)
        z_wait_a(3)
        x_rest(3, zs[3], b_cols)
        project(3)
        sends.finish()

    sends = Sends()

    @pl.when(jnp.logical_not(is_edge))
    def _():
        outer = jnp.where(z == 1, 0, NZ - 1)
        inner = NZ - 1 - z
        start_gather([(0, outer), (1, inner)])
        z_wait_b(1)
        z_send_b(1, zs[1], 1, inner)
        for i in (x, xm, xp, xo):
            z_send_a(0, z, i, 1, inner)
        x_own(1, zs[1], b_cols, True)
        x_own(1, zs[1], b_cols, False)
        z_wait_b(2)
        z_send_b(2, zs[2], 0, outer)
        x_own(2, zs[2], b_cols, True)
        x_own(2, zs[2], b_cols, False)
        for c in range(1, 4):
            turn(c)
        x_rest(0, z, b_cols)
        project(0)
        z_wait_a(1)
        for i in range(NX):
            z_send_a(1, zs[1], i, 1, inner)
        z_wait_b(3)
        z_send_b(3, zs[3], 0, outer)
        x_forward(1, zs[1], b_cols)
        x_own(3, zs[3], b_cols, True)
        x_own(3, zs[3], b_cols, False)
        for c in range(4, 7):
            turn(c)
        x_forward(2, zs[2], b_cols)
        z_wait_a(2)
        for i in range(NX):
            z_send_a(2, zs[2], i, 0, outer)
        for c in range(7, TURNS):
            turn(c)
        x_rest(1, zs[1], b_cols)
        project(1)
        z_wait_a(3)
        for i in range(NX):
            z_send_a(3, zs[3], i, 0, outer)
        x_forward(3, zs[3], b_cols)
        x_rest(2, zs[2], b_cols)
        project(2)
        x_rest(3, zs[3], b_cols)
        project(3)
        sends.finish()

    hd = HEAD_SIZE
    last = (((1,), (1,)), ((), ()))

    def two_heads(ref, qt):
        return jnp.concatenate([ref[qt, :, 0:hd], ref[qt, :, hd : 2 * hd]], axis=0)

    row_at = lax.broadcasted_iota(jnp.int32, (hd, 2 * hd), 0)
    col_at = lax.broadcasted_iota(jnp.int32, (hd, 2 * hd), 1) % hd

    def scores(qt, c, q2, do2):
        j = qt + c
        raw = lax.dot_general(kv[j, :, 0:hd], q2, last, preferred_element_type=jnp.float32)
        bent = jnp.tanh(raw * (SCALE / CAP))
        expo = jnp.exp(CAP * bent)
        if c == 0:
            expo = jnp.where(row_at > col_at, expo, 0.0)
        if c == 5:
            expo = jnp.where(row_at <= col_at, expo, 0.0)
        if j < 5:
            expo = expo * jnp.where(s >= (1 if j > 0 else 2), 1.0, 0.0)
        d_probs = lax.dot_general(
            kv[j, :, hd : 2 * hd], do2, last, preferred_element_type=jnp.float32
        )
        e_buf[qt, c] = expo
        dp_buf[qt, c] = d_probs
        b_buf[qt, c] = bent
        shape = (hd // 8, 8, 2 * hd)
        return (
            jnp.sum(expo.reshape(shape), axis=0),
            jnp.sum((expo * d_probs).reshape(shape), axis=0),
        )

    def transpose_keys(j):
        kt[:, pl.ds(j * hd, hd)] = kv[j, :, 0:hd].astype(jnp.float32).T.astype(jnp.bfloat16)

    sums = []
    for qt in range(NX):
        q2, do2 = two_heads(qb, qt), two_heads(dout, qt)
        parts = [scores(qt, c, q2, do2) for c in range(5 - qt, 6)]
        sums.append((sum(p[0] for p in parts), sum(p[1] for p in parts)))
    for j in range(5, 9):
        transpose_keys(j)

    @pl.when(s > 0)
    def _():
        for k in range(NZ):
            near_copy(k, zs[k]).wait_recv()

    @pl.when(s > 1)
    def _():
        for k in range(NZ):
            far_copy(k, zs[k]).wait_recv()

    for j in range(5):
        transpose_keys(j)

    rest = []
    for qt in range(NX):
        q2, do2 = two_heads(qb, qt), two_heads(dout, qt)
        parts = [scores(qt, c, q2, do2) for c in range(0, 5 - qt)]
        norm = jnp.sum(sums[qt][0] + sum(p[0] for p in parts), axis=0, keepdims=True)
        inner = jnp.sum(sums[qt][1] + sum(p[1] for p in parts), axis=0, keepdims=True)
        inverse = 1.0 / norm
        rest.append((inverse, inner * inverse))

    def tile_grads(j):
        d_key = d_value = 0.0
        for qt in range(max(0, j - 5), min(NX, j + 1)):
            c = j - qt
            inverse, delta = rest[qt]
            probs = e_buf[qt, c] * inverse
            bent = b_buf[qt, c]
            d_raw = (
                probs * (dp_buf[qt, c] - delta) * (1.0 - bent * bent) * SCALE
            ).astype(jnp.bfloat16)
            dr_buf[qt, pl.ds(c * hd, hd), :] = d_raw
            d_key += jnp.dot(d_raw, two_heads(qb, qt), preferred_element_type=jnp.float32)
            d_value += jnp.dot(
                probs.astype(jnp.bfloat16), two_heads(dout, qt), preferred_element_type=jnp.float32
            )
        return d_key, d_value

    far_back = send_along(
        back_out.at[0], back_far, s_bf.at[0], r_bf.at[0], jnp.maximum(s - 2, 0)
    )
    near_back = [
        send_along(
            back_out.at[j], back_near.at[j - 1], s_bn.at[j - 1], r_bn.at[j - 1],
            jnp.maximum(s - 1, 0),
        )
        for j in range(1, 5)
    ]
    for j in range(5):
        d_key, d_value = tile_grads(j)
        back_out[j, :, 0:hd] = d_key.astype(jnp.bfloat16)
        back_out[j, :, hd : 2 * hd] = d_value.astype(jnp.bfloat16)
        if j == 0:
            pl.when(s > 1)(lambda: far_back.start())
        else:
            pl.when(s > 0)(lambda j=j: near_back[j - 1].start())
    for j in range(5, 9):
        d_key, d_value = tile_grads(j)
        acc[j - 5, :, 0:hd] = d_key
        acc[j - 5, :, hd : 2 * hd] = d_value
    for qt in range(NX):
        d_query = jnp.dot(
            kt[:, pl.ds(qt * hd, 6 * hd)], dr_buf[qt], preferred_element_type=jnp.float32
        )
        grads[qt, :, 0:hd] = d_query[:, 0:hd].T.astype(jnp.bfloat16)
        grads[qt, :, hd : 2 * hd] = d_query[:, hd : 2 * hd].T.astype(jnp.bfloat16)

    @pl.when(s < blocks - 2)
    def _():
        send_along(back_out.at[0], back_far, s_bf.at[0], r_bf.at[0], s).wait_recv()

    @pl.when(s < blocks - 1)
    def _():
        for i in range(NX):
            send_along(
                back_out.at[i + 1], back_near.at[i], s_bn.at[i], r_bn.at[i], s
            ).wait_recv()

    for i in range(NX):
        own = acc[i] + back_near[i].astype(jnp.float32)
        if i == NX - 1:
            own = own + back_far[...].astype(jnp.float32)
        grads[i, :, q_cols:] = own.astype(jnp.bfloat16)

    zs = zs[::-1]
    p = g
    tile = 768
    a_width = B_TILES * 128
    a_cols = pl.ds(0, a_width)
    b_cols = pl.ds(a_width, width - a_width)

    def row_ds(xr, h=None):
        if h is None:
            return pl.ds(pl.multiple_of(xr * rows, rows), rows)
        return pl.ds(pl.multiple_of(xr * rows + h * half, half), half)

    def compute(zr):
        lhs = grads[:, pl.ds(pl.multiple_of(zr * rows, rows), rows), :].reshape(NX * rows, -1)

        for j in range(width // tile):
            at = pl.ds(j * tile, tile)
            p[zr, :, at] = jnp.dot(
                lhs, wt[:, at], preferred_element_type=jnp.float32
            ).astype(jnp.bfloat16)

    def way(zr):
        return jnp.where(zr > z, 1, 0)

    def nearer(zr):
        return tp_of(x, jnp.where(zr > z, z + 1, z - 1))

    def step1(k, zr, cols):
        for direction, to in ((0, xm), (1, xp)):
            sends.start(
                send_to(
                    p.at[zr, row_ds(xo, direction), cols],
                    got_opp.at[direction, zr, :, cols],
                    s1.at[direction, k],
                    r1.at[direction, k],
                    tp_of(to, z),
                )
            )

    def step2(k, zr, cols):
        for direction, to in ((0, xm), (1, xp)):
            land = got_opp.at[direction, zr, :, cols]
            send_to(land, land, s1.at[direction, k], r1.at[direction, k], tp_of(to, z)).wait_recv()
            at = row_ds(to, direction)
            p[zr, at, cols] = (
                p[zr, at, cols].astype(jnp.float32)
                + got_opp[direction, zr, :, cols].astype(jnp.float32)
            ).astype(jnp.bfloat16)
            sends.start(
                send_to(
                    p.at[zr, row_ds(to), cols],
                    got_x.at[direction, zr, :, cols],
                    s2.at[direction, k],
                    r2.at[direction, k],
                    tp_of(to, z),
                )
            )

    def x_sum(k, zr, cols):
        for direction, to in ((0, xm), (1, xp)):
            land = got_x.at[direction, zr, :, cols]
            send_to(land, land, s2.at[direction, k], r2.at[direction, k], tp_of(to, z)).wait_recv()
        return (
            p[zr, row_ds(x), cols].astype(jnp.float32)
            + got_x[0, zr, :, cols].astype(jnp.float32)
            + got_x[1, zr, :, cols].astype(jnp.float32)
        )

    def line_wait_b(d, zr):
        land = got_zb.at[d, zr]
        send_to(land, land, tzb.at[0], uzb.at[d, zr], tp_of(xp, z)).wait_recv()

    def line_wait_a(d, zr):
        land = got_za.at[d, zr]
        send_to(land, land, tza.at[0], uza.at[d, zr], tp_of(xp, z)).wait_recv()

    def step3(k, far):
        zr = zs[k]
        value = x_sum(k, zr, b_cols)
        if far:
            line_wait_b(way(zr), zr)
            value = value + got_zb[way(zr), zr].astype(jnp.float32)
        p[zr, row_ds(x), b_cols] = value.astype(jnp.bfloat16)
        sends.start(
            send_to(
                p.at[zr, row_ds(x), b_cols], got_zb.at[way(zr), zr], tzb.at[k],
                uzb.at[way(zr), zr], nearer(zr),
            )
        )

    def add_a(d, zr):
        line_wait_a(d, zr)
        p[zr, :, a_cols] = (
            p[zr, :, a_cols].astype(jnp.float32) + got_za[d, zr].astype(jnp.float32)
        ).astype(jnp.bfloat16)

    def line_a(k, far, when=None):
        zr = zs[k]
        if far:
            add_a(way(zr), zr)
        sends.start(
            send_to(
                p.at[zr, :, a_cols], got_za.at[way(zr), zr], tza.at[k],
                uza.at[way(zr), zr], nearer(zr),
            ),
            when,
        )

    def finish(sources):
        total[:, b_cols] = x_sum(3, z, b_cols)
        for d in sources:
            line_wait_b(d, z)
            total[:, b_cols] = total[:, b_cols] + got_zb[d, z].astype(jnp.float32)
        total[:, a_cols] = x_sum(4, z, a_cols)
        values = tok[...].astype(jnp.float32)
        inv_rms = lax.rsqrt(jnp.mean(values * values, axis=1, keepdims=True) + EPS)
        upper = total[...] * gain_row()
        xhat = values * inv_rms
        out_ref[...] = (
            inv_rms * (upper - xhat * jnp.mean(upper * xhat, axis=1, keepdims=True))
        ).astype(jnp.bfloat16)
        sends.finish()

    sends = Sends()
    compute(zs[0])
    step1(0, zs[0], b_cols)
    line_a(0, False, is_edge)
    compute(zs[1])
    step1(1, zs[1], b_cols)
    line_a(1, False, is_edge)
    compute(zs[2])
    compute(z)
    opening, sends = sends, Sends()

    @pl.when(is_edge)
    def _():
        source = jnp.where(z == 0, 0, 1)
        step2(0, zs[0], b_cols)
        step1(2, zs[2], b_cols)
        step2(1, zs[1], b_cols)
        step3(0, False)
        line_a(2, False)
        step1(3, z, b_cols)
        step2(2, zs[2], b_cols)
        step3(1, False)
        add_a(source, z)
        step1(4, z, a_cols)
        step2(3, z, b_cols)
        step2(4, z, a_cols)
        step3(2, False)
        finish([source])

    sends = Sends()

    @pl.when(jnp.logical_not(is_edge))
    def _():
        step2(0, zs[0], b_cols)
        step1(2, zs[2], b_cols)
        line_a(0, True)
        step2(1, zs[1], b_cols)
        step1(3, z, b_cols)
        line_a(1, True)
        step2(2, zs[2], b_cols)
        line_a(2, True)
        step3(0, True)
        step2(3, z, b_cols)
        add_a(0, z)
        add_a(1, z)
        step1(4, z, a_cols)
        step3(2, True)
        step3(1, True)
        step2(4, z, a_cols)
        finish([0, 1])

    opening.finish()

    @pl.when(s > 0)
    def _():
        for copy in near_back:
            copy.wait_send()

    @pl.when(s > 1)
    def _():
        far_back.wait_send()

    @pl.when(s + 1 < blocks)
    def _():
        for k in range(NZ):
            near_copy(k, zs[NZ - 1 - k]).wait_send()

    @pl.when(s + 2 < blocks)
    def _():
        for k in range(NZ):
            far_copy(k, zs[NZ - 1 - k]).wait_send()


def on_device(tokens, norm_gain, query_weight, key_matrix, value_matrix, output_grad):
    rows, width = tokens.shape
    q_cols, k_cols = query_weight.shape[1], key_matrix.shape[1]
    cols = q_cols + 2 * k_cols
    a_width = B_TILES * 128
    hd = HEAD_SIZE
    any_space = pl.BlockSpec(memory_space=pltpu.HBM)
    dma = pltpu.SemaphoreType.DMA
    low, full = jnp.bfloat16, jnp.float32

    def vmem(kind, *shape):
        return pltpu.VMEM(shape, kind)

    return pl.pallas_call(
        whole,
        out_shape=jax.ShapeDtypeStruct((rows, width), low),
        in_specs=[any_space] * 6,
        out_specs=pl.BlockSpec(memory_space=pltpu.VMEM),
        scratch_shapes=[
            vmem(low, rows, width),
            vmem(full, width // 128, 128),
            vmem(low, width, cols),
            vmem(low, cols, width),
            vmem(low, NZ, NX * rows, width),
            vmem(low, NX, hd, q_cols),
            vmem(low, NX, hd, q_cols),
            vmem(low, 9, hd, 2 * k_cols),
            vmem(low, hd, 9 * hd),
            vmem(full, NX, 6, hd, 2 * hd),
            vmem(full, NX, 6, hd, 2 * hd),
            vmem(full, NX, 6, hd, 2 * hd),
            vmem(low, NX, 6 * hd, 2 * hd),
            vmem(full, NX, hd, 2 * k_cols),
            vmem(low, 5, hd, 2 * k_cols),
            vmem(low, NX, hd, 2 * k_cols),
            vmem(low, hd, 2 * k_cols),
            vmem(low, NX, hd, cols),
            vmem(full, rows, width),
            vmem(low, 2, NZ, rows // 2, width),
            vmem(low, 2, NZ, rows, width),
            vmem(low, 2, NZ, NX * rows, a_width),
            vmem(low, 2, NZ, rows, width - a_width),
            dma((6,)),
            dma((2, NZ + 1, 3)),
            dma((2, NZ, NX, 2)),
            dma((2, NZ)),
            dma((NZ,)),
            dma((2, NZ, NX)),
            dma((NZ, NX)),
            dma((NZ,)),
            dma((NZ,)),
            dma((NZ,)),
            dma((NZ,)),
            dma((NX,)),
            dma((NX,)),
            dma((1,)),
            dma((1,)),
            dma((2, NZ + 1)),
            dma((2, NZ + 1)),
            dma((2, NZ + 1)),
            dma((2, NZ + 1)),
            dma((NZ,)),
            dma((2, NZ)),
            dma((NZ,)),
            dma((2, NZ)),
        ],
        compiler_params=pltpu.CompilerParams(
            collective_id=0, has_side_effects=True, vmem_limit_bytes=62 * 1024 * 1024
        ),
    )(
        tokens,
        norm_gain.reshape(-1, 128),
        output_grad.reshape(NX, hd, q_cols),
        query_weight,
        key_matrix,
        value_matrix,
    )


def solution(mesh):
    tp, both = "tp", ("seq", "tp")
    in_specs = (P(both, None), P(), P(None, tp), P(None, tp), P(None, tp), P("seq", tp))
    return jax.shard_map(
        on_device, mesh=mesh, in_specs=in_specs, out_specs=P(both, None), check_vma=False
    )
```

```python
import jax
import jax.numpy as jnp
from jax import lax
from jax.experimental import pallas as pl
from jax.experimental.pallas import tpu as pltpu
from jax.sharding import PartitionSpec as P

HEAD_SIZE = 128
WINDOW = 640
SCALE = 1.0 / 12.0
CAP = 50.0
EPS = 1e-06
MESH = pl.DeviceIdType.MESH
NX = 4
NZ = 4
A_TILES = 5
B_TILES = 8
TURN = 512
TURNS = 9


def place():
    t = lax.axis_index("tp")
    return t // NZ, t % NZ


def near_to_far(z):
    def high(q):
        return (q, 5 - q, jnp.int32(1), jnp.int32(0))

    up = high(z)
    low = high(3 - z)
    return [jnp.where(z >= 2, u, 3 - v) for u, v in zip(up, low)]


def send_to(src, dst, send_sem, recv_sem, tp):
    return pltpu.make_async_remote_copy(
        src_ref=src,
        dst_ref=dst,
        send_sem=send_sem,
        recv_sem=recv_sem,
        device_id={"tp": tp},
        device_id_type=MESH,
    )


def tp_of(x, z):
    return x * NZ + z


def send_along(src, dst, send_sem, recv_sem, seq):
    return pltpu.make_async_remote_copy(
        src_ref=src,
        dst_ref=dst,
        send_sem=send_sem,
        recv_sem=recv_sem,
        device_id={"seq": seq},
        device_id_type=MESH,
    )


def greet(device):
    barrier = pltpu.get_barrier_semaphore()
    pl.semaphore_signal(barrier, inc=1, device_id=device, device_id_type=MESH)


def meet(x, z, s, blocks):
    barrier = pltpu.get_barrier_semaphore()
    early = (s // 2) % 2 == 0
    greet({"tp": tp_of((x + 1) % NX, z)})
    greet({"tp": tp_of((x + 3) % NX, z)})
    pl.when(z > 0)(lambda: greet({"tp": tp_of(x, z - 1)}))
    pl.when(z < NZ - 1)(lambda: greet({"tp": tp_of(x, z + 1)}))
    greet({"seq": s + 1 - 2 * (s % 2)})
    near = jnp.where((z == 0) | (z == NZ - 1), 4, 5)
    others = [s - 2, s + 2, s - 1 + 2 * (s % 2)]
    there = [(o >= 0) & (o < blocks) for o in others]
    far = sum(jnp.where(t, 1, 0) for t in there)

    def first():
        pl.semaphore_wait(barrier, near + jnp.where(early, 0, far))
        for o, t in zip(others, there):
            pl.when(t)(lambda o=o: greet({"seq": o}))

    def second():
        pl.when(early)(lambda: pl.semaphore_wait(barrier, far))

    return first, second


class Sends:
    def __init__(self):
        self.started = []

    def start(self, copy, when=None):
        self.started.append((copy, when))
        if when is None:
            copy.start()
        else:
            pl.when(when)(lambda: copy.start())

    def finish(self):
        for copy, when in self.started:
            if when is None:
                copy.wait_send()
            else:
                pl.when(when)(lambda copy=copy: copy.wait_send())


def whole(
    tokens_ref, gain_ref, grad_ref, wq_ref, wk_ref, wv_ref, out_ref,
    tok, gain, w, wt, g, dout, qb, kv, kt, e_buf, dp_buf, b_buf, dr_buf, acc,
    back_out, back_near, back_far, grads, total, got_opp, got_x, got_za, got_zb,
    load_sem, sx, rx, szb, rzb, sza, rza, s_near, r_near, s_far, r_far,
    s_bn, r_bn, s_bf, r_bf, s1, r1, s2, r2, tza, uza, tzb, uzb,
):
    x, z = place()
    s = lax.axis_index("seq")
    blocks = lax.axis_size("seq")
    rows, width = tok.shape
    half = rows // 2
    a_width = A_TILES * 128
    a_cols = pl.ds(0, a_width)
    b_cols = pl.ds(a_width, width - a_width)
    xp, xm, xo = (x + 1) % NX, (x + 3) % NX, (x + 2) % NX
    zs = near_to_far(z)
    q_cols, k_cols = wq_ref.shape[1], wk_ref.shape[1]
    meet_first, meet_second = meet(x, z, s, blocks)
    loads = [
        pltpu.make_async_copy(tokens_ref, tok, load_sem.at[0]),
        pltpu.make_async_copy(gain_ref, gain, load_sem.at[1]),
        pltpu.make_async_copy(wq_ref, w.at[:, pl.ds(0, q_cols)], load_sem.at[2]),
        pltpu.make_async_copy(wk_ref, w.at[:, pl.ds(q_cols, k_cols)], load_sem.at[3]),
        pltpu.make_async_copy(wv_ref, w.at[:, pl.ds(q_cols + k_cols, k_cols)], load_sem.at[4]),
        pltpu.make_async_copy(grad_ref, dout, load_sem.at[5]),
    ]
    for load in loads:
        load.start()
    loads[0].wait()
    loads[1].wait()

    def gain_row():
        return jnp.concatenate([gain[i : i + 1, :] for i in range(gain.shape[0])], axis=1)

    values = tok[...].astype(jnp.float32)
    inv_rms = lax.rsqrt(jnp.mean(values * values, axis=1, keepdims=True) + EPS)
    g[z, pl.ds(x * rows, rows), :] = (values * inv_rms * gain_row()).astype(jnp.bfloat16)
    meet_first()
    sends = Sends()

    def part(zr, xr, h, cols):
        if h is None:
            return g.at[zr, pl.ds(pl.multiple_of(xr * rows, rows), rows), cols]
        return g.at[zr, pl.ds(pl.multiple_of(xr * rows + h * half, half), half), cols]

    def x_send(k, zr, xr, h, cols, to, direction, slot):
        piece = part(zr, xr, h, cols)
        p = 1 if k == NZ else 0
        sends.start(
            send_to(piece, piece, sx.at[direction, k, slot], rx.at[p, zr, xr, h], tp_of(to, z))
        )

    def x_wait(k, zr, xr, h, cols):
        piece = part(zr, xr, h, cols)
        p = 1 if k == NZ else 0
        send_to(piece, piece, sx.at[0, k, 0], rx.at[p, zr, xr, h], tp_of(xp, z)).wait_recv()

    def x_own(k, zr, cols, first):
        h_right, h_left = (0, 1) if first else (1, 0)
        slot = 0 if first else 1
        x_send(k, zr, x, h_right, cols, xp, 0, slot)
        x_send(k, zr, x, h_left, cols, xm, 1, slot)

    def x_forward(k, zr, cols):
        x_wait(k, zr, xm, 0, cols)
        x_send(k, zr, xm, 0, cols, xp, 0, 2)
        x_wait(k, zr, xp, 1, cols)
        x_send(k, zr, xp, 1, cols, xm, 1, 2)

    def x_rest_near(k, zr, cols):
        x_wait(k, zr, xm, 1, cols)
        x_wait(k, zr, xp, 0, cols)

    def x_rest_opposite(k, zr, cols):
        x_wait(k, zr, xo, 0, cols)
        x_wait(k, zr, xo, 1, cols)

    def x_rest(k, zr, cols):
        x_rest_near(k, zr, cols)
        x_rest_opposite(k, zr, cols)

    def z_send_b(k, zr, way, to):
        piece = part(zr, x, None, b_cols)
        sends.start(send_to(piece, piece, szb.at[way, k], rzb.at[zr], tp_of(x, to)))

    def z_send_a(k, zr, xr, way, to):
        piece = part(zr, xr, None, a_cols)
        sends.start(
            send_to(piece, piece, sza.at[way, k, xr], rza.at[zr, xr], tp_of(x, to))
        )

    def z_wait_b(k):
        piece = part(zs[k], x, None, b_cols)
        send_to(piece, piece, szb.at[0, 0], rzb.at[zs[k]], tp_of(xp, z)).wait_recv()

    def z_wait_a(k):
        for i in range(NX):
            piece = part(zs[k], i, None, a_cols)
            send_to(piece, piece, sza.at[0, 0, i], rza.at[zs[k], i], tp_of(xp, z)).wait_recv()

    def turn(c):
        at = pl.ds(c * TURN, TURN)
        wt[:, at] = w[at, :].T

    def slab(first, count, zr):
        return kv.at[pl.ds(first, count), pl.ds(pl.multiple_of(zr * rows, rows), rows), :]

    def near_copy(k, zr):
        return send_along(
            slab(5, 4, zr), slab(1, 4, zr), s_near.at[k], r_near.at[k],
            jnp.minimum(s + 1, blocks - 1),
        )

    def far_copy(k, zr):
        return send_along(
            slab(8, 1, zr), slab(0, 1, zr), s_far.at[k], r_far.at[k],
            jnp.minimum(s + 2, blocks - 1),
        )

    def project(k):
        zr = zs[k]
        out = jnp.dot(g[zr], w[...], preferred_element_type=jnp.float32).astype(jnp.bfloat16)
        at = pl.ds(pl.multiple_of(zr * rows, rows), rows)
        for i in range(NX):
            kv[5 + i, at, :] = out[i * rows : (i + 1) * rows, q_cols:]
            qb[i, at, :] = out[i * rows : (i + 1) * rows, :q_cols]
        pl.when(s + 1 < blocks)(lambda: near_copy(k, zr).start())
        pl.when(s + 2 < blocks)(lambda: far_copy(k, zr).start())

    is_edge = (z == 0) | (z == NZ - 1)

    def start_gather(neighbours):
        x_own(NZ, z, a_cols, True)
        x_own(NZ, z, a_cols, False)
        for way, to in neighbours:
            z_send_b(0, z, way, to)
        x_own(0, z, b_cols, True)
        x_forward(NZ, z, a_cols)
        x_own(0, z, b_cols, False)
        way, to = neighbours[0]
        x_rest_near(NZ, z, a_cols)
        for i in (x, xm, xp):
            z_send_a(0, z, i, way, to)
        for load in loads[2:]:
            load.wait()
        clear_edges()
        turn(0)
        x_rest_opposite(NZ, z, a_cols)
        z_send_a(0, z, xo, way, to)
        x_forward(0, z, b_cols)
        meet_second()

    def clear_edges():
        @pl.when(s == 0)
        def _():
            kv[0:5] = jnp.zeros_like(kv[0:5])

        @pl.when(s == 1)
        def _():
            kv[0] = jnp.zeros_like(kv[0])

        @pl.when(s == blocks - 1)
        def _():
            back_near[...] = jnp.zeros_like(back_near)

        @pl.when(s >= blocks - 2)
        def _():
            back_far[...] = jnp.zeros_like(back_far)

    @pl.when(is_edge)
    def _():
        start_gather([(0, jnp.where(z == 0, 1, NZ - 2))])
        z_wait_b(1)
        x_own(1, zs[1], b_cols, True)
        x_own(1, zs[1], b_cols, False)
        for c in range(1, 5):
            turn(c)
        x_rest(0, z, b_cols)
        project(0)
        x_forward(1, zs[1], b_cols)
        turn(5)
        z_wait_b(2)
        x_own(2, zs[2], b_cols, True)
        x_own(2, zs[2], b_cols, False)
        z_wait_a(1)
        x_rest(1, zs[1], b_cols)
        project(1)
        x_forward(2, zs[2], b_cols)
        z_wait_b(3)
        x_own(3, zs[3], b_cols, True)
        x_own(3, zs[3], b_cols, False)
        for c in range(6, TURNS):
            turn(c)
        z_wait_a(2)
        x_rest(2, zs[2], b_cols)
        project(2)
        x_forward(3, zs[3], b_cols)
        z_wait_a(3)
        x_rest(3, zs[3], b_cols)
        project(3)
        sends.finish()

    sends = Sends()

    @pl.when(jnp.logical_not(is_edge))
    def _():
        outer = jnp.where(z == 1, 0, NZ - 1)
        inner = NZ - 1 - z
        start_gather([(0, outer), (1, inner)])
        z_wait_b(1)
        z_send_b(1, zs[1], 1, inner)
        for i in (x, xm, xp, xo):
            z_send_a(0, z, i, 1, inner)
        x_own(1, zs[1], b_cols, True)
        x_own(1, zs[1], b_cols, False)
        z_wait_b(2)
        z_send_b(2, zs[2], 0, outer)
        x_own(2, zs[2], b_cols, True)
        x_own(2, zs[2], b_cols, False)
        for c in range(1, 4):
            turn(c)
        x_rest(0, z, b_cols)
        project(0)
        z_wait_a(1)
        for i in range(NX):
            z_send_a(1, zs[1], i, 1, inner)
        z_wait_b(3)
        z_send_b(3, zs[3], 0, outer)
        x_forward(1, zs[1], b_cols)
        x_own(3, zs[3], b_cols, True)
        x_own(3, zs[3], b_cols, False)
        for c in range(4, 7):
            turn(c)
        x_forward(2, zs[2], b_cols)
        z_wait_a(2)
        for i in range(NX):
            z_send_a(2, zs[2], i, 0, outer)
        for c in range(7, TURNS):
            turn(c)
        x_rest(1, zs[1], b_cols)
        project(1)
        z_wait_a(3)
        for i in range(NX):
            z_send_a(3, zs[3], i, 0, outer)
        x_forward(3, zs[3], b_cols)
        x_rest(2, zs[2], b_cols)
        project(2)
        x_rest(3, zs[3], b_cols)
        project(3)
        sends.finish()

    hd = HEAD_SIZE
    last = (((1,), (1,)), ((), ()))

    def two_heads(ref, qt):
        return jnp.concatenate([ref[qt, :, 0:hd], ref[qt, :, hd : 2 * hd]], axis=0)

    row_at = lax.broadcasted_iota(jnp.int32, (hd, 2 * hd), 0)
    col_at = lax.broadcasted_iota(jnp.int32, (hd, 2 * hd), 1) % hd

    def scores(qt, c, q2, do2):
        j = qt + c
        raw = lax.dot_general(kv[j, :, 0:hd], q2, last, preferred_element_type=jnp.float32)
        bent = jnp.tanh(raw * (SCALE / CAP))
        expo = jnp.exp(CAP * bent)
        if c == 0:
            expo = jnp.where(row_at > col_at, expo, 0.0)
        if c == 5:
            expo = jnp.where(row_at <= col_at, expo, 0.0)
        if j < 5:
            expo = expo * jnp.where(s >= (1 if j > 0 else 2), 1.0, 0.0)
        d_probs = lax.dot_general(
            kv[j, :, hd : 2 * hd], do2, last, preferred_element_type=jnp.float32
        )
        e_buf[qt, c] = expo
        dp_buf[qt, c] = d_probs
        b_buf[qt, c] = bent
        shape = (hd // 8, 8, 2 * hd)
        return (
            jnp.sum(expo.reshape(shape), axis=0),
            jnp.sum((expo * d_probs).reshape(shape), axis=0),
        )

    def transpose_keys(j):
        kt[:, pl.ds(j * hd, hd)] = kv[j, :, 0:hd].astype(jnp.float32).T.astype(jnp.bfloat16)

    sums = []
    for qt in range(NX):
        q2, do2 = two_heads(qb, qt), two_heads(dout, qt)
        parts = [scores(qt, c, q2, do2) for c in range(5 - qt, 6)]
        sums.append((sum(p[0] for p in parts), sum(p[1] for p in parts)))
    for j in range(5, 9):
        transpose_keys(j)

    @pl.when(s > 0)
    def _():
        for k in range(NZ):
            near_copy(k, zs[k]).wait_recv()

    @pl.when(s > 1)
    def _():
        for k in range(NZ):
            far_copy(k, zs[k]).wait_recv()

    for j in range(5):
        transpose_keys(j)

    rest = []
    for qt in range(NX):
        q2, do2 = two_heads(qb, qt), two_heads(dout, qt)
        parts = [scores(qt, c, q2, do2) for c in range(0, 5 - qt)]
        norm = jnp.sum(sums[qt][0] + sum(p[0] for p in parts), axis=0, keepdims=True)
        inner = jnp.sum(sums[qt][1] + sum(p[1] for p in parts), axis=0, keepdims=True)
        inverse = 1.0 / norm
        rest.append((inverse, inner * inverse))

    def tile_grads(j):
        d_key = d_value = 0.0
        for qt in range(max(0, j - 5), min(NX, j + 1)):
            c = j - qt
            inverse, delta = rest[qt]
            probs = e_buf[qt, c] * inverse
            bent = b_buf[qt, c]
            d_raw = (
                probs * (dp_buf[qt, c] - delta) * (1.0 - bent * bent) * SCALE
            ).astype(jnp.bfloat16)
            dr_buf[qt, pl.ds(c * hd, hd), :] = d_raw
            d_key += jnp.dot(d_raw, two_heads(qb, qt), preferred_element_type=jnp.float32)
            d_value += jnp.dot(
                probs.astype(jnp.bfloat16), two_heads(dout, qt), preferred_element_type=jnp.float32
            )
        return d_key, d_value

    far_back = send_along(
        back_out.at[0], back_far, s_bf.at[0], r_bf.at[0], jnp.maximum(s - 2, 0)
    )
    near_back = [
        send_along(
            back_out.at[j], back_near.at[j - 1], s_bn.at[j - 1], r_bn.at[j - 1],
            jnp.maximum(s - 1, 0),
        )
        for j in range(1, 5)
    ]
    for j in range(5):
        d_key, d_value = tile_grads(j)
        back_out[j, :, 0:hd] = d_key.astype(jnp.bfloat16)
        back_out[j, :, hd : 2 * hd] = d_value.astype(jnp.bfloat16)
        if j == 0:
            pl.when(s > 1)(lambda: far_back.start())
        else:
            pl.when(s > 0)(lambda j=j: near_back[j - 1].start())
    for j in range(5, 9):
        d_key, d_value = tile_grads(j)
        acc[j - 5, :, 0:hd] = d_key
        acc[j - 5, :, hd : 2 * hd] = d_value
    for qt in range(NX):
        d_query = jnp.dot(
            kt[:, pl.ds(qt * hd, 6 * hd)], dr_buf[qt], preferred_element_type=jnp.float32
        )
        grads[qt, :, 0:hd] = d_query[:, 0:hd].T.astype(jnp.bfloat16)
        grads[qt, :, hd : 2 * hd] = d_query[:, hd : 2 * hd].T.astype(jnp.bfloat16)

    @pl.when(s < blocks - 2)
    def _():
        send_along(back_out.at[0], back_far, s_bf.at[0], r_bf.at[0], s).wait_recv()

    @pl.when(s < blocks - 1)
    def _():
        for i in range(NX):
            send_along(
                back_out.at[i + 1], back_near.at[i], s_bn.at[i], r_bn.at[i], s
            ).wait_recv()

    for i in range(NX):
        own = acc[i] + back_near[i].astype(jnp.float32)
        if i == NX - 1:
            own = own + back_far[...].astype(jnp.float32)
        grads[i, :, q_cols:] = own.astype(jnp.bfloat16)

    zs = zs[::-1]
    p = g
    tile = 768
    a_width = B_TILES * 128
    a_cols = pl.ds(0, a_width)
    b_cols = pl.ds(a_width, width - a_width)
    b_half = (width - a_width) // 2
    b_parts = [pl.ds(a_width, b_half), pl.ds(a_width + b_half, b_half)]

    def row_ds(xr, h=None):
        if h is None:
            return pl.ds(pl.multiple_of(xr * rows, rows), rows)
        return pl.ds(pl.multiple_of(xr * rows + h * half, half), half)

    def compute(zr):
        lhs = grads[:, pl.ds(pl.multiple_of(zr * rows, rows), rows), :].reshape(NX * rows, -1)

        for j in range(width // tile):
            at = pl.ds(j * tile, tile)
            p[zr, :, at] = jnp.dot(
                lhs, wt[:, at], preferred_element_type=jnp.float32
            ).astype(jnp.bfloat16)

    def way(zr):
        return jnp.where(zr > z, 1, 0)

    def nearer(zr):
        return tp_of(x, jnp.where(zr > z, z + 1, z - 1))

    def step1(k, zr, cols):
        for direction, to in ((0, xm), (1, xp)):
            sends.start(
                send_to(
                    p.at[zr, row_ds(xo, direction), cols],
                    got_opp.at[direction, zr, :, cols],
                    s1.at[direction, k],
                    r1.at[direction, k],
                    tp_of(to, z),
                )
            )

    def step2(k, zr, parts):
        for direction, to in ((0, xm), (1, xp)):
            for cols in parts if len(parts) == 1 else [b_cols]:
                land = got_opp.at[direction, zr, :, cols]
                send_to(
                    land, land, s1.at[direction, k], r1.at[direction, k], tp_of(to, z)
                ).wait_recv()
            at = row_ds(to, direction)
            for h, cols in enumerate(parts):
                p[zr, at, cols] = (
                    p[zr, at, cols].astype(jnp.float32)
                    + got_opp[direction, zr, :, cols].astype(jnp.float32)
                ).astype(jnp.bfloat16)
                sends.start(
                    send_to(
                        p.at[zr, row_ds(to), cols],
                        got_x.at[direction, zr, :, cols],
                        s2.at[direction, k, h],
                        r2.at[direction, k, h],
                        tp_of(to, z),
                    )
                )

    def x_sum(k, h, zr, cols):
        for direction, to in ((0, xm), (1, xp)):
            land = got_x.at[direction, zr, :, cols]
            send_to(
                land, land, s2.at[direction, k, h], r2.at[direction, k, h], tp_of(to, z)
            ).wait_recv()
        return (
            p[zr, row_ds(x), cols].astype(jnp.float32)
            + got_x[0, zr, :, cols].astype(jnp.float32)
            + got_x[1, zr, :, cols].astype(jnp.float32)
        )

    def line_b(d, zr, h):
        return got_zb.at[d, zr, h]

    def line_wait_b(d, zr, h):
        land = line_b(d, zr, h)
        send_to(land, land, tzb.at[0, h], uzb.at[d, zr, h], tp_of(xp, z)).wait_recv()

    def line_wait_a(d, zr):
        land = got_za.at[d, zr]
        send_to(land, land, tza.at[0], uza.at[d, zr], tp_of(xp, z)).wait_recv()

    def step3(k, far):
        zr = zs[k]
        for h, cols in enumerate(b_parts):
            value = x_sum(k, h, zr, cols)
            if far:
                line_wait_b(way(zr), zr, h)
                value = value + got_zb[way(zr), zr, h].astype(jnp.float32)
            p[zr, row_ds(x), cols] = value.astype(jnp.bfloat16)
            sends.start(
                send_to(
                    p.at[zr, row_ds(x), cols], line_b(way(zr), zr, h), tzb.at[k, h],
                    uzb.at[way(zr), zr, h], nearer(zr),
                )
            )

    def add_a(d, zr):
        line_wait_a(d, zr)
        p[zr, :, a_cols] = (
            p[zr, :, a_cols].astype(jnp.float32) + got_za[d, zr].astype(jnp.float32)
        ).astype(jnp.bfloat16)

    def line_a(k, far, when=None):
        zr = zs[k]
        if far:
            add_a(way(zr), zr)
        sends.start(
            send_to(
                p.at[zr, :, a_cols], got_za.at[way(zr), zr], tza.at[k],
                uza.at[way(zr), zr], nearer(zr),
            ),
            when,
        )

    def finish(sources):
        for h, cols in enumerate(b_parts):
            value = x_sum(3, h, z, cols)
            for d in sources:
                line_wait_b(d, z, h)
                value = value + got_zb[d, z, h].astype(jnp.float32)
            total[:, cols] = value
        total[:, a_cols] = x_sum(4, 0, z, a_cols)
        values = tok[...].astype(jnp.float32)
        inv_rms = lax.rsqrt(jnp.mean(values * values, axis=1, keepdims=True) + EPS)
        upper = total[...] * gain_row()
        xhat = values * inv_rms
        out_ref[...] = (
            inv_rms * (upper - xhat * jnp.mean(upper * xhat, axis=1, keepdims=True))
        ).astype(jnp.bfloat16)
        sends.finish()

    sends = Sends()
    compute(zs[0])
    step1(0, zs[0], b_cols)
    line_a(0, False, is_edge)
    compute(zs[1])
    step1(1, zs[1], b_cols)
    line_a(1, False, is_edge)
    compute(zs[2])
    line_a(2, False, is_edge)
    compute(z)
    opening, sends = sends, Sends()

    @pl.when(is_edge)
    def _():
        source = jnp.where(z == 0, 0, 1)
        step2(0, zs[0], b_parts)
        step1(2, zs[2], b_cols)
        step2(1, zs[1], b_parts)
        step1(3, z, b_cols)
        step2(2, zs[2], b_parts)
        step3(0, False)
        step3(1, False)
        step2(3, z, b_parts)
        add_a(source, z)
        step1(4, z, a_cols)
        step3(2, False)
        step2(4, z, [a_cols])
        finish([source])

    sends = Sends()

    @pl.when(jnp.logical_not(is_edge))
    def _():
        step2(0, zs[0], b_parts)
        step1(2, zs[2], b_cols)
        line_a(0, True)
        step2(1, zs[1], b_parts)
        step1(3, z, b_cols)
        line_a(1, True)
        step2(2, zs[2], b_parts)
        line_a(2, True)
        step3(0, True)
        step2(3, z, b_parts)
        add_a(0, z)
        add_a(1, z)
        step1(4, z, a_cols)
        step3(2, True)
        step3(1, True)
        step2(4, z, [a_cols])
        finish([0, 1])

    opening.finish()

    @pl.when(s > 0)
    def _():
        for copy in near_back:
            copy.wait_send()

    @pl.when(s > 1)
    def _():
        far_back.wait_send()

    @pl.when(s + 1 < blocks)
    def _():
        for k in range(NZ):
            near_copy(k, zs[NZ - 1 - k]).wait_send()

    @pl.when(s + 2 < blocks)
    def _():
        for k in range(NZ):
            far_copy(k, zs[NZ - 1 - k]).wait_send()


def on_device(tokens, norm_gain, query_weight, key_matrix, value_matrix, output_grad):
    rows, width = tokens.shape
    q_cols, k_cols = query_weight.shape[1], key_matrix.shape[1]
    cols = q_cols + 2 * k_cols
    a_width = B_TILES * 128
    hd = HEAD_SIZE
    any_space = pl.BlockSpec(memory_space=pltpu.HBM)
    dma = pltpu.SemaphoreType.DMA
    low, full = jnp.bfloat16, jnp.float32

    def vmem(kind, *shape):
        return pltpu.VMEM(shape, kind)

    return pl.pallas_call(
        whole,
        out_shape=jax.ShapeDtypeStruct((rows, width), low),
        in_specs=[any_space] * 6,
        out_specs=pl.BlockSpec(memory_space=pltpu.VMEM),
        scratch_shapes=[
            vmem(low, rows, width),
            vmem(full, width // 128, 128),
            vmem(low, width, cols),
            vmem(low, cols, width),
            vmem(low, NZ, NX * rows, width),
            vmem(low, NX, hd, q_cols),
            vmem(low, NX, hd, q_cols),
            vmem(low, 9, hd, 2 * k_cols),
            vmem(low, hd, 9 * hd),
            vmem(full, NX, 6, hd, 2 * hd),
            vmem(full, NX, 6, hd, 2 * hd),
            vmem(full, NX, 6, hd, 2 * hd),
            vmem(low, NX, 6 * hd, 2 * hd),
            vmem(full, NX, hd, 2 * k_cols),
            vmem(low, 5, hd, 2 * k_cols),
            vmem(low, NX, hd, 2 * k_cols),
            vmem(low, hd, 2 * k_cols),
            vmem(low, NX, hd, cols),
            vmem(full, rows, width),
            vmem(low, 2, NZ, rows // 2, width),
            vmem(low, 2, NZ, rows, width),
            vmem(low, 2, NZ, NX * rows, a_width),
            vmem(low, 2, NZ, 2, rows, (width - a_width) // 2),
            dma((6,)),
            dma((2, NZ + 1, 3)),
            dma((2, NZ, NX, 2)),
            dma((2, NZ)),
            dma((NZ,)),
            dma((2, NZ, NX)),
            dma((NZ, NX)),
            dma((NZ,)),
            dma((NZ,)),
            dma((NZ,)),
            dma((NZ,)),
            dma((NX,)),
            dma((NX,)),
            dma((1,)),
            dma((1,)),
            dma((2, NZ + 1)),
            dma((2, NZ + 1)),
            dma((2, NZ + 1, 2)),
            dma((2, NZ + 1, 2)),
            dma((NZ,)),
            dma((2, NZ)),
            dma((NZ, 2)),
            dma((2, NZ, 2)),
        ],
        compiler_params=pltpu.CompilerParams(
            collective_id=0, has_side_effects=True, vmem_limit_bytes=62 * 1024 * 1024
        ),
    )(
        tokens,
        norm_gain.reshape(-1, 128),
        output_grad.reshape(NX, hd, q_cols),
        query_weight,
        key_matrix,
        value_matrix,
    )


def solution(mesh):
    tp, both = "tp", ("seq", "tp")
    in_specs = (P(both, None), P(), P(None, tp), P(None, tp), P(None, tp), P("seq", tp))
    return jax.shard_map(
        on_device, mesh=mesh, in_specs=in_specs, out_specs=P(both, None), check_vma=False
    )
```

```python
import jax
import jax.numpy as jnp
from jax import lax
from jax.experimental import pallas as pl
from jax.experimental.pallas import tpu as pltpu
from jax.sharding import PartitionSpec as P

HEAD_SIZE = 128
WINDOW = 640
SCALE = 1.0 / 12.0
CAP = 50.0
EPS = 1e-06
MESH = pl.DeviceIdType.MESH
NX = 4
NZ = 4
A_TILES = 5
B_TILES = 8
TURN = 512
TURNS = 9


def place():
    t = lax.axis_index("tp")
    return t // NZ, t % NZ


def near_to_far(z):
    def high(q):
        return (q, 5 - q, jnp.int32(1), jnp.int32(0))

    up = high(z)
    low = high(3 - z)
    return [jnp.where(z >= 2, u, 3 - v) for u, v in zip(up, low)]


def send_to(src, dst, send_sem, recv_sem, tp):
    return pltpu.make_async_remote_copy(
        src_ref=src,
        dst_ref=dst,
        send_sem=send_sem,
        recv_sem=recv_sem,
        device_id={"tp": tp},
        device_id_type=MESH,
    )


def tp_of(x, z):
    return x * NZ + z


def send_along(src, dst, send_sem, recv_sem, seq):
    return pltpu.make_async_remote_copy(
        src_ref=src,
        dst_ref=dst,
        send_sem=send_sem,
        recv_sem=recv_sem,
        device_id={"seq": seq},
        device_id_type=MESH,
    )


def greet(device):
    barrier = pltpu.get_barrier_semaphore()
    pl.semaphore_signal(barrier, inc=1, device_id=device, device_id_type=MESH)


def meet(x, z, s, blocks):
    barrier = pltpu.get_barrier_semaphore()
    early = (s // 2) % 2 == 0
    greet({"tp": tp_of((x + 1) % NX, z)})
    greet({"tp": tp_of((x + 3) % NX, z)})
    pl.when(z > 0)(lambda: greet({"tp": tp_of(x, z - 1)}))
    pl.when(z < NZ - 1)(lambda: greet({"tp": tp_of(x, z + 1)}))
    greet({"seq": s + 1 - 2 * (s % 2)})
    near = jnp.where((z == 0) | (z == NZ - 1), 4, 5)
    others = [s - 2, s + 2, s - 1 + 2 * (s % 2)]
    there = [(o >= 0) & (o < blocks) for o in others]
    far = sum(jnp.where(t, 1, 0) for t in there)

    def first():
        pl.semaphore_wait(barrier, near + jnp.where(early, 0, far))
        for o, t in zip(others, there):
            pl.when(t)(lambda o=o: greet({"seq": o}))

    def second():
        pl.when(early)(lambda: pl.semaphore_wait(barrier, far))

    return first, second


class Sends:
    def __init__(self):
        self.started = []

    def start(self, copy, when=None):
        self.started.append((copy, when))
        if when is None:
            copy.start()
        else:
            pl.when(when)(lambda: copy.start())

    def finish(self):
        for copy, when in self.started:
            if when is None:
                copy.wait_send()
            else:
                pl.when(when)(lambda copy=copy: copy.wait_send())


def whole(
    tokens_ref, gain_ref, grad_ref, wq_ref, wk_ref, wv_ref, out_ref,
    tok, gain, w, wt, g, dout, qb, kv, kt, e_buf, dp_buf, b_buf, dr_buf, acc,
    back_out, back_near, back_far, back_chip, grads, total, got_opp, got_x, got_za, got_zb,
    load_sem, sx, rx, szb, rzb, sza, rza, s_near, r_near, s_far, r_far,
    s_bn, r_bn, s_bf, r_bf, s_bc, r_bc, s1, r1, s2, r2, tza, uza, tzb, uzb,
):
    x, z = place()
    s = lax.axis_index("seq")
    blocks = lax.axis_size("seq")
    rows, width = tok.shape
    half = rows // 2
    a_width = A_TILES * 128
    a_cols = pl.ds(0, a_width)
    b_cols = pl.ds(a_width, width - a_width)
    xp, xm, xo = (x + 1) % NX, (x + 3) % NX, (x + 2) % NX
    zs = near_to_far(z)
    q_cols, k_cols = wq_ref.shape[1], wk_ref.shape[1]
    meet_first, meet_second = meet(x, z, s, blocks)
    loads = [
        pltpu.make_async_copy(tokens_ref, tok, load_sem.at[0]),
        pltpu.make_async_copy(gain_ref, gain, load_sem.at[1]),
        pltpu.make_async_copy(wq_ref, w.at[:, pl.ds(0, q_cols)], load_sem.at[2]),
        pltpu.make_async_copy(wk_ref, w.at[:, pl.ds(q_cols, k_cols)], load_sem.at[3]),
        pltpu.make_async_copy(wv_ref, w.at[:, pl.ds(q_cols + k_cols, k_cols)], load_sem.at[4]),
        pltpu.make_async_copy(grad_ref, dout, load_sem.at[5]),
    ]
    for load in loads:
        load.start()
    loads[0].wait()
    loads[1].wait()

    def gain_row():
        return jnp.concatenate([gain[i : i + 1, :] for i in range(gain.shape[0])], axis=1)

    values = tok[...].astype(jnp.float32)
    inv_rms = lax.rsqrt(jnp.mean(values * values, axis=1, keepdims=True) + EPS)
    g[z, pl.ds(x * rows, rows), :] = (values * inv_rms * gain_row()).astype(jnp.bfloat16)
    meet_first()
    sends = Sends()

    def part(zr, xr, h, cols):
        if h is None:
            return g.at[zr, pl.ds(pl.multiple_of(xr * rows, rows), rows), cols]
        return g.at[zr, pl.ds(pl.multiple_of(xr * rows + h * half, half), half), cols]

    def x_send(k, zr, xr, h, cols, to, direction, slot):
        piece = part(zr, xr, h, cols)
        p = 1 if k == NZ else 0
        sends.start(
            send_to(piece, piece, sx.at[direction, k, slot], rx.at[p, zr, xr, h], tp_of(to, z))
        )

    def x_wait(k, zr, xr, h, cols):
        piece = part(zr, xr, h, cols)
        p = 1 if k == NZ else 0
        send_to(piece, piece, sx.at[0, k, 0], rx.at[p, zr, xr, h], tp_of(xp, z)).wait_recv()

    def x_own(k, zr, cols, first):
        h_right, h_left = (0, 1) if first else (1, 0)
        slot = 0 if first else 1
        x_send(k, zr, x, h_right, cols, xp, 0, slot)
        x_send(k, zr, x, h_left, cols, xm, 1, slot)

    def x_forward(k, zr, cols):
        x_wait(k, zr, xm, 0, cols)
        x_send(k, zr, xm, 0, cols, xp, 0, 2)
        x_wait(k, zr, xp, 1, cols)
        x_send(k, zr, xp, 1, cols, xm, 1, 2)

    def x_rest_near(k, zr, cols):
        x_wait(k, zr, xm, 1, cols)
        x_wait(k, zr, xp, 0, cols)

    def x_rest_opposite(k, zr, cols):
        x_wait(k, zr, xo, 0, cols)
        x_wait(k, zr, xo, 1, cols)

    def x_rest(k, zr, cols):
        x_rest_near(k, zr, cols)
        x_rest_opposite(k, zr, cols)

    def z_send_b(k, zr, way, to):
        piece = part(zr, x, None, b_cols)
        sends.start(send_to(piece, piece, szb.at[way, k], rzb.at[zr], tp_of(x, to)))

    def z_send_a(k, zr, xr, way, to):
        piece = part(zr, xr, None, a_cols)
        sends.start(
            send_to(piece, piece, sza.at[way, k, xr], rza.at[zr, xr], tp_of(x, to))
        )

    def z_wait_b(k):
        piece = part(zs[k], x, None, b_cols)
        send_to(piece, piece, szb.at[0, 0], rzb.at[zs[k]], tp_of(xp, z)).wait_recv()

    def z_wait_a(k):
        for i in range(NX):
            piece = part(zs[k], i, None, a_cols)
            send_to(piece, piece, sza.at[0, 0, i], rza.at[zs[k], i], tp_of(xp, z)).wait_recv()

    def turn(c):
        at = pl.ds(c * TURN, TURN)
        wt[:, at] = w[at, :].T

    def slab(first, count, zr):
        return kv.at[pl.ds(first, count), pl.ds(pl.multiple_of(zr * rows, rows), rows), :]

    def near_copy(k, zr):
        return send_along(
            slab(5, 4, zr), slab(1, 4, zr), s_near.at[k], r_near.at[k],
            jnp.minimum(s + 1, blocks - 1),
        )

    def far_copy(k, zr):
        return send_along(
            slab(8, 1, zr), slab(0, 1, zr), s_far.at[k], r_far.at[k],
            jnp.minimum(s + 2, blocks - 1),
        )

    def project(k):
        zr = zs[k]
        out = jnp.dot(g[zr], w[...], preferred_element_type=jnp.float32).astype(jnp.bfloat16)
        at = pl.ds(pl.multiple_of(zr * rows, rows), rows)
        for i in range(NX):
            kv[5 + i, at, :] = out[i * rows : (i + 1) * rows, q_cols:]
            qb[i, at, :] = out[i * rows : (i + 1) * rows, :q_cols]
        pl.when(s + 2 < blocks)(lambda: far_copy(k, zr).start())
        pl.when(s + 1 < blocks)(lambda: near_copy(k, zr).start())

    is_edge = (z == 0) | (z == NZ - 1)

    def start_gather(neighbours):
        x_own(NZ, z, a_cols, True)
        x_own(NZ, z, a_cols, False)
        for way, to in neighbours:
            z_send_b(0, z, way, to)
        x_own(0, z, b_cols, True)
        x_forward(NZ, z, a_cols)
        x_own(0, z, b_cols, False)
        way, to = neighbours[0]
        x_rest_near(NZ, z, a_cols)
        for i in (x, xm, xp):
            z_send_a(0, z, i, way, to)
        for load in loads[2:]:
            load.wait()
        clear_edges()
        turn(0)
        x_rest_opposite(NZ, z, a_cols)
        z_send_a(0, z, xo, way, to)
        x_forward(0, z, b_cols)
        meet_second()

    def clear_edges():
        @pl.when(s == 0)
        def _():
            kv[0:5] = jnp.zeros_like(kv[0:5])

        @pl.when(s == 1)
        def _():
            kv[0] = jnp.zeros_like(kv[0])

        @pl.when(s == blocks - 1)
        def _():
            back_near[...] = jnp.zeros_like(back_near)

        @pl.when((s >= blocks - 2) | (s % 2 == 1))
        def _():
            back_far[...] = jnp.zeros_like(back_far)

    @pl.when(is_edge)
    def _():
        start_gather([(0, jnp.where(z == 0, 1, NZ - 2))])
        z_wait_b(1)
        x_own(1, zs[1], b_cols, True)
        x_own(1, zs[1], b_cols, False)
        for c in range(1, 5):
            turn(c)
        x_rest(0, z, b_cols)
        project(0)
        x_forward(1, zs[1], b_cols)
        turn(5)
        z_wait_b(2)
        x_own(2, zs[2], b_cols, True)
        x_own(2, zs[2], b_cols, False)
        z_wait_a(1)
        x_rest(1, zs[1], b_cols)
        project(1)
        x_forward(2, zs[2], b_cols)
        z_wait_b(3)
        x_own(3, zs[3], b_cols, True)
        x_own(3, zs[3], b_cols, False)
        for c in range(6, TURNS):
            turn(c)
        z_wait_a(2)
        x_rest(2, zs[2], b_cols)
        project(2)
        x_forward(3, zs[3], b_cols)
        z_wait_a(3)
        x_rest(3, zs[3], b_cols)
        project(3)
        sends.finish()

    sends = Sends()

    @pl.when(jnp.logical_not(is_edge))
    def _():
        outer = jnp.where(z == 1, 0, NZ - 1)
        inner = NZ - 1 - z
        start_gather([(0, outer), (1, inner)])
        z_wait_b(1)
        z_send_b(1, zs[1], 1, inner)
        for i in (x, xm, xp, xo):
            z_send_a(0, z, i, 1, inner)
        x_own(1, zs[1], b_cols, True)
        x_own(1, zs[1], b_cols, False)
        z_wait_b(2)
        z_send_b(2, zs[2], 0, outer)
        x_own(2, zs[2], b_cols, True)
        x_own(2, zs[2], b_cols, False)
        for c in range(1, 4):
            turn(c)
        x_rest(0, z, b_cols)
        project(0)
        z_wait_a(1)
        for i in range(NX):
            z_send_a(1, zs[1], i, 1, inner)
        z_wait_b(3)
        z_send_b(3, zs[3], 0, outer)
        x_forward(1, zs[1], b_cols)
        x_own(3, zs[3], b_cols, True)
        x_own(3, zs[3], b_cols, False)
        for c in range(4, 7):
            turn(c)
        x_forward(2, zs[2], b_cols)
        z_wait_a(2)
        for i in range(NX):
            z_send_a(2, zs[2], i, 0, outer)
        for c in range(7, TURNS):
            turn(c)
        x_rest(1, zs[1], b_cols)
        project(1)
        z_wait_a(3)
        for i in range(NX):
            z_send_a(3, zs[3], i, 0, outer)
        x_forward(3, zs[3], b_cols)
        x_rest(2, zs[2], b_cols)
        project(2)
        x_rest(3, zs[3], b_cols)
        project(3)
        sends.finish()

    hd = HEAD_SIZE
    last = (((1,), (1,)), ((), ()))

    def two_heads(ref, qt):
        return jnp.concatenate([ref[qt, :, 0:hd], ref[qt, :, hd : 2 * hd]], axis=0)

    row_at = lax.broadcasted_iota(jnp.int32, (hd, 2 * hd), 0)
    col_at = lax.broadcasted_iota(jnp.int32, (hd, 2 * hd), 1) % hd

    def scores(qt, c, q2, do2):
        j = qt + c
        raw = lax.dot_general(kv[j, :, 0:hd], q2, last, preferred_element_type=jnp.float32)
        bent = jnp.tanh(raw * (SCALE / CAP))
        expo = jnp.exp(CAP * bent)
        if c == 0:
            expo = jnp.where(row_at > col_at, expo, 0.0)
        if c == 5:
            expo = jnp.where(row_at <= col_at, expo, 0.0)
        if j < 5:
            expo = expo * jnp.where(s >= (1 if j > 0 else 2), 1.0, 0.0)
        d_probs = lax.dot_general(
            kv[j, :, hd : 2 * hd], do2, last, preferred_element_type=jnp.float32
        )
        e_buf[qt, c] = expo
        dp_buf[qt, c] = d_probs
        b_buf[qt, c] = bent
        shape = (hd // 8, 8, 2 * hd)
        return (
            jnp.sum(expo.reshape(shape), axis=0),
            jnp.sum((expo * d_probs).reshape(shape), axis=0),
        )

    def transpose_keys(j):
        kt[:, pl.ds(j * hd, hd)] = kv[j, :, 0:hd].astype(jnp.float32).T.astype(jnp.bfloat16)

    sums = []
    for qt in range(NX):
        q2, do2 = two_heads(qb, qt), two_heads(dout, qt)
        parts = [scores(qt, c, q2, do2) for c in range(5 - qt, 6)]
        sums.append((sum(p[0] for p in parts), sum(p[1] for p in parts)))
    for j in range(5, 9):
        transpose_keys(j)

    @pl.when(s > 0)
    def _():
        for k in range(NZ):
            near_copy(k, zs[k]).wait_recv()

    @pl.when(s > 1)
    def _():
        for k in range(NZ):
            far_copy(k, zs[k]).wait_recv()

    for j in range(5):
        transpose_keys(j)

    rest = []
    for qt in range(NX):
        q2, do2 = two_heads(qb, qt), two_heads(dout, qt)
        parts = [scores(qt, c, q2, do2) for c in range(0, 5 - qt)]
        norm = jnp.sum(sums[qt][0] + sum(p[0] for p in parts), axis=0, keepdims=True)
        inner = jnp.sum(sums[qt][1] + sum(p[1] for p in parts), axis=0, keepdims=True)
        inverse = 1.0 / norm
        rest.append((inverse, inner * inverse))

    def tile_grads(j):
        d_key = d_value = 0.0
        for qt in range(max(0, j - 5), min(NX, j + 1)):
            c = j - qt
            inverse, delta = rest[qt]
            probs = e_buf[qt, c] * inverse
            bent = b_buf[qt, c]
            d_raw = (
                probs * (dp_buf[qt, c] - delta) * (1.0 - bent * bent) * SCALE
            ).astype(jnp.bfloat16)
            dr_buf[qt, pl.ds(c * hd, hd), :] = d_raw
            d_key += jnp.dot(d_raw, two_heads(qb, qt), preferred_element_type=jnp.float32)
            d_value += jnp.dot(
                probs.astype(jnp.bfloat16), two_heads(dout, qt), preferred_element_type=jnp.float32
            )
        return d_key, d_value

    far_back = send_along(
        back_out.at[0], back_far, s_bf.at[0], r_bf.at[0], jnp.maximum(s - 2, 0)
    )
    near_back = [
        send_along(
            back_out.at[j], back_near.at[j - 1], s_bn.at[j - 1], r_bn.at[j - 1],
            jnp.maximum(s - 1, 0),
        )
        for j in range(1, 5)
    ]
    chip_back = send_along(
        back_out.at[0], back_chip, s_bc.at[0], r_bc.at[0], jnp.maximum(s - 1, 0)
    )
    is_odd = s % 2 == 1
    for j in range(5):
        d_key, d_value = tile_grads(j)
        back_out[j, :, 0:hd] = d_key.astype(jnp.bfloat16)
        back_out[j, :, hd : 2 * hd] = d_value.astype(jnp.bfloat16)
        if j == 0:
            pl.when(is_odd)(lambda: chip_back.start())
        elif j < 4:
            pl.when(s > 0)(lambda j=j: near_back[j - 1].start())
        else:

            @pl.when(jnp.logical_not(is_odd))
            def _():
                chip_back.wait_recv()
                other = back_chip[...].astype(jnp.float32)
                back_out[j, :, 0:hd] = (d_key + other[:, 0:hd]).astype(jnp.bfloat16)
                back_out[j, :, hd : 2 * hd] = (d_value + other[:, hd : 2 * hd]).astype(
                    jnp.bfloat16
                )

            pl.when(s > 0)(lambda: near_back[3].start())
            pl.when((s > 1) & jnp.logical_not(is_odd))(lambda: far_back.start())
    for j in range(5, 9):
        d_key, d_value = tile_grads(j)
        acc[j - 5, :, 0:hd] = d_key
        acc[j - 5, :, hd : 2 * hd] = d_value
    for qt in range(NX):
        d_query = jnp.dot(
            kt[:, pl.ds(qt * hd, 6 * hd)], dr_buf[qt], preferred_element_type=jnp.float32
        )
        grads[qt, :, 0:hd] = d_query[:, 0:hd].T.astype(jnp.bfloat16)
        grads[qt, :, hd : 2 * hd] = d_query[:, hd : 2 * hd].T.astype(jnp.bfloat16)

    @pl.when((s < blocks - 2) & jnp.logical_not(is_odd))
    def _():
        far_back.wait_recv()

    @pl.when(s < blocks - 1)
    def _():
        for i in range(NX):
            send_along(
                back_out.at[i + 1], back_near.at[i], s_bn.at[i], r_bn.at[i], s
            ).wait_recv()

    for i in range(NX):
        own = acc[i] + back_near[i].astype(jnp.float32)
        if i == NX - 1:
            own = own + back_far[...].astype(jnp.float32)
        grads[i, :, q_cols:] = own.astype(jnp.bfloat16)

    zs = zs[::-1]
    p = g
    tile = 768
    a_width = B_TILES * 128
    a_cols = pl.ds(0, a_width)
    b_cols = pl.ds(a_width, width - a_width)
    b_half = (width - a_width) // 2
    a_half = a_width // 2
    a_parts = [pl.ds(0, a_half), pl.ds(a_half, a_half)]
    b_parts = [pl.ds(a_width, b_half), pl.ds(a_width + b_half, b_half)]

    def row_ds(xr, h=None):
        if h is None:
            return pl.ds(pl.multiple_of(xr * rows, rows), rows)
        return pl.ds(pl.multiple_of(xr * rows + h * half, half), half)

    def compute(zr):
        lhs = grads[:, pl.ds(pl.multiple_of(zr * rows, rows), rows), :].reshape(NX * rows, -1)

        for j in range(width // tile):
            at = pl.ds(j * tile, tile)
            p[zr, :, at] = jnp.dot(
                lhs, wt[:, at], preferred_element_type=jnp.float32
            ).astype(jnp.bfloat16)

    def way(zr):
        return jnp.where(zr > z, 1, 0)

    def nearer(zr):
        return tp_of(x, jnp.where(zr > z, z + 1, z - 1))

    def step1(k, zr, cols):
        for direction, to in ((0, xm), (1, xp)):
            sends.start(
                send_to(
                    p.at[zr, row_ds(xo, direction), cols],
                    got_opp.at[direction, zr, :, cols],
                    s1.at[direction, k],
                    r1.at[direction, k],
                    tp_of(to, z),
                )
            )

    def step2(k, zr, parts):
        for direction, to in ((0, xm), (1, xp)):
            for cols in parts if len(parts) == 1 else [b_cols]:
                land = got_opp.at[direction, zr, :, cols]
                send_to(
                    land, land, s1.at[direction, k], r1.at[direction, k], tp_of(to, z)
                ).wait_recv()
            at = row_ds(to, direction)
            for h, cols in enumerate(parts):
                p[zr, at, cols] = (
                    p[zr, at, cols].astype(jnp.float32)
                    + got_opp[direction, zr, :, cols].astype(jnp.float32)
                ).astype(jnp.bfloat16)
                sends.start(
                    send_to(
                        p.at[zr, row_ds(to), cols],
                        got_x.at[direction, zr, :, cols],
                        s2.at[direction, k, h],
                        r2.at[direction, k, h],
                        tp_of(to, z),
                    )
                )

    def x_sum(k, h, zr, cols):
        for direction, to in ((0, xm), (1, xp)):
            land = got_x.at[direction, zr, :, cols]
            send_to(
                land, land, s2.at[direction, k, h], r2.at[direction, k, h], tp_of(to, z)
            ).wait_recv()
        return (
            p[zr, row_ds(x), cols].astype(jnp.float32)
            + got_x[0, zr, :, cols].astype(jnp.float32)
            + got_x[1, zr, :, cols].astype(jnp.float32)
        )

    def line_b(d, zr, h):
        return got_zb.at[d, zr, h]

    def line_wait_b(d, zr, h):
        land = line_b(d, zr, h)
        send_to(land, land, tzb.at[0, h], uzb.at[d, zr, h], tp_of(xp, z)).wait_recv()

    def line_wait_a(d, zr, h):
        land = got_za.at[d, zr, :, a_parts[h]]
        send_to(land, land, tza.at[0, h], uza.at[d, zr, h], tp_of(xp, z)).wait_recv()

    def step3(k, far):
        zr = zs[k]
        for h, cols in enumerate(b_parts):
            value = x_sum(k, h, zr, cols)
            if far:
                line_wait_b(way(zr), zr, h)
                value = value + got_zb[way(zr), zr, h].astype(jnp.float32)
            p[zr, row_ds(x), cols] = value.astype(jnp.bfloat16)
            sends.start(
                send_to(
                    p.at[zr, row_ds(x), cols], line_b(way(zr), zr, h), tzb.at[k, h],
                    uzb.at[way(zr), zr, h], nearer(zr),
                )
            )

    def add_a(d, zr, h):
        line_wait_a(d, zr, h)
        cols = a_parts[h]
        p[zr, :, cols] = (
            p[zr, :, cols].astype(jnp.float32) + got_za[d, zr, :, cols].astype(jnp.float32)
        ).astype(jnp.bfloat16)

    def line_a(k, far, when=None):
        zr = zs[k]
        for h, cols in enumerate(a_parts):
            if far:
                add_a(way(zr), zr, h)
            sends.start(
                send_to(
                    p.at[zr, :, cols], got_za.at[way(zr), zr, :, cols], tza.at[k, h],
                    uza.at[way(zr), zr, h], nearer(zr),
                ),
                when,
            )

    def finish(sources):
        for h, cols in enumerate(b_parts):
            value = x_sum(3, h, z, cols)
            for d in sources:
                line_wait_b(d, z, h)
                value = value + got_zb[d, z, h].astype(jnp.float32)
            total[:, cols] = value
        total[:, a_cols] = x_sum(4, 0, z, a_cols)
        values = tok[...].astype(jnp.float32)
        inv_rms = lax.rsqrt(jnp.mean(values * values, axis=1, keepdims=True) + EPS)
        upper = total[...] * gain_row()
        xhat = values * inv_rms
        out_ref[...] = (
            inv_rms * (upper - xhat * jnp.mean(upper * xhat, axis=1, keepdims=True))
        ).astype(jnp.bfloat16)
        sends.finish()

    sends = Sends()
    compute(zs[0])
    step1(0, zs[0], b_cols)
    line_a(0, False, is_edge)
    compute(zs[1])
    step1(1, zs[1], b_cols)
    line_a(1, False, is_edge)
    compute(zs[2])
    line_a(2, False, is_edge)
    compute(z)
    opening, sends = sends, Sends()

    @pl.when(is_edge)
    def _():
        source = jnp.where(z == 0, 0, 1)
        step2(0, zs[0], b_parts)
        step1(2, zs[2], b_cols)
        step2(1, zs[1], b_parts)
        step1(3, z, b_cols)
        step2(2, zs[2], b_parts)
        step3(0, False)
        step3(1, False)
        add_a(source, z, 0)
        add_a(source, z, 1)
        step1(4, z, a_cols)
        step2(3, z, b_parts)
        step3(2, False)
        step2(4, z, [a_cols])
        finish([source])

    sends = Sends()

    @pl.when(jnp.logical_not(is_edge))
    def _():
        step2(0, zs[0], b_parts)
        step1(2, zs[2], b_cols)
        line_a(0, True)
        step2(1, zs[1], b_parts)
        step1(3, z, b_cols)
        line_a(1, True)
        step2(2, zs[2], b_parts)
        line_a(2, True)
        for d in (0, 1):
            for h in (0, 1):
                add_a(d, z, h)
        step1(4, z, a_cols)
        step2(3, z, b_parts)
        step3(0, True)
        step3(2, True)
        step3(1, True)
        step2(4, z, [a_cols])
        finish([0, 1])

    opening.finish()

    @pl.when(s > 0)
    def _():
        for copy in near_back:
            copy.wait_send()

    @pl.when((s > 1) & jnp.logical_not(is_odd))
    def _():
        far_back.wait_send()

    @pl.when(is_odd)
    def _():
        chip_back.wait_send()

    @pl.when(s + 1 < blocks)
    def _():
        for k in range(NZ):
            near_copy(k, zs[NZ - 1 - k]).wait_send()

    @pl.when(s + 2 < blocks)
    def _():
        for k in range(NZ):
            far_copy(k, zs[NZ - 1 - k]).wait_send()


def on_device(tokens, norm_gain, query_weight, key_matrix, value_matrix, output_grad):
    rows, width = tokens.shape
    q_cols, k_cols = query_weight.shape[1], key_matrix.shape[1]
    cols = q_cols + 2 * k_cols
    a_width = B_TILES * 128
    hd = HEAD_SIZE
    any_space = pl.BlockSpec(memory_space=pltpu.HBM)
    dma = pltpu.SemaphoreType.DMA
    low, full = jnp.bfloat16, jnp.float32

    def vmem(kind, *shape):
        return pltpu.VMEM(shape, kind)

    return pl.pallas_call(
        whole,
        out_shape=jax.ShapeDtypeStruct((rows, width), low),
        in_specs=[any_space] * 6,
        out_specs=pl.BlockSpec(memory_space=pltpu.VMEM),
        scratch_shapes=[
            vmem(low, rows, width),
            vmem(full, width // 128, 128),
            vmem(low, width, cols),
            vmem(low, cols, width),
            vmem(low, NZ, NX * rows, width),
            vmem(low, NX, hd, q_cols),
            vmem(low, NX, hd, q_cols),
            vmem(low, 9, hd, 2 * k_cols),
            vmem(low, hd, 9 * hd),
            vmem(full, NX, 6, hd, 2 * hd),
            vmem(full, NX, 6, hd, 2 * hd),
            vmem(full, NX, 6, hd, 2 * hd),
            vmem(low, NX, 6 * hd, 2 * hd),
            vmem(full, NX, hd, 2 * k_cols),
            vmem(low, 5, hd, 2 * k_cols),
            vmem(low, NX, hd, 2 * k_cols),
            vmem(low, hd, 2 * k_cols),
            vmem(low, hd, 2 * k_cols),
            vmem(low, NX, hd, cols),
            vmem(full, rows, width),
            vmem(low, 2, NZ, rows // 2, width),
            vmem(low, 2, NZ, rows, width),
            vmem(low, 2, NZ, NX * rows, a_width),
            vmem(low, 2, NZ, 2, rows, (width - a_width) // 2),
            dma((6,)),
            dma((2, NZ + 1, 3)),
            dma((2, NZ, NX, 2)),
            dma((2, NZ)),
            dma((NZ,)),
            dma((2, NZ, NX)),
            dma((NZ, NX)),
            dma((NZ,)),
            dma((NZ,)),
            dma((NZ,)),
            dma((NZ,)),
            dma((NX,)),
            dma((NX,)),
            dma((1,)),
            dma((1,)),
            dma((1,)),
            dma((1,)),
            dma((2, NZ + 1)),
            dma((2, NZ + 1)),
            dma((2, NZ + 1, 2)),
            dma((2, NZ + 1, 2)),
            dma((NZ, 2)),
            dma((2, NZ, 2)),
            dma((NZ, 2)),
            dma((2, NZ, 2)),
        ],
        compiler_params=pltpu.CompilerParams(
            collective_id=0, has_side_effects=True, vmem_limit_bytes=62 * 1024 * 1024
        ),
    )(
        tokens,
        norm_gain.reshape(-1, 128),
        output_grad.reshape(NX, hd, q_cols),
        query_weight,
        key_matrix,
        value_matrix,
    )


def solution(mesh):
    tp, both = "tp", ("seq", "tp")
    in_specs = (P(both, None), P(), P(None, tp), P(None, tp), P(None, tp), P("seq", tp))
    return jax.shard_map(
        on_device, mesh=mesh, in_specs=in_specs, out_specs=P(both, None), check_vma=False
    )
```

```python
import jax
import jax.numpy as jnp
from jax import lax
from jax.experimental import pallas as pl
from jax.experimental.pallas import tpu as pltpu
from jax.sharding import PartitionSpec as P

HEAD_SIZE = 128
WINDOW = 640
SCALE = 1.0 / 12.0
CAP = 50.0
EPS = 1e-06
MESH = pl.DeviceIdType.MESH
NX = 4
NZ = 4
A_TILES = 5
B_TILES = 8
TURN = 512
TURNS = 9


def place():
    t = lax.axis_index("tp")
    return t // NZ, t % NZ


def near_to_far(z):
    def high(q):
        return (q, 5 - q, jnp.int32(1), jnp.int32(0))

    up = high(z)
    low = high(3 - z)
    return [jnp.where(z >= 2, u, 3 - v) for u, v in zip(up, low)]


def send_to(src, dst, send_sem, recv_sem, tp):
    return pltpu.make_async_remote_copy(
        src_ref=src,
        dst_ref=dst,
        send_sem=send_sem,
        recv_sem=recv_sem,
        device_id={"tp": tp},
        device_id_type=MESH,
    )


def tp_of(x, z):
    return x * NZ + z


def send_along(src, dst, send_sem, recv_sem, seq):
    return pltpu.make_async_remote_copy(
        src_ref=src,
        dst_ref=dst,
        send_sem=send_sem,
        recv_sem=recv_sem,
        device_id={"seq": seq},
        device_id_type=MESH,
    )


def greet(device):
    barrier = pltpu.get_barrier_semaphore()
    pl.semaphore_signal(barrier, inc=1, device_id=device, device_id_type=MESH)


def meet(x, z, s, blocks):
    barrier = pltpu.get_barrier_semaphore()
    early = (s // 2) % 2 == 0
    greet({"tp": tp_of((x + 1) % NX, z)})
    greet({"tp": tp_of((x + 3) % NX, z)})
    pl.when(z > 0)(lambda: greet({"tp": tp_of(x, z - 1)}))
    pl.when(z < NZ - 1)(lambda: greet({"tp": tp_of(x, z + 1)}))
    greet({"seq": s + 1 - 2 * (s % 2)})
    near = jnp.where((z == 0) | (z == NZ - 1), 4, 5)
    others = [s - 2, s + 2, s - 1 + 2 * (s % 2)]
    there = [(o >= 0) & (o < blocks) for o in others]
    far = sum(jnp.where(t, 1, 0) for t in there)

    def first():
        pl.semaphore_wait(barrier, near + jnp.where(early, 0, far))
        for o, t in zip(others, there):
            pl.when(t)(lambda o=o: greet({"seq": o}))

    def second():
        pl.when(early)(lambda: pl.semaphore_wait(barrier, far))

    return first, second


class Sends:
    def __init__(self):
        self.started = []

    def start(self, copy, when=None):
        self.started.append((copy, when))
        if when is None:
            copy.start()
        else:
            pl.when(when)(lambda: copy.start())

    def finish(self):
        for copy, when in self.started:
            if when is None:
                copy.wait_send()
            else:
                pl.when(when)(lambda copy=copy: copy.wait_send())


def whole(
    tokens_ref, gain_ref, grad_ref, wq_ref, wk_ref, wv_ref, out_ref,
    tok, gain, w, wt, g, dout, qb, kv, kt, e_buf, dp_buf, b_buf, dr_buf, acc,
    back_out, back_near, back_far, back_chip, grads, total, got_opp, got_x, got_za, got_zb,
    load_sem, sx, rx, szb, rzb, sza, rza, s_near, r_near, s_far, r_far,
    s_bn, r_bn, s_bf, r_bf, s_bc, r_bc, s1, r1, s2, r2, tza, uza, tzb, uzb,
):
    x, z = place()
    s = lax.axis_index("seq")
    blocks = lax.axis_size("seq")
    rows, width = tok.shape
    half = rows // 2
    a_width = A_TILES * 128
    a_cols = pl.ds(0, a_width)
    b_cols = pl.ds(a_width, width - a_width)
    xp, xm, xo = (x + 1) % NX, (x + 3) % NX, (x + 2) % NX
    zs = near_to_far(z)
    q_cols, k_cols = wq_ref.shape[1], wk_ref.shape[1]
    meet_first, meet_second = meet(x, z, s, blocks)
    loads = [
        pltpu.make_async_copy(tokens_ref, tok, load_sem.at[0]),
        pltpu.make_async_copy(gain_ref, gain, load_sem.at[1]),
        pltpu.make_async_copy(wq_ref, w.at[:, pl.ds(0, q_cols)], load_sem.at[2]),
        pltpu.make_async_copy(wk_ref, w.at[:, pl.ds(q_cols, k_cols)], load_sem.at[3]),
        pltpu.make_async_copy(wv_ref, w.at[:, pl.ds(q_cols + k_cols, k_cols)], load_sem.at[4]),
        pltpu.make_async_copy(grad_ref, dout, load_sem.at[5]),
    ]
    for load in loads:
        load.start()
    loads[0].wait()
    loads[1].wait()

    def gain_row():
        return jnp.concatenate([gain[i : i + 1, :] for i in range(gain.shape[0])], axis=1)

    values = tok[...].astype(jnp.float32)
    inv_rms = lax.rsqrt(jnp.mean(values * values, axis=1, keepdims=True) + EPS)
    g[z, pl.ds(x * rows, rows), :] = (values * inv_rms * gain_row()).astype(jnp.bfloat16)
    meet_first()
    sends = Sends()

    def part(zr, xr, h, cols):
        if h is None:
            return g.at[zr, pl.ds(pl.multiple_of(xr * rows, rows), rows), cols]
        return g.at[zr, pl.ds(pl.multiple_of(xr * rows + h * half, half), half), cols]

    def x_send(k, zr, xr, h, cols, to, direction, slot):
        piece = part(zr, xr, h, cols)
        p = 1 if k == NZ else 0
        sends.start(
            send_to(piece, piece, sx.at[direction, k, slot], rx.at[p, zr, xr, h], tp_of(to, z))
        )

    def x_wait(k, zr, xr, h, cols):
        piece = part(zr, xr, h, cols)
        p = 1 if k == NZ else 0
        send_to(piece, piece, sx.at[0, k, 0], rx.at[p, zr, xr, h], tp_of(xp, z)).wait_recv()

    def x_own(k, zr, cols, first):
        h_right, h_left = (0, 1) if first else (1, 0)
        slot = 0 if first else 1
        x_send(k, zr, x, h_right, cols, xp, 0, slot)
        x_send(k, zr, x, h_left, cols, xm, 1, slot)

    def x_forward(k, zr, cols):
        x_wait(k, zr, xm, 0, cols)
        x_send(k, zr, xm, 0, cols, xp, 0, 2)
        x_wait(k, zr, xp, 1, cols)
        x_send(k, zr, xp, 1, cols, xm, 1, 2)

    def x_rest_near(k, zr, cols):
        x_wait(k, zr, xm, 1, cols)
        x_wait(k, zr, xp, 0, cols)

    def x_rest_opposite(k, zr, cols):
        x_wait(k, zr, xo, 0, cols)
        x_wait(k, zr, xo, 1, cols)

    def x_rest(k, zr, cols):
        x_rest_near(k, zr, cols)
        x_rest_opposite(k, zr, cols)

    def z_send_b(k, zr, way, to):
        piece = part(zr, x, None, b_cols)
        sends.start(send_to(piece, piece, szb.at[way, k], rzb.at[zr], tp_of(x, to)))

    def z_send_a(k, zr, xr, way, to):
        piece = part(zr, xr, None, a_cols)
        sends.start(
            send_to(piece, piece, sza.at[way, k, xr], rza.at[zr, xr], tp_of(x, to))
        )

    def z_wait_b(k):
        piece = part(zs[k], x, None, b_cols)
        send_to(piece, piece, szb.at[0, 0], rzb.at[zs[k]], tp_of(xp, z)).wait_recv()

    def z_wait_a(k):
        for i in range(NX):
            piece = part(zs[k], i, None, a_cols)
            send_to(piece, piece, sza.at[0, 0, i], rza.at[zs[k], i], tp_of(xp, z)).wait_recv()

    def turn(c):
        at = pl.ds(c * TURN, TURN)
        wt[:, at] = w[at, :].T

    def slab(first, count, zr):
        return kv.at[pl.ds(first, count), pl.ds(pl.multiple_of(zr * rows, rows), rows), :]

    def near_copy(k, zr):
        return send_along(
            slab(5, 4, zr), slab(1, 4, zr), s_near.at[k], r_near.at[k],
            jnp.minimum(s + 1, blocks - 1),
        )

    def far_copy(k, zr):
        return send_along(
            slab(8, 1, zr), slab(0, 1, zr), s_far.at[k], r_far.at[k],
            jnp.minimum(s + 2, blocks - 1),
        )

    def project(k):
        zr = zs[k]
        out = jnp.dot(g[zr], w[...], preferred_element_type=jnp.float32).astype(jnp.bfloat16)
        at = pl.ds(pl.multiple_of(zr * rows, rows), rows)
        for i in range(NX):
            kv[5 + i, at, :] = out[i * rows : (i + 1) * rows, q_cols:]
            qb[i, at, :] = out[i * rows : (i + 1) * rows, :q_cols]
        pl.when(s + 2 < blocks)(lambda: far_copy(k, zr).start())
        pl.when(s + 1 < blocks)(lambda: near_copy(k, zr).start())

    is_edge = (z == 0) | (z == NZ - 1)

    def start_gather(neighbours):
        x_own(NZ, z, a_cols, True)
        x_own(NZ, z, a_cols, False)
        for way, to in neighbours:
            z_send_b(0, z, way, to)
        x_own(0, z, b_cols, True)
        x_forward(NZ, z, a_cols)
        x_own(0, z, b_cols, False)
        way, to = neighbours[0]
        x_rest_near(NZ, z, a_cols)
        for i in (x, xm, xp):
            z_send_a(0, z, i, way, to)
        for load in loads[2:]:
            load.wait()
        clear_edges()
        turn(0)
        x_rest_opposite(NZ, z, a_cols)
        z_send_a(0, z, xo, way, to)
        x_forward(0, z, b_cols)
        meet_second()

    def clear_edges():
        @pl.when(s == 0)
        def _():
            kv[0:5] = jnp.zeros_like(kv[0:5])

        @pl.when(s == 1)
        def _():
            kv[0] = jnp.zeros_like(kv[0])

        @pl.when(s == blocks - 1)
        def _():
            back_near[...] = jnp.zeros_like(back_near)

        @pl.when((s >= blocks - 2) | (s % 2 == 1))
        def _():
            back_far[...] = jnp.zeros_like(back_far)

    @pl.when(is_edge)
    def _():
        start_gather([(0, jnp.where(z == 0, 1, NZ - 2))])
        z_wait_b(1)
        x_own(1, zs[1], b_cols, True)
        x_own(1, zs[1], b_cols, False)
        for c in range(1, 5):
            turn(c)
        x_rest(0, z, b_cols)
        project(0)
        x_forward(1, zs[1], b_cols)
        turn(5)
        z_wait_b(2)
        x_own(2, zs[2], b_cols, True)
        x_own(2, zs[2], b_cols, False)
        z_wait_a(1)
        x_rest(1, zs[1], b_cols)
        project(1)
        x_forward(2, zs[2], b_cols)
        z_wait_b(3)
        x_own(3, zs[3], b_cols, True)
        x_own(3, zs[3], b_cols, False)
        for c in range(6, TURNS):
            turn(c)
        z_wait_a(2)
        x_rest(2, zs[2], b_cols)
        project(2)
        x_forward(3, zs[3], b_cols)
        z_wait_a(3)
        x_rest(3, zs[3], b_cols)
        project(3)
        sends.finish()

    sends = Sends()

    @pl.when(jnp.logical_not(is_edge))
    def _():
        outer = jnp.where(z == 1, 0, NZ - 1)
        inner = NZ - 1 - z
        start_gather([(0, outer), (1, inner)])
        z_wait_b(1)
        z_send_b(1, zs[1], 1, inner)
        for i in (x, xm, xp, xo):
            z_send_a(0, z, i, 1, inner)
        x_own(1, zs[1], b_cols, True)
        x_own(1, zs[1], b_cols, False)
        z_wait_b(2)
        z_send_b(2, zs[2], 0, outer)
        x_own(2, zs[2], b_cols, True)
        x_own(2, zs[2], b_cols, False)
        for c in range(1, 4):
            turn(c)
        x_rest(0, z, b_cols)
        project(0)
        z_wait_a(1)
        for i in range(NX):
            z_send_a(1, zs[1], i, 1, inner)
        z_wait_b(3)
        z_send_b(3, zs[3], 0, outer)
        x_forward(1, zs[1], b_cols)
        x_own(3, zs[3], b_cols, True)
        x_own(3, zs[3], b_cols, False)
        for c in range(4, 7):
            turn(c)
        x_forward(2, zs[2], b_cols)
        z_wait_a(2)
        for i in range(NX):
            z_send_a(2, zs[2], i, 0, outer)
        for c in range(7, TURNS):
            turn(c)
        x_rest(1, zs[1], b_cols)
        project(1)
        z_wait_a(3)
        for i in range(NX):
            z_send_a(3, zs[3], i, 0, outer)
        x_forward(3, zs[3], b_cols)
        x_rest(2, zs[2], b_cols)
        project(2)
        x_rest(3, zs[3], b_cols)
        project(3)
        sends.finish()

    hd = HEAD_SIZE
    last = (((1,), (1,)), ((), ()))

    def two_heads(ref, qt):
        return jnp.concatenate([ref[qt, :, 0:hd], ref[qt, :, hd : 2 * hd]], axis=0)

    row_at = lax.broadcasted_iota(jnp.int32, (hd, 2 * hd), 0)
    col_at = lax.broadcasted_iota(jnp.int32, (hd, 2 * hd), 1) % hd

    def scores(qt, c, q2, do2):
        j = qt + c
        raw = lax.dot_general(kv[j, :, 0:hd], q2, last, preferred_element_type=jnp.float32)
        bent = jnp.tanh(raw * (SCALE / CAP))
        expo = jnp.exp(CAP * bent)
        if c == 0:
            expo = jnp.where(row_at > col_at, expo, 0.0)
        if c == 5:
            expo = jnp.where(row_at <= col_at, expo, 0.0)
        if j < 5:
            expo = expo * jnp.where(s >= (1 if j > 0 else 2), 1.0, 0.0)
        d_probs = lax.dot_general(
            kv[j, :, hd : 2 * hd], do2, last, preferred_element_type=jnp.float32
        )
        e_buf[qt, c] = expo
        dp_buf[qt, c] = d_probs
        b_buf[qt, c] = bent
        shape = (hd // 8, 8, 2 * hd)
        return (
            jnp.sum(expo.reshape(shape), axis=0),
            jnp.sum((expo * d_probs).reshape(shape), axis=0),
        )

    def transpose_keys(j):
        kt[:, pl.ds(j * hd, hd)] = kv[j, :, 0:hd].astype(jnp.float32).T.astype(jnp.bfloat16)

    sums = []
    for qt in range(NX):
        q2, do2 = two_heads(qb, qt), two_heads(dout, qt)
        parts = [scores(qt, c, q2, do2) for c in range(5 - qt, 6)]
        sums.append((sum(p[0] for p in parts), sum(p[1] for p in parts)))
    for j in range(5, 9):
        transpose_keys(j)

    @pl.when(s > 0)
    def _():
        for k in range(NZ):
            near_copy(k, zs[k]).wait_recv()

    @pl.when(s > 1)
    def _():
        for k in range(NZ):
            far_copy(k, zs[k]).wait_recv()

    for j in range(5):
        transpose_keys(j)

    rest = []
    for qt in range(NX):
        q2, do2 = two_heads(qb, qt), two_heads(dout, qt)
        parts = [scores(qt, c, q2, do2) for c in range(0, 5 - qt)]
        norm = jnp.sum(sums[qt][0] + sum(p[0] for p in parts), axis=0, keepdims=True)
        inner = jnp.sum(sums[qt][1] + sum(p[1] for p in parts), axis=0, keepdims=True)
        inverse = 1.0 / norm
        rest.append((inverse, inner * inverse))

    def tile_grads(j):
        d_key = d_value = 0.0
        for qt in range(max(0, j - 5), min(NX, j + 1)):
            c = j - qt
            inverse, delta = rest[qt]
            probs = e_buf[qt, c] * inverse
            bent = b_buf[qt, c]
            d_raw = (
                probs * (dp_buf[qt, c] - delta) * (1.0 - bent * bent) * SCALE
            ).astype(jnp.bfloat16)
            dr_buf[qt, pl.ds(c * hd, hd), :] = d_raw
            d_key += jnp.dot(d_raw, two_heads(qb, qt), preferred_element_type=jnp.float32)
            d_value += jnp.dot(
                probs.astype(jnp.bfloat16), two_heads(dout, qt), preferred_element_type=jnp.float32
            )
        return d_key, d_value

    far_back = send_along(
        back_out.at[0], back_far, s_bf.at[0], r_bf.at[0], jnp.maximum(s - 2, 0)
    )
    near_back = [
        send_along(
            back_out.at[j], back_near.at[j - 1], s_bn.at[j - 1], r_bn.at[j - 1],
            jnp.maximum(s - 1, 0),
        )
        for j in range(1, 5)
    ]
    chip_back = send_along(
        back_out.at[0], back_chip, s_bc.at[0], r_bc.at[0], jnp.maximum(s - 1, 0)
    )
    is_odd = s % 2 == 1
    for j in range(5):
        d_key, d_value = tile_grads(j)
        back_out[j, :, 0:hd] = d_key.astype(jnp.bfloat16)
        back_out[j, :, hd : 2 * hd] = d_value.astype(jnp.bfloat16)
        if j == 0:
            pl.when(is_odd)(lambda: chip_back.start())
            pl.when((s > 1) & jnp.logical_not(is_odd))(lambda: far_back.start())
        elif j < 4:
            pl.when(s > 0)(lambda j=j: near_back[j - 1].start())
        else:

            @pl.when(jnp.logical_not(is_odd))
            def _():
                chip_back.wait_recv()
                other = back_chip[...].astype(jnp.float32)
                back_out[j, :, 0:hd] = (d_key + other[:, 0:hd]).astype(jnp.bfloat16)
                back_out[j, :, hd : 2 * hd] = (d_value + other[:, hd : 2 * hd]).astype(
                    jnp.bfloat16
                )

            pl.when(s > 0)(lambda: near_back[3].start())
    for j in range(5, 9):
        d_key, d_value = tile_grads(j)
        acc[j - 5, :, 0:hd] = d_key
        acc[j - 5, :, hd : 2 * hd] = d_value
    for qt in range(NX):
        d_query = jnp.dot(
            kt[:, pl.ds(qt * hd, 6 * hd)], dr_buf[qt], preferred_element_type=jnp.float32
        )
        grads[qt, :, 0:hd] = d_query[:, 0:hd].T.astype(jnp.bfloat16)
        grads[qt, :, hd : 2 * hd] = d_query[:, hd : 2 * hd].T.astype(jnp.bfloat16)

    @pl.when((s < blocks - 2) & jnp.logical_not(is_odd))
    def _():
        far_back.wait_recv()

    @pl.when(s < blocks - 1)
    def _():
        for i in range(NX):
            send_along(
                back_out.at[i + 1], back_near.at[i], s_bn.at[i], r_bn.at[i], s
            ).wait_recv()

    for i in range(NX):
        own = acc[i] + back_near[i].astype(jnp.float32)
        if i == NX - 1:
            own = own + back_far[...].astype(jnp.float32)
        grads[i, :, q_cols:] = own.astype(jnp.bfloat16)

    zs = zs[::-1]
    p = g
    tile = 768
    a_width = B_TILES * 128
    a_cols = pl.ds(0, a_width)
    b_cols = pl.ds(a_width, width - a_width)
    b_half = (width - a_width) // 2
    a_half = a_width // 2
    a_parts = [pl.ds(0, a_half), pl.ds(a_half, a_half)]
    b_parts = [pl.ds(a_width, b_half), pl.ds(a_width + b_half, b_half)]

    def row_ds(xr, h=None):
        if h is None:
            return pl.ds(pl.multiple_of(xr * rows, rows), rows)
        return pl.ds(pl.multiple_of(xr * rows + h * half, half), half)

    def compute(zr):
        lhs = grads[:, pl.ds(pl.multiple_of(zr * rows, rows), rows), :].reshape(NX * rows, -1)

        for j in range(width // tile):
            at = pl.ds(j * tile, tile)
            p[zr, :, at] = jnp.dot(
                lhs, wt[:, at], preferred_element_type=jnp.float32
            ).astype(jnp.bfloat16)

    def way(zr):
        return jnp.where(zr > z, 1, 0)

    def nearer(zr):
        return tp_of(x, jnp.where(zr > z, z + 1, z - 1))

    def step1(k, zr, cols):
        for direction, to in ((0, xm), (1, xp)):
            sends.start(
                send_to(
                    p.at[zr, row_ds(xo, direction), cols],
                    got_opp.at[direction, zr, :, cols],
                    s1.at[direction, k],
                    r1.at[direction, k],
                    tp_of(to, z),
                )
            )

    def step2(k, zr, parts):
        for direction, to in ((0, xm), (1, xp)):
            for cols in parts if len(parts) == 1 else [b_cols]:
                land = got_opp.at[direction, zr, :, cols]
                send_to(
                    land, land, s1.at[direction, k], r1.at[direction, k], tp_of(to, z)
                ).wait_recv()
            at = row_ds(to, direction)
            for h, cols in enumerate(parts):
                p[zr, at, cols] = (
                    p[zr, at, cols].astype(jnp.float32)
                    + got_opp[direction, zr, :, cols].astype(jnp.float32)
                ).astype(jnp.bfloat16)
                sends.start(
                    send_to(
                        p.at[zr, row_ds(to), cols],
                        got_x.at[direction, zr, :, cols],
                        s2.at[direction, k, h],
                        r2.at[direction, k, h],
                        tp_of(to, z),
                    )
                )

    def x_sum(k, h, zr, cols):
        for direction, to in ((0, xm), (1, xp)):
            land = got_x.at[direction, zr, :, cols]
            send_to(
                land, land, s2.at[direction, k, h], r2.at[direction, k, h], tp_of(to, z)
            ).wait_recv()
        return (
            p[zr, row_ds(x), cols].astype(jnp.float32)
            + got_x[0, zr, :, cols].astype(jnp.float32)
            + got_x[1, zr, :, cols].astype(jnp.float32)
        )

    def line_b(d, zr, h):
        return got_zb.at[d, zr, h]

    def line_wait_b(d, zr, h):
        land = line_b(d, zr, h)
        send_to(land, land, tzb.at[0, h], uzb.at[d, zr, h], tp_of(xp, z)).wait_recv()

    def line_wait_a(d, zr, h):
        land = got_za.at[d, zr, :, a_parts[h]]
        send_to(land, land, tza.at[0, h], uza.at[d, zr, h], tp_of(xp, z)).wait_recv()

    def step3(k, far):
        zr = zs[k]
        for h, cols in enumerate(b_parts):
            value = x_sum(k, h, zr, cols)
            if far:
                line_wait_b(way(zr), zr, h)
                value = value + got_zb[way(zr), zr, h].astype(jnp.float32)
            p[zr, row_ds(x), cols] = value.astype(jnp.bfloat16)
            sends.start(
                send_to(
                    p.at[zr, row_ds(x), cols], line_b(way(zr), zr, h), tzb.at[k, h],
                    uzb.at[way(zr), zr, h], nearer(zr),
                )
            )

    def add_a(d, zr, h):
        line_wait_a(d, zr, h)
        cols = a_parts[h]
        p[zr, :, cols] = (
            p[zr, :, cols].astype(jnp.float32) + got_za[d, zr, :, cols].astype(jnp.float32)
        ).astype(jnp.bfloat16)

    def line_a(k, far, when=None):
        zr = zs[k]
        for h, cols in enumerate(a_parts):
            if far:
                add_a(way(zr), zr, h)
            sends.start(
                send_to(
                    p.at[zr, :, cols], got_za.at[way(zr), zr, :, cols], tza.at[k, h],
                    uza.at[way(zr), zr, h], nearer(zr),
                ),
                when,
            )

    def finish(sources):
        for h, cols in enumerate(b_parts):
            value = x_sum(3, h, z, cols)
            for d in sources:
                line_wait_b(d, z, h)
                value = value + got_zb[d, z, h].astype(jnp.float32)
            total[:, cols] = value
        total[:, a_cols] = x_sum(4, 0, z, a_cols)
        values = tok[...].astype(jnp.float32)
        inv_rms = lax.rsqrt(jnp.mean(values * values, axis=1, keepdims=True) + EPS)
        upper = total[...] * gain_row()
        xhat = values * inv_rms
        out_ref[...] = (
            inv_rms * (upper - xhat * jnp.mean(upper * xhat, axis=1, keepdims=True))
        ).astype(jnp.bfloat16)
        sends.finish()

    sends = Sends()
    compute(zs[0])
    step1(0, zs[0], b_cols)
    line_a(0, False, is_edge)
    compute(zs[1])
    step1(1, zs[1], b_cols)
    line_a(1, False, is_edge)
    compute(zs[2])
    line_a(2, False, is_edge)
    compute(z)
    opening, sends = sends, Sends()

    @pl.when(is_edge)
    def _():
        source = jnp.where(z == 0, 0, 1)
        step2(0, zs[0], b_parts)
        step1(2, zs[2], b_cols)
        step2(1, zs[1], b_parts)
        step1(3, z, b_cols)
        step2(2, zs[2], b_parts)
        step3(0, False)
        step3(1, False)
        add_a(source, z, 0)
        add_a(source, z, 1)
        step1(4, z, a_cols)
        step2(3, z, b_parts)
        step3(2, False)
        step2(4, z, [a_cols])
        finish([source])

    sends = Sends()

    @pl.when(jnp.logical_not(is_edge))
    def _():
        step2(0, zs[0], b_parts)
        step1(2, zs[2], b_cols)
        line_a(0, True)
        step2(1, zs[1], b_parts)
        step1(3, z, b_cols)
        line_a(1, True)
        step2(2, zs[2], b_parts)
        line_a(2, True)
        for d in (0, 1):
            for h in (0, 1):
                add_a(d, z, h)
        step1(4, z, a_cols)
        step3(0, True)
        step2(3, z, b_parts)
        step3(2, True)
        step3(1, True)
        step2(4, z, [a_cols])
        finish([0, 1])

    opening.finish()

    @pl.when(s > 0)
    def _():
        for copy in near_back:
            copy.wait_send()

    @pl.when((s > 1) & jnp.logical_not(is_odd))
    def _():
        far_back.wait_send()

    @pl.when(is_odd)
    def _():
        chip_back.wait_send()

    @pl.when(s + 1 < blocks)
    def _():
        for k in range(NZ):
            near_copy(k, zs[NZ - 1 - k]).wait_send()

    @pl.when(s + 2 < blocks)
    def _():
        for k in range(NZ):
            far_copy(k, zs[NZ - 1 - k]).wait_send()


def on_device(tokens, norm_gain, query_weight, key_matrix, value_matrix, output_grad):
    rows, width = tokens.shape
    q_cols, k_cols = query_weight.shape[1], key_matrix.shape[1]
    cols = q_cols + 2 * k_cols
    a_width = B_TILES * 128
    hd = HEAD_SIZE
    any_space = pl.BlockSpec(memory_space=pltpu.HBM)
    dma = pltpu.SemaphoreType.DMA
    low, full = jnp.bfloat16, jnp.float32

    def vmem(kind, *shape):
        return pltpu.VMEM(shape, kind)

    return pl.pallas_call(
        whole,
        out_shape=jax.ShapeDtypeStruct((rows, width), low),
        in_specs=[any_space] * 6,
        out_specs=pl.BlockSpec(memory_space=pltpu.VMEM),
        scratch_shapes=[
            vmem(low, rows, width),
            vmem(full, width // 128, 128),
            vmem(low, width, cols),
            vmem(low, cols, width),
            vmem(low, NZ, NX * rows, width),
            vmem(low, NX, hd, q_cols),
            vmem(low, NX, hd, q_cols),
            vmem(low, 9, hd, 2 * k_cols),
            vmem(low, hd, 9 * hd),
            vmem(full, NX, 6, hd, 2 * hd),
            vmem(full, NX, 6, hd, 2 * hd),
            vmem(full, NX, 6, hd, 2 * hd),
            vmem(low, NX, 6 * hd, 2 * hd),
            vmem(full, NX, hd, 2 * k_cols),
            vmem(low, 5, hd, 2 * k_cols),
            vmem(low, NX, hd, 2 * k_cols),
            vmem(low, hd, 2 * k_cols),
            vmem(low, hd, 2 * k_cols),
            vmem(low, NX, hd, cols),
            vmem(full, rows, width),
            vmem(low, 2, NZ, rows // 2, width),
            vmem(low, 2, NZ, rows, width),
            vmem(low, 2, NZ, NX * rows, a_width),
            vmem(low, 2, NZ, 2, rows, (width - a_width) // 2),
            dma((6,)),
            dma((2, NZ + 1, 3)),
            dma((2, NZ, NX, 2)),
            dma((2, NZ)),
            dma((NZ,)),
            dma((2, NZ, NX)),
            dma((NZ, NX)),
            dma((NZ,)),
            dma((NZ,)),
            dma((NZ,)),
            dma((NZ,)),
            dma((NX,)),
            dma((NX,)),
            dma((1,)),
            dma((1,)),
            dma((1,)),
            dma((1,)),
            dma((2, NZ + 1)),
            dma((2, NZ + 1)),
            dma((2, NZ + 1, 2)),
            dma((2, NZ + 1, 2)),
            dma((NZ, 2)),
            dma((2, NZ, 2)),
            dma((NZ, 2)),
            dma((2, NZ, 2)),
        ],
        compiler_params=pltpu.CompilerParams(
            collective_id=0, has_side_effects=True, vmem_limit_bytes=62 * 1024 * 1024
        ),
    )(
        tokens,
        norm_gain.reshape(-1, 128),
        output_grad.reshape(NX, hd, q_cols),
        query_weight,
        key_matrix,
        value_matrix,
    )


def solution(mesh):
    tp, both = "tp", ("seq", "tp")
    in_specs = (P(both, None), P(), P(None, tp), P(None, tp), P(None, tp), P("seq", tp))
    return jax.shard_map(
        on_device, mesh=mesh, in_specs=in_specs, out_specs=P(both, None), check_vma=False
    )
```

```python
import jax
import jax.numpy as jnp
from jax import lax
from jax.experimental import pallas as pl
from jax.experimental.pallas import tpu as pltpu
from jax.sharding import PartitionSpec as P

HEAD_SIZE = 128
WINDOW = 640
SCALE = 1.0 / 12.0
CAP = 50.0
EPS = 1e-06
MESH = pl.DeviceIdType.MESH
NX = 4
NZ = 4
A_TILES = 5
B_TILES = 8
TURN = 512
TURNS = 9


def place():
    t = lax.axis_index("tp")
    return t // NZ, t % NZ


def near_to_far(z):
    def high(q):
        return (q, 5 - q, jnp.int32(1), jnp.int32(0))

    up = high(z)
    low = high(3 - z)
    return [jnp.where(z >= 2, u, 3 - v) for u, v in zip(up, low)]


def send_to(src, dst, send_sem, recv_sem, tp):
    return pltpu.make_async_remote_copy(
        src_ref=src,
        dst_ref=dst,
        send_sem=send_sem,
        recv_sem=recv_sem,
        device_id={"tp": tp},
        device_id_type=MESH,
    )


def tp_of(x, z):
    return x * NZ + z


def send_along(src, dst, send_sem, recv_sem, seq):
    return pltpu.make_async_remote_copy(
        src_ref=src,
        dst_ref=dst,
        send_sem=send_sem,
        recv_sem=recv_sem,
        device_id={"seq": seq},
        device_id_type=MESH,
    )


def greet(device):
    barrier = pltpu.get_barrier_semaphore()
    pl.semaphore_signal(barrier, inc=1, device_id=device, device_id_type=MESH)


def meet(x, z, s, blocks):
    barrier = pltpu.get_barrier_semaphore()
    early = (s // 2) % 2 == 0
    greet({"tp": tp_of((x + 1) % NX, z)})
    greet({"tp": tp_of((x + 3) % NX, z)})
    pl.when(z > 0)(lambda: greet({"tp": tp_of(x, z - 1)}))
    pl.when(z < NZ - 1)(lambda: greet({"tp": tp_of(x, z + 1)}))
    greet({"seq": s + 1 - 2 * (s % 2)})
    near = jnp.where((z == 0) | (z == NZ - 1), 4, 5)
    others = [s - 2, s + 2, s - 1 + 2 * (s % 2)]
    there = [(o >= 0) & (o < blocks) for o in others]
    far = sum(jnp.where(t, 1, 0) for t in there)

    def first():
        pl.semaphore_wait(barrier, near + jnp.where(early, 0, far))
        for o, t in zip(others, there):
            pl.when(t)(lambda o=o: greet({"seq": o}))

    def second():
        pl.when(early)(lambda: pl.semaphore_wait(barrier, far))

    return first, second


class Sends:
    def __init__(self):
        self.started = []

    def start(self, copy, when=None):
        self.started.append((copy, when))
        if when is None:
            copy.start()
        else:
            pl.when(when)(lambda: copy.start())

    def finish(self):
        for copy, when in self.started:
            if when is None:
                copy.wait_send()
            else:
                pl.when(when)(lambda copy=copy: copy.wait_send())


def whole(
    tokens_ref, gain_ref, grad_ref, wq_ref, wk_ref, wv_ref, out_ref,
    tok, gain, w, wt, g, dout, qb, kv, kt, e_buf, dp_buf, b_buf, dr_buf, acc,
    back_out, back_near, back_far, back_chip, grads, total, got_opp, got_x, got_za, got_zb,
    load_sem, sx, rx, szb, rzb, sza, rza, s_near, r_near, s_far, r_far,
    s_bn, r_bn, s_bf, r_bf, s_bc, r_bc, s1, r1, s2, r2, tza, uza, tzb, uzb,
):
    x, z = place()
    s = lax.axis_index("seq")
    blocks = lax.axis_size("seq")
    rows, width = tok.shape
    half = rows // 2
    a_width = A_TILES * 128
    a_cols = pl.ds(0, a_width)
    b_cols = pl.ds(a_width, width - a_width)
    xp, xm, xo = (x + 1) % NX, (x + 3) % NX, (x + 2) % NX
    zs = near_to_far(z)
    q_cols, k_cols = wq_ref.shape[1], wk_ref.shape[1]
    meet_first, meet_second = meet(x, z, s, blocks)
    loads = [
        pltpu.make_async_copy(tokens_ref, tok, load_sem.at[0]),
        pltpu.make_async_copy(gain_ref, gain, load_sem.at[1]),
        pltpu.make_async_copy(wq_ref, w.at[:, pl.ds(0, q_cols)], load_sem.at[2]),
        pltpu.make_async_copy(wk_ref, w.at[:, pl.ds(q_cols, k_cols)], load_sem.at[3]),
        pltpu.make_async_copy(wv_ref, w.at[:, pl.ds(q_cols + k_cols, k_cols)], load_sem.at[4]),
        pltpu.make_async_copy(grad_ref, dout, load_sem.at[5]),
    ]
    for load in loads:
        load.start()
    loads[0].wait()
    loads[1].wait()

    def gain_row():
        return jnp.concatenate([gain[i : i + 1, :] for i in range(gain.shape[0])], axis=1)

    values = tok[...].astype(jnp.float32)
    inv_rms = lax.rsqrt(jnp.mean(values * values, axis=1, keepdims=True) + EPS)
    g[z, pl.ds(x * rows, rows), :] = (values * inv_rms * gain_row()).astype(jnp.bfloat16)
    meet_first()
    sends = Sends()

    def part(zr, xr, h, cols):
        if h is None:
            return g.at[zr, pl.ds(pl.multiple_of(xr * rows, rows), rows), cols]
        return g.at[zr, pl.ds(pl.multiple_of(xr * rows + h * half, half), half), cols]

    def x_send(k, zr, xr, h, cols, to, direction, slot):
        piece = part(zr, xr, h, cols)
        p = 1 if k == NZ else 0
        sends.start(
            send_to(piece, piece, sx.at[direction, k, slot], rx.at[p, zr, xr, h], tp_of(to, z))
        )

    def x_wait(k, zr, xr, h, cols):
        piece = part(zr, xr, h, cols)
        p = 1 if k == NZ else 0
        send_to(piece, piece, sx.at[0, k, 0], rx.at[p, zr, xr, h], tp_of(xp, z)).wait_recv()

    def x_own(k, zr, cols, first):
        h_right, h_left = (0, 1) if first else (1, 0)
        slot = 0 if first else 1
        x_send(k, zr, x, h_right, cols, xp, 0, slot)
        x_send(k, zr, x, h_left, cols, xm, 1, slot)

    def x_forward(k, zr, cols):
        x_wait(k, zr, xm, 0, cols)
        x_send(k, zr, xm, 0, cols, xp, 0, 2)
        x_wait(k, zr, xp, 1, cols)
        x_send(k, zr, xp, 1, cols, xm, 1, 2)

    def x_rest_near(k, zr, cols):
        x_wait(k, zr, xm, 1, cols)
        x_wait(k, zr, xp, 0, cols)

    def x_rest_opposite(k, zr, cols):
        x_wait(k, zr, xo, 0, cols)
        x_wait(k, zr, xo, 1, cols)

    def x_rest(k, zr, cols):
        x_rest_near(k, zr, cols)
        x_rest_opposite(k, zr, cols)

    def z_send_b(k, zr, way, to):
        piece = part(zr, x, None, b_cols)
        sends.start(send_to(piece, piece, szb.at[way, k], rzb.at[zr], tp_of(x, to)))

    def z_send_a(k, zr, xr, way, to):
        piece = part(zr, xr, None, a_cols)
        sends.start(
            send_to(piece, piece, sza.at[way, k, xr], rza.at[zr, xr], tp_of(x, to))
        )

    def z_wait_b(k):
        piece = part(zs[k], x, None, b_cols)
        send_to(piece, piece, szb.at[0, 0], rzb.at[zs[k]], tp_of(xp, z)).wait_recv()

    def z_wait_a(k):
        for i in range(NX):
            piece = part(zs[k], i, None, a_cols)
            send_to(piece, piece, sza.at[0, 0, i], rza.at[zs[k], i], tp_of(xp, z)).wait_recv()

    def turn(c):
        at = pl.ds(c * TURN, TURN)
        wt[:, at] = w[at, :].T

    def slab(first, count, zr):
        return kv.at[pl.ds(first, count), pl.ds(pl.multiple_of(zr * rows, rows), rows), :]

    def near_copy(k, zr):
        return send_along(
            slab(5, 4, zr), slab(1, 4, zr), s_near.at[k], r_near.at[k],
            jnp.minimum(s + 1, blocks - 1),
        )

    def far_copy(k, zr):
        return send_along(
            slab(8, 1, zr), slab(0, 1, zr), s_far.at[k], r_far.at[k],
            jnp.minimum(s + 2, blocks - 1),
        )

    def project(k):
        zr = zs[k]
        out = jnp.dot(g[zr], w[...], preferred_element_type=jnp.float32).astype(jnp.bfloat16)
        at = pl.ds(pl.multiple_of(zr * rows, rows), rows)
        for i in range(NX):
            kv[5 + i, at, :] = out[i * rows : (i + 1) * rows, q_cols:]
            qb[i, at, :] = out[i * rows : (i + 1) * rows, :q_cols]
        pl.when(s + 2 < blocks)(lambda: far_copy(k, zr).start())
        pl.when(s + 1 < blocks)(lambda: near_copy(k, zr).start())

    is_edge = (z == 0) | (z == NZ - 1)

    def start_gather(neighbours):
        x_own(NZ, z, a_cols, True)
        x_own(NZ, z, a_cols, False)
        for way, to in neighbours:
            z_send_b(0, z, way, to)
        x_own(0, z, b_cols, True)
        x_forward(NZ, z, a_cols)
        x_own(0, z, b_cols, False)
        way, to = neighbours[0]
        x_rest_near(NZ, z, a_cols)
        for i in (x, xm, xp):
            z_send_a(0, z, i, way, to)
        for load in loads[2:]:
            load.wait()
        clear_edges()
        turn(0)
        x_rest_opposite(NZ, z, a_cols)
        z_send_a(0, z, xo, way, to)
        x_forward(0, z, b_cols)
        meet_second()

    def clear_edges():
        @pl.when(s == 0)
        def _():
            kv[0:5] = jnp.zeros_like(kv[0:5])

        @pl.when(s == 1)
        def _():
            kv[0] = jnp.zeros_like(kv[0])

        @pl.when(s == blocks - 1)
        def _():
            back_near[...] = jnp.zeros_like(back_near)

        @pl.when((s >= blocks - 2) | (s % 2 == 1))
        def _():
            back_far[...] = jnp.zeros_like(back_far)

    @pl.when(is_edge)
    def _():
        start_gather([(0, jnp.where(z == 0, 1, NZ - 2))])
        z_wait_b(1)
        x_own(1, zs[1], b_cols, True)
        x_own(1, zs[1], b_cols, False)
        for c in range(1, 5):
            turn(c)
        x_rest(0, z, b_cols)
        project(0)
        x_forward(1, zs[1], b_cols)
        turn(5)
        z_wait_b(2)
        x_own(2, zs[2], b_cols, True)
        x_own(2, zs[2], b_cols, False)
        z_wait_a(1)
        x_rest(1, zs[1], b_cols)
        project(1)
        x_forward(2, zs[2], b_cols)
        z_wait_b(3)
        x_own(3, zs[3], b_cols, True)
        x_own(3, zs[3], b_cols, False)
        for c in range(6, TURNS):
            turn(c)
        z_wait_a(2)
        x_rest(2, zs[2], b_cols)
        project(2)
        x_forward(3, zs[3], b_cols)
        z_wait_a(3)
        x_rest(3, zs[3], b_cols)
        project(3)
        sends.finish()

    sends = Sends()

    @pl.when(jnp.logical_not(is_edge))
    def _():
        outer = jnp.where(z == 1, 0, NZ - 1)
        inner = NZ - 1 - z
        start_gather([(0, outer), (1, inner)])
        z_wait_b(1)
        z_send_b(1, zs[1], 1, inner)
        for i in (x, xm, xp, xo):
            z_send_a(0, z, i, 1, inner)
        x_own(1, zs[1], b_cols, True)
        x_own(1, zs[1], b_cols, False)
        z_wait_b(2)
        z_send_b(2, zs[2], 0, outer)
        x_own(2, zs[2], b_cols, True)
        x_own(2, zs[2], b_cols, False)
        for c in range(1, 4):
            turn(c)
        x_rest(0, z, b_cols)
        project(0)
        z_wait_a(1)
        for i in range(NX):
            z_send_a(1, zs[1], i, 1, inner)
        z_wait_b(3)
        z_send_b(3, zs[3], 0, outer)
        x_forward(1, zs[1], b_cols)
        x_own(3, zs[3], b_cols, True)
        x_own(3, zs[3], b_cols, False)
        for c in range(4, 7):
            turn(c)
        x_forward(2, zs[2], b_cols)
        z_wait_a(2)
        for i in range(NX):
            z_send_a(2, zs[2], i, 0, outer)
        for c in range(7, TURNS):
            turn(c)
        x_rest(1, zs[1], b_cols)
        project(1)
        z_wait_a(3)
        for i in range(NX):
            z_send_a(3, zs[3], i, 0, outer)
        x_forward(3, zs[3], b_cols)
        x_rest(2, zs[2], b_cols)
        project(2)
        x_rest(3, zs[3], b_cols)
        project(3)
        sends.finish()

    hd = HEAD_SIZE
    last = (((1,), (1,)), ((), ()))

    def two_heads(ref, qt):
        return jnp.concatenate([ref[qt, :, 0:hd], ref[qt, :, hd : 2 * hd]], axis=0)

    row_at = lax.broadcasted_iota(jnp.int32, (hd, 2 * hd), 0)
    col_at = lax.broadcasted_iota(jnp.int32, (hd, 2 * hd), 1) % hd

    def scores(qt, c, q2, do2):
        j = qt + c
        raw = lax.dot_general(kv[j, :, 0:hd], q2, last, preferred_element_type=jnp.float32)
        bent = jnp.tanh(raw * (SCALE / CAP))
        expo = jnp.exp(CAP * bent)
        if c == 0:
            expo = jnp.where(row_at > col_at, expo, 0.0)
        if c == 5:
            expo = jnp.where(row_at <= col_at, expo, 0.0)
        if j < 5:
            expo = expo * jnp.where(s >= (1 if j > 0 else 2), 1.0, 0.0)
        d_probs = lax.dot_general(
            kv[j, :, hd : 2 * hd], do2, last, preferred_element_type=jnp.float32
        )
        e_buf[qt, c] = expo
        dp_buf[qt, c] = d_probs
        b_buf[qt, c] = bent
        shape = (hd // 8, 8, 2 * hd)
        return (
            jnp.sum(expo.reshape(shape), axis=0),
            jnp.sum((expo * d_probs).reshape(shape), axis=0),
        )

    def transpose_keys(j):
        kt[:, pl.ds(j * hd, hd)] = kv[j, :, 0:hd].astype(jnp.float32).T.astype(jnp.bfloat16)

    sums = []
    for qt in range(NX):
        q2, do2 = two_heads(qb, qt), two_heads(dout, qt)
        parts = [scores(qt, c, q2, do2) for c in range(5 - qt, 6)]
        sums.append((sum(p[0] for p in parts), sum(p[1] for p in parts)))
    for j in range(5, 9):
        transpose_keys(j)

    @pl.when(s > 0)
    def _():
        for k in range(NZ):
            near_copy(k, zs[k]).wait_recv()

    @pl.when(s > 1)
    def _():
        for k in range(NZ):
            far_copy(k, zs[k]).wait_recv()

    for j in range(5):
        transpose_keys(j)

    rest = []
    for qt in range(NX):
        q2, do2 = two_heads(qb, qt), two_heads(dout, qt)
        parts = [scores(qt, c, q2, do2) for c in range(0, 5 - qt)]
        norm = jnp.sum(sums[qt][0] + sum(p[0] for p in parts), axis=0, keepdims=True)
        inner = jnp.sum(sums[qt][1] + sum(p[1] for p in parts), axis=0, keepdims=True)
        inverse = 1.0 / norm
        rest.append((inverse, inner * inverse))

    def tile_grads(j):
        d_key = d_value = 0.0
        for qt in range(max(0, j - 5), min(NX, j + 1)):
            c = j - qt
            inverse, delta = rest[qt]
            probs = e_buf[qt, c] * inverse
            bent = b_buf[qt, c]
            d_raw = (
                probs * (dp_buf[qt, c] - delta) * (1.0 - bent * bent) * SCALE
            ).astype(jnp.bfloat16)
            dr_buf[qt, pl.ds(c * hd, hd), :] = d_raw
            d_key += jnp.dot(d_raw, two_heads(qb, qt), preferred_element_type=jnp.float32)
            d_value += jnp.dot(
                probs.astype(jnp.bfloat16), two_heads(dout, qt), preferred_element_type=jnp.float32
            )
        return d_key, d_value

    far_back = send_along(
        back_out.at[0], back_far, s_bf.at[0], r_bf.at[0], jnp.maximum(s - 2, 0)
    )
    near_back = [
        send_along(
            back_out.at[j], back_near.at[j - 1], s_bn.at[j - 1], r_bn.at[j - 1],
            jnp.maximum(s - 1, 0),
        )
        for j in range(1, 5)
    ]
    chip_back = send_along(
        back_out.at[0], back_chip, s_bc.at[0], r_bc.at[0], jnp.maximum(s - 1, 0)
    )
    is_odd = s % 2 == 1
    for j in range(5):
        d_key, d_value = tile_grads(j)
        back_out[j, :, 0:hd] = d_key.astype(jnp.bfloat16)
        back_out[j, :, hd : 2 * hd] = d_value.astype(jnp.bfloat16)
        if j == 0:
            pl.when(is_odd)(lambda: chip_back.start())
            pl.when((s > 1) & jnp.logical_not(is_odd))(lambda: far_back.start())
        elif j < 4:
            pl.when(s > 0)(lambda j=j: near_back[j - 1].start())
        else:

            @pl.when(jnp.logical_not(is_odd))
            def _():
                chip_back.wait_recv()
                other = back_chip[...].astype(jnp.float32)
                back_out[j, :, 0:hd] = (d_key + other[:, 0:hd]).astype(jnp.bfloat16)
                back_out[j, :, hd : 2 * hd] = (d_value + other[:, hd : 2 * hd]).astype(
                    jnp.bfloat16
                )

            pl.when(s > 0)(lambda: near_back[3].start())
    for j in range(5, 9):
        d_key, d_value = tile_grads(j)
        acc[j - 5, :, 0:hd] = d_key
        acc[j - 5, :, hd : 2 * hd] = d_value
    for qt in range(NX):
        d_query = jnp.dot(
            kt[:, pl.ds(qt * hd, 6 * hd)], dr_buf[qt], preferred_element_type=jnp.float32
        )
        grads[qt, :, 0:hd] = d_query[:, 0:hd].T.astype(jnp.bfloat16)
        grads[qt, :, hd : 2 * hd] = d_query[:, hd : 2 * hd].T.astype(jnp.bfloat16)

    @pl.when((s < blocks - 2) & jnp.logical_not(is_odd))
    def _():
        far_back.wait_recv()

    @pl.when(s < blocks - 1)
    def _():
        for i in range(NX):
            send_along(
                back_out.at[i + 1], back_near.at[i], s_bn.at[i], r_bn.at[i], s
            ).wait_recv()

    for i in range(NX):
        own = acc[i] + back_near[i].astype(jnp.float32)
        if i == NX - 1:
            own = own + back_far[...].astype(jnp.float32)
        grads[i, :, q_cols:] = own.astype(jnp.bfloat16)

    zs = zs[::-1]
    p = g
    tile = 768
    a_width = B_TILES * 128
    a_cols = pl.ds(0, a_width)
    b_cols = pl.ds(a_width, width - a_width)
    b_half = (width - a_width) // 2
    a_half = a_width // 2
    a_parts = [pl.ds(0, a_half), pl.ds(a_half, a_half)]
    b_parts = [pl.ds(a_width, b_half), pl.ds(a_width + b_half, b_half)]

    def row_ds(xr, h=None):
        if h is None:
            return pl.ds(pl.multiple_of(xr * rows, rows), rows)
        return pl.ds(pl.multiple_of(xr * rows + h * half, half), half)

    def compute(zr):
        lhs = grads[:, pl.ds(pl.multiple_of(zr * rows, rows), rows), :].reshape(NX * rows, -1)

        for j in range(width // tile):
            at = pl.ds(j * tile, tile)
            p[zr, :, at] = jnp.dot(
                lhs, wt[:, at], preferred_element_type=jnp.float32
            ).astype(jnp.bfloat16)

    def way(zr):
        return jnp.where(zr > z, 1, 0)

    def nearer(zr):
        return tp_of(x, jnp.where(zr > z, z + 1, z - 1))

    def step1(k, zr, cols):
        for direction, to in ((0, xm), (1, xp)):
            sends.start(
                send_to(
                    p.at[zr, row_ds(xo, direction), cols],
                    got_opp.at[direction, zr, :, cols],
                    s1.at[direction, k],
                    r1.at[direction, k],
                    tp_of(to, z),
                )
            )

    def step2(k, zr, parts):
        for direction, to in ((0, xm), (1, xp)):
            for cols in parts if len(parts) == 1 else [b_cols]:
                land = got_opp.at[direction, zr, :, cols]
                send_to(
                    land, land, s1.at[direction, k], r1.at[direction, k], tp_of(to, z)
                ).wait_recv()
            at = row_ds(to, direction)
            for h, cols in enumerate(parts):
                p[zr, at, cols] = (
                    p[zr, at, cols].astype(jnp.float32)
                    + got_opp[direction, zr, :, cols].astype(jnp.float32)
                ).astype(jnp.bfloat16)
                sends.start(
                    send_to(
                        p.at[zr, row_ds(to), cols],
                        got_x.at[direction, zr, :, cols],
                        s2.at[direction, k, h],
                        r2.at[direction, k, h],
                        tp_of(to, z),
                    )
                )

    def x_sum(k, h, zr, cols):
        for direction, to in ((0, xm), (1, xp)):
            land = got_x.at[direction, zr, :, cols]
            send_to(
                land, land, s2.at[direction, k, h], r2.at[direction, k, h], tp_of(to, z)
            ).wait_recv()
        return (
            p[zr, row_ds(x), cols].astype(jnp.float32)
            + got_x[0, zr, :, cols].astype(jnp.float32)
            + got_x[1, zr, :, cols].astype(jnp.float32)
        )

    def line_b(d, zr, h):
        return got_zb.at[d, zr, h]

    def line_wait_b(d, zr, h):
        land = line_b(d, zr, h)
        send_to(land, land, tzb.at[0, h], uzb.at[d, zr, h], tp_of(xp, z)).wait_recv()

    def line_wait_a(d, zr, h):
        land = got_za.at[d, zr, :, a_parts[h]]
        send_to(land, land, tza.at[0, h], uza.at[d, zr, h], tp_of(xp, z)).wait_recv()

    def step3(k, far):
        zr = zs[k]
        for h, cols in enumerate(b_parts):
            value = x_sum(k, h, zr, cols)
            if far:
                line_wait_b(way(zr), zr, h)
                value = value + got_zb[way(zr), zr, h].astype(jnp.float32)
            p[zr, row_ds(x), cols] = value.astype(jnp.bfloat16)
            sends.start(
                send_to(
                    p.at[zr, row_ds(x), cols], line_b(way(zr), zr, h), tzb.at[k, h],
                    uzb.at[way(zr), zr, h], nearer(zr),
                )
            )

    def add_a(d, zr, h):
        line_wait_a(d, zr, h)
        cols = a_parts[h]
        p[zr, :, cols] = (
            p[zr, :, cols].astype(jnp.float32) + got_za[d, zr, :, cols].astype(jnp.float32)
        ).astype(jnp.bfloat16)

    def line_a(k, far, when=None):
        zr = zs[k]
        for h, cols in enumerate(a_parts):
            if far:
                add_a(way(zr), zr, h)
            sends.start(
                send_to(
                    p.at[zr, :, cols], got_za.at[way(zr), zr, :, cols], tza.at[k, h],
                    uza.at[way(zr), zr, h], nearer(zr),
                ),
                when,
            )

    def finish(sources):
        for h, cols in enumerate(b_parts):
            value = x_sum(3, h, z, cols)
            for d in sources:
                line_wait_b(d, z, h)
                value = value + got_zb[d, z, h].astype(jnp.float32)
            total[:, cols] = value
        total[:, a_cols] = x_sum(4, 0, z, a_cols)
        values = tok[...].astype(jnp.float32)
        inv_rms = lax.rsqrt(jnp.mean(values * values, axis=1, keepdims=True) + EPS)
        upper = total[...] * gain_row()
        xhat = values * inv_rms
        out_ref[...] = (
            inv_rms * (upper - xhat * jnp.mean(upper * xhat, axis=1, keepdims=True))
        ).astype(jnp.bfloat16)
        sends.finish()

    sends = Sends()
    compute(zs[0])
    step1(0, zs[0], b_cols)
    line_a(0, False, is_edge)
    compute(zs[1])
    step1(1, zs[1], b_cols)
    line_a(1, False, is_edge)
    compute(zs[2])
    line_a(2, False, is_edge)
    compute(z)
    opening, sends = sends, Sends()

    @pl.when(is_edge)
    def _():
        source = jnp.where(z == 0, 0, 1)
        step2(0, zs[0], b_parts)
        step2(1, zs[1], b_parts)
        step1(2, zs[2], b_cols)
        step1(3, z, b_cols)
        step3(0, False)
        step3(1, False)
        step2(2, zs[2], b_parts)
        add_a(source, z, 0)
        add_a(source, z, 1)
        step1(4, z, a_cols)
        step2(3, z, b_parts)
        step3(2, False)
        step2(4, z, [a_cols])
        finish([source])

    sends = Sends()

    @pl.when(jnp.logical_not(is_edge))
    def _():
        step2(0, zs[0], b_parts)
        step2(1, zs[1], b_parts)
        step1(2, zs[2], b_cols)
        step1(3, z, b_cols)
        line_a(0, True)
        line_a(1, True)
        line_a(2, True)
        step3(0, True)
        step2(2, zs[2], b_parts)
        for d in (0, 1):
            for h in (0, 1):
                add_a(d, z, h)
        step1(4, z, a_cols)
        step2(3, z, b_parts)
        step3(1, True)
        step3(2, True)
        step2(4, z, [a_cols])
        finish([0, 1])

    opening.finish()

    @pl.when(s > 0)
    def _():
        for copy in near_back:
            copy.wait_send()

    @pl.when((s > 1) & jnp.logical_not(is_odd))
    def _():
        far_back.wait_send()

    @pl.when(is_odd)
    def _():
        chip_back.wait_send()

    @pl.when(s + 1 < blocks)
    def _():
        for k in range(NZ):
            near_copy(k, zs[NZ - 1 - k]).wait_send()

    @pl.when(s + 2 < blocks)
    def _():
        for k in range(NZ):
            far_copy(k, zs[NZ - 1 - k]).wait_send()


def on_device(tokens, norm_gain, query_weight, key_matrix, value_matrix, output_grad):
    rows, width = tokens.shape
    q_cols, k_cols = query_weight.shape[1], key_matrix.shape[1]
    cols = q_cols + 2 * k_cols
    a_width = B_TILES * 128
    hd = HEAD_SIZE
    any_space = pl.BlockSpec(memory_space=pltpu.HBM)
    dma = pltpu.SemaphoreType.DMA
    low, full = jnp.bfloat16, jnp.float32

    def vmem(kind, *shape):
        return pltpu.VMEM(shape, kind)

    return pl.pallas_call(
        whole,
        out_shape=jax.ShapeDtypeStruct((rows, width), low),
        in_specs=[any_space] * 6,
        out_specs=pl.BlockSpec(memory_space=pltpu.VMEM),
        scratch_shapes=[
            vmem(low, rows, width),
            vmem(full, width // 128, 128),
            vmem(low, width, cols),
            vmem(low, cols, width),
            vmem(low, NZ, NX * rows, width),
            vmem(low, NX, hd, q_cols),
            vmem(low, NX, hd, q_cols),
            vmem(low, 9, hd, 2 * k_cols),
            vmem(low, hd, 9 * hd),
            vmem(full, NX, 6, hd, 2 * hd),
            vmem(full, NX, 6, hd, 2 * hd),
            vmem(full, NX, 6, hd, 2 * hd),
            vmem(low, NX, 6 * hd, 2 * hd),
            vmem(full, NX, hd, 2 * k_cols),
            vmem(low, 5, hd, 2 * k_cols),
            vmem(low, NX, hd, 2 * k_cols),
            vmem(low, hd, 2 * k_cols),
            vmem(low, hd, 2 * k_cols),
            vmem(low, NX, hd, cols),
            vmem(full, rows, width),
            vmem(low, 2, NZ, rows // 2, width),
            vmem(low, 2, NZ, rows, width),
            vmem(low, 2, NZ, NX * rows, a_width),
            vmem(low, 2, NZ, 2, rows, (width - a_width) // 2),
            dma((6,)),
            dma((2, NZ + 1, 3)),
            dma((2, NZ, NX, 2)),
            dma((2, NZ)),
            dma((NZ,)),
            dma((2, NZ, NX)),
            dma((NZ, NX)),
            dma((NZ,)),
            dma((NZ,)),
            dma((NZ,)),
            dma((NZ,)),
            dma((NX,)),
            dma((NX,)),
            dma((1,)),
            dma((1,)),
            dma((1,)),
            dma((1,)),
            dma((2, NZ + 1)),
            dma((2, NZ + 1)),
            dma((2, NZ + 1, 2)),
            dma((2, NZ + 1, 2)),
            dma((NZ, 2)),
            dma((2, NZ, 2)),
            dma((NZ, 2)),
            dma((2, NZ, 2)),
        ],
        compiler_params=pltpu.CompilerParams(
            collective_id=0, has_side_effects=True, vmem_limit_bytes=62 * 1024 * 1024
        ),
    )(
        tokens,
        norm_gain.reshape(-1, 128),
        output_grad.reshape(NX, hd, q_cols),
        query_weight,
        key_matrix,
        value_matrix,
    )


def solution(mesh):
    tp, both = "tp", ("seq", "tp")
    in_specs = (P(both, None), P(), P(None, tp), P(None, tp), P(None, tp), P("seq", tp))
    return jax.shard_map(
        on_device, mesh=mesh, in_specs=in_specs, out_specs=P(both, None), check_vma=False
    )
```

```python
import jax
import jax.numpy as jnp
from jax import lax
from jax.experimental import pallas as pl
from jax.experimental.pallas import tpu as pltpu
from jax.sharding import PartitionSpec as P

HEAD_SIZE = 128
WINDOW = 640
SCALE = 1.0 / 12.0
CAP = 50.0
EPS = 1e-06
MESH = pl.DeviceIdType.MESH
NX = 4
NZ = 4
A_TILES = 5
B_TILES = 8
TURN = 512
TURNS = 9


def place():
    t = lax.axis_index("tp")
    return t // NZ, t % NZ


def near_to_far(z):
    def high(q):
        return (q, 5 - q, jnp.int32(1), jnp.int32(0))

    up = high(z)
    low = high(3 - z)
    return [jnp.where(z >= 2, u, 3 - v) for u, v in zip(up, low)]


def send_to(src, dst, send_sem, recv_sem, tp):
    return pltpu.make_async_remote_copy(
        src_ref=src,
        dst_ref=dst,
        send_sem=send_sem,
        recv_sem=recv_sem,
        device_id={"tp": tp},
        device_id_type=MESH,
    )


def tp_of(x, z):
    return x * NZ + z


def send_along(src, dst, send_sem, recv_sem, seq):
    return pltpu.make_async_remote_copy(
        src_ref=src,
        dst_ref=dst,
        send_sem=send_sem,
        recv_sem=recv_sem,
        device_id={"seq": seq},
        device_id_type=MESH,
    )


def greet(device):
    barrier = pltpu.get_barrier_semaphore()
    pl.semaphore_signal(barrier, inc=1, device_id=device, device_id_type=MESH)


def meet(x, z, s, blocks):
    barrier = pltpu.get_barrier_semaphore()
    early = (s // 2) % 2 == 0
    greet({"tp": tp_of((x + 1) % NX, z)})
    greet({"tp": tp_of((x + 3) % NX, z)})
    pl.when(z > 0)(lambda: greet({"tp": tp_of(x, z - 1)}))
    pl.when(z < NZ - 1)(lambda: greet({"tp": tp_of(x, z + 1)}))
    greet({"seq": s + 1 - 2 * (s % 2)})
    near = jnp.where((z == 0) | (z == NZ - 1), 4, 5)
    others = [s - 2, s + 2, s - 1 + 2 * (s % 2)]
    there = [(o >= 0) & (o < blocks) for o in others]
    far = sum(jnp.where(t, 1, 0) for t in there)

    def first():
        pl.semaphore_wait(barrier, near + jnp.where(early, 0, far))
        for o, t in zip(others, there):
            pl.when(t)(lambda o=o: greet({"seq": o}))

    def second():
        pl.when(early)(lambda: pl.semaphore_wait(barrier, far))

    return first, second


class Sends:
    def __init__(self):
        self.started = []

    def start(self, copy, when=None):
        self.started.append((copy, when))
        if when is None:
            copy.start()
        else:
            pl.when(when)(lambda: copy.start())

    def finish(self):
        for copy, when in self.started:
            if when is None:
                copy.wait_send()
            else:
                pl.when(when)(lambda copy=copy: copy.wait_send())


def whole(
    tokens_ref, gain_ref, grad_ref, wq_ref, wk_ref, wv_ref, out_ref,
    tok, gain, w, wt, g, dout, qb, kv, kt, e_buf, dp_buf, b_buf, dr_buf, acc,
    back_out, back_near, back_far, back_chip, grads, total, got_opp, got_x, got_za, got_zb,
    load_sem, sx, rx, szb, rzb, sza, rza, s_near, r_near, s_far, r_far,
    s_bn, r_bn, s_bf, r_bf, s_bc, r_bc, s1, r1, s2, r2, tza, uza, tzb, uzb,
):
    x, z = place()
    s = lax.axis_index("seq")
    blocks = lax.axis_size("seq")
    rows, width = tok.shape
    half = rows // 2
    a_width = A_TILES * 128
    a_cols = pl.ds(0, a_width)
    b_cols = pl.ds(a_width, width - a_width)
    xp, xm, xo = (x + 1) % NX, (x + 3) % NX, (x + 2) % NX
    zs = near_to_far(z)
    q_cols, k_cols = wq_ref.shape[1], wk_ref.shape[1]
    meet_first, meet_second = meet(x, z, s, blocks)
    loads = [
        pltpu.make_async_copy(tokens_ref, tok, load_sem.at[0]),
        pltpu.make_async_copy(gain_ref, gain, load_sem.at[1]),
        pltpu.make_async_copy(wq_ref, w.at[:, pl.ds(0, q_cols)], load_sem.at[2]),
        pltpu.make_async_copy(wk_ref, w.at[:, pl.ds(q_cols, k_cols)], load_sem.at[3]),
        pltpu.make_async_copy(wv_ref, w.at[:, pl.ds(q_cols + k_cols, k_cols)], load_sem.at[4]),
        pltpu.make_async_copy(grad_ref, dout, load_sem.at[5]),
    ]
    for load in loads:
        load.start()
    loads[0].wait()
    loads[1].wait()

    def gain_row():
        return jnp.concatenate([gain[i : i + 1, :] for i in range(gain.shape[0])], axis=1)

    values = tok[...].astype(jnp.float32)
    inv_rms = lax.rsqrt(jnp.mean(values * values, axis=1, keepdims=True) + EPS)
    g[z, pl.ds(x * rows, rows), :] = (values * inv_rms * gain_row()).astype(jnp.bfloat16)
    meet_first()
    sends = Sends()

    def part(zr, xr, h, cols):
        if h is None:
            return g.at[zr, pl.ds(pl.multiple_of(xr * rows, rows), rows), cols]
        return g.at[zr, pl.ds(pl.multiple_of(xr * rows + h * half, half), half), cols]

    def x_send(k, zr, xr, h, cols, to, direction, slot):
        piece = part(zr, xr, h, cols)
        p = 1 if k == NZ else 0
        sends.start(
            send_to(piece, piece, sx.at[direction, k, slot], rx.at[p, zr, xr, h], tp_of(to, z))
        )

    def x_wait(k, zr, xr, h, cols):
        piece = part(zr, xr, h, cols)
        p = 1 if k == NZ else 0
        send_to(piece, piece, sx.at[0, k, 0], rx.at[p, zr, xr, h], tp_of(xp, z)).wait_recv()

    def x_own(k, zr, cols, first):
        h_right, h_left = (0, 1) if first else (1, 0)
        slot = 0 if first else 1
        x_send(k, zr, x, h_right, cols, xp, 0, slot)
        x_send(k, zr, x, h_left, cols, xm, 1, slot)

    def x_forward(k, zr, cols):
        x_wait(k, zr, xm, 0, cols)
        x_send(k, zr, xm, 0, cols, xp, 0, 2)
        x_wait(k, zr, xp, 1, cols)
        x_send(k, zr, xp, 1, cols, xm, 1, 2)

    def x_rest_near(k, zr, cols):
        x_wait(k, zr, xm, 1, cols)
        x_wait(k, zr, xp, 0, cols)

    def x_rest_opposite(k, zr, cols):
        x_wait(k, zr, xo, 0, cols)
        x_wait(k, zr, xo, 1, cols)

    def x_rest(k, zr, cols):
        x_rest_near(k, zr, cols)
        x_rest_opposite(k, zr, cols)

    def z_send_b(k, zr, way, to):
        piece = part(zr, x, None, b_cols)
        sends.start(send_to(piece, piece, szb.at[way, k], rzb.at[zr], tp_of(x, to)))

    def z_send_a(k, zr, xr, way, to):
        piece = part(zr, xr, None, a_cols)
        sends.start(
            send_to(piece, piece, sza.at[way, k, xr], rza.at[zr, xr], tp_of(x, to))
        )

    def z_wait_b(k):
        piece = part(zs[k], x, None, b_cols)
        send_to(piece, piece, szb.at[0, 0], rzb.at[zs[k]], tp_of(xp, z)).wait_recv()

    def z_wait_a(k):
        for i in range(NX):
            piece = part(zs[k], i, None, a_cols)
            send_to(piece, piece, sza.at[0, 0, i], rza.at[zs[k], i], tp_of(xp, z)).wait_recv()

    def turn(c):
        at = pl.ds(c * TURN, TURN)
        wt[:, at] = w[at, :].T

    def slab(first, count, zr):
        return kv.at[pl.ds(first, count), pl.ds(pl.multiple_of(zr * rows, rows), rows), :]

    def near_copy(k, zr):
        return send_along(
            slab(5, 4, zr), slab(1, 4, zr), s_near.at[k], r_near.at[k],
            jnp.minimum(s + 1, blocks - 1),
        )

    def far_copy(k, zr):
        return send_along(
            slab(8, 1, zr), slab(0, 1, zr), s_far.at[k], r_far.at[k],
            jnp.minimum(s + 2, blocks - 1),
        )

    def project(k):
        zr = zs[k]
        out = jnp.dot(g[zr], w[...], preferred_element_type=jnp.float32).astype(jnp.bfloat16)
        at = pl.ds(pl.multiple_of(zr * rows, rows), rows)
        for i in range(NX):
            kv[5 + i, at, :] = out[i * rows : (i + 1) * rows, q_cols:]
            qb[i, at, :] = out[i * rows : (i + 1) * rows, :q_cols]
        pl.when(s + 2 < blocks)(lambda: far_copy(k, zr).start())
        pl.when(s + 1 < blocks)(lambda: near_copy(k, zr).start())

    is_edge = (z == 0) | (z == NZ - 1)

    def start_gather(neighbours):
        x_own(NZ, z, a_cols, True)
        x_own(NZ, z, a_cols, False)
        for way, to in neighbours:
            z_send_b(0, z, way, to)
        x_own(0, z, b_cols, True)
        x_forward(NZ, z, a_cols)
        x_own(0, z, b_cols, False)
        way, to = neighbours[0]
        x_rest_near(NZ, z, a_cols)
        for i in (x, xm, xp):
            z_send_a(0, z, i, way, to)
        for load in loads[2:]:
            load.wait()
        clear_edges()
        turn(0)
        x_rest_opposite(NZ, z, a_cols)
        z_send_a(0, z, xo, way, to)
        x_forward(0, z, b_cols)
        meet_second()

    def clear_edges():
        @pl.when(s == 0)
        def _():
            kv[0:5] = jnp.zeros_like(kv[0:5])

        @pl.when(s == 1)
        def _():
            kv[0] = jnp.zeros_like(kv[0])

        @pl.when(s == blocks - 1)
        def _():
            back_near[...] = jnp.zeros_like(back_near)

        @pl.when((s >= blocks - 2) | (s % 2 == 1))
        def _():
            back_far[...] = jnp.zeros_like(back_far)

    @pl.when(is_edge)
    def _():
        start_gather([(0, jnp.where(z == 0, 1, NZ - 2))])
        z_wait_b(1)
        x_own(1, zs[1], b_cols, True)
        x_own(1, zs[1], b_cols, False)
        for c in range(1, 5):
            turn(c)
        x_rest(0, z, b_cols)
        project(0)
        x_forward(1, zs[1], b_cols)
        turn(5)
        z_wait_b(2)
        x_own(2, zs[2], b_cols, True)
        x_own(2, zs[2], b_cols, False)
        z_wait_a(1)
        x_rest(1, zs[1], b_cols)
        project(1)
        x_forward(2, zs[2], b_cols)
        z_wait_b(3)
        x_own(3, zs[3], b_cols, True)
        x_own(3, zs[3], b_cols, False)
        for c in range(6, TURNS):
            turn(c)
        z_wait_a(2)
        x_rest(2, zs[2], b_cols)
        project(2)
        x_forward(3, zs[3], b_cols)
        z_wait_a(3)
        x_rest(3, zs[3], b_cols)
        project(3)
        sends.finish()

    sends = Sends()

    @pl.when(jnp.logical_not(is_edge))
    def _():
        outer = jnp.where(z == 1, 0, NZ - 1)
        inner = NZ - 1 - z
        start_gather([(0, outer), (1, inner)])
        z_wait_b(1)
        z_send_b(1, zs[1], 1, inner)
        for i in (x, xm, xp, xo):
            z_send_a(0, z, i, 1, inner)
        x_own(1, zs[1], b_cols, True)
        x_own(1, zs[1], b_cols, False)
        z_wait_b(2)
        z_send_b(2, zs[2], 0, outer)
        x_own(2, zs[2], b_cols, True)
        x_own(2, zs[2], b_cols, False)
        for c in range(1, 4):
            turn(c)
        x_rest(0, z, b_cols)
        project(0)
        z_wait_a(1)
        for i in range(NX):
            z_send_a(1, zs[1], i, 1, inner)
        z_wait_b(3)
        z_send_b(3, zs[3], 0, outer)
        x_forward(1, zs[1], b_cols)
        x_own(3, zs[3], b_cols, True)
        x_own(3, zs[3], b_cols, False)
        for c in range(4, 7):
            turn(c)
        x_forward(2, zs[2], b_cols)
        z_wait_a(2)
        for i in range(NX):
            z_send_a(2, zs[2], i, 0, outer)
        for c in range(7, TURNS):
            turn(c)
        x_rest(1, zs[1], b_cols)
        project(1)
        z_wait_a(3)
        for i in range(NX):
            z_send_a(3, zs[3], i, 0, outer)
        x_forward(3, zs[3], b_cols)
        x_rest(2, zs[2], b_cols)
        project(2)
        x_rest(3, zs[3], b_cols)
        project(3)
        sends.finish()

    hd = HEAD_SIZE
    last = (((1,), (1,)), ((), ()))

    def two_heads(ref, qt):
        return jnp.concatenate([ref[qt, :, 0:hd], ref[qt, :, hd : 2 * hd]], axis=0)

    row_at = lax.broadcasted_iota(jnp.int32, (hd, 2 * hd), 0)
    col_at = lax.broadcasted_iota(jnp.int32, (hd, 2 * hd), 1) % hd

    def scores(qt, c, q2, do2):
        j = qt + c
        raw = lax.dot_general(kv[j, :, 0:hd], q2, last, preferred_element_type=jnp.float32)
        bent = jnp.tanh(raw * (SCALE / CAP))
        expo = jnp.exp(CAP * bent)
        if c == 0:
            expo = jnp.where(row_at > col_at, expo, 0.0)
        if c == 5:
            expo = jnp.where(row_at <= col_at, expo, 0.0)
        if j < 5:
            expo = expo * jnp.where(s >= (1 if j > 0 else 2), 1.0, 0.0)
        d_probs = lax.dot_general(
            kv[j, :, hd : 2 * hd], do2, last, preferred_element_type=jnp.float32
        )
        e_buf[qt, c] = expo
        dp_buf[qt, c] = d_probs
        b_buf[qt, c] = bent
        shape = (hd // 8, 8, 2 * hd)
        return (
            jnp.sum(expo.reshape(shape), axis=0),
            jnp.sum((expo * d_probs).reshape(shape), axis=0),
        )

    def transpose_keys(j):
        kt[:, pl.ds(j * hd, hd)] = kv[j, :, 0:hd].astype(jnp.float32).T.astype(jnp.bfloat16)

    sums = []
    for qt in range(NX):
        q2, do2 = two_heads(qb, qt), two_heads(dout, qt)
        parts = [scores(qt, c, q2, do2) for c in range(5 - qt, 6)]
        sums.append((sum(p[0] for p in parts), sum(p[1] for p in parts)))
    for j in range(5, 9):
        transpose_keys(j)

    @pl.when(s > 0)
    def _():
        for k in range(NZ):
            near_copy(k, zs[k]).wait_recv()

    @pl.when(s > 1)
    def _():
        for k in range(NZ):
            far_copy(k, zs[k]).wait_recv()

    for j in range(5):
        transpose_keys(j)

    rest = []
    for qt in range(NX):
        q2, do2 = two_heads(qb, qt), two_heads(dout, qt)
        parts = [scores(qt, c, q2, do2) for c in range(0, 5 - qt)]
        norm = jnp.sum(sums[qt][0] + sum(p[0] for p in parts), axis=0, keepdims=True)
        inner = jnp.sum(sums[qt][1] + sum(p[1] for p in parts), axis=0, keepdims=True)
        inverse = 1.0 / norm
        rest.append((inverse, inner * inverse))

    def tile_grads(j):
        d_key = d_value = 0.0
        for qt in range(max(0, j - 5), min(NX, j + 1)):
            c = j - qt
            inverse, delta = rest[qt]
            probs = e_buf[qt, c] * inverse
            bent = b_buf[qt, c]
            d_raw = (
                probs * (dp_buf[qt, c] - delta) * (1.0 - bent * bent) * SCALE
            ).astype(jnp.bfloat16)
            dr_buf[qt, pl.ds(c * hd, hd), :] = d_raw
            d_key += jnp.dot(d_raw, two_heads(qb, qt), preferred_element_type=jnp.float32)
            d_value += jnp.dot(
                probs.astype(jnp.bfloat16), two_heads(dout, qt), preferred_element_type=jnp.float32
            )
        return d_key, d_value

    far_back = send_along(
        back_out.at[0], back_far, s_bf.at[0], r_bf.at[0], jnp.maximum(s - 2, 0)
    )
    near_back = [
        send_along(
            back_out.at[j], back_near.at[j - 1], s_bn.at[j - 1], r_bn.at[j - 1],
            jnp.maximum(s - 1, 0),
        )
        for j in range(1, 5)
    ]
    chip_back = send_along(
        back_out.at[0], back_chip, s_bc.at[0], r_bc.at[0], jnp.maximum(s - 1, 0)
    )
    is_odd = s % 2 == 1
    for j in range(5):
        d_key, d_value = tile_grads(j)
        back_out[j, :, 0:hd] = d_key.astype(jnp.bfloat16)
        back_out[j, :, hd : 2 * hd] = d_value.astype(jnp.bfloat16)
        if j == 0:
            pl.when(is_odd)(lambda: chip_back.start())
            pl.when((s > 1) & jnp.logical_not(is_odd))(lambda: far_back.start())
        elif j < 4:
            pl.when(s > 0)(lambda j=j: near_back[j - 1].start())
        else:

            @pl.when(jnp.logical_not(is_odd))
            def _():
                chip_back.wait_recv()
                other = back_chip[...].astype(jnp.float32)
                back_out[j, :, 0:hd] = (d_key + other[:, 0:hd]).astype(jnp.bfloat16)
                back_out[j, :, hd : 2 * hd] = (d_value + other[:, hd : 2 * hd]).astype(
                    jnp.bfloat16
                )

            pl.when(s > 0)(lambda: near_back[3].start())
    for j in range(5, 9):
        d_key, d_value = tile_grads(j)
        acc[j - 5, :, 0:hd] = d_key
        acc[j - 5, :, hd : 2 * hd] = d_value
    for qt in range(NX):
        d_query = jnp.dot(
            kt[:, pl.ds(qt * hd, 6 * hd)], dr_buf[qt], preferred_element_type=jnp.float32
        )
        grads[qt, :, 0:hd] = d_query[:, 0:hd].T.astype(jnp.bfloat16)
        grads[qt, :, hd : 2 * hd] = d_query[:, hd : 2 * hd].T.astype(jnp.bfloat16)

    @pl.when((s < blocks - 2) & jnp.logical_not(is_odd))
    def _():
        far_back.wait_recv()

    @pl.when(s < blocks - 1)
    def _():
        for i in range(NX):
            send_along(
                back_out.at[i + 1], back_near.at[i], s_bn.at[i], r_bn.at[i], s
            ).wait_recv()

    for i in range(NX):
        own = acc[i] + back_near[i].astype(jnp.float32)
        if i == NX - 1:
            own = own + back_far[...].astype(jnp.float32)
        grads[i, :, q_cols:] = own.astype(jnp.bfloat16)

    zs = zs[::-1]
    p = g
    tile = 768
    a_width = B_TILES * 128
    a_cols = pl.ds(0, a_width)
    b_cols = pl.ds(a_width, width - a_width)
    b_half = (width - a_width) // 2
    a_half = a_width // 2
    a_parts = [pl.ds(0, a_half), pl.ds(a_half, a_half)]
    b_parts = [pl.ds(a_width, b_half), pl.ds(a_width + b_half, b_half)]

    def row_ds(xr, h=None):
        if h is None:
            return pl.ds(pl.multiple_of(xr * rows, rows), rows)
        return pl.ds(pl.multiple_of(xr * rows + h * half, half), half)

    def compute(zr):
        lhs = grads[:, pl.ds(pl.multiple_of(zr * rows, rows), rows), :].reshape(NX * rows, -1)

        for j in range(width // tile):
            at = pl.ds(j * tile, tile)
            p[zr, :, at] = jnp.dot(
                lhs, wt[:, at], preferred_element_type=jnp.float32
            ).astype(jnp.bfloat16)

    def way(zr):
        return jnp.where(zr > z, 1, 0)

    def nearer(zr):
        return tp_of(x, jnp.where(zr > z, z + 1, z - 1))

    def step1(k, zr, cols):
        for direction, to in ((0, xm), (1, xp)):
            sends.start(
                send_to(
                    p.at[zr, row_ds(xo, direction), cols],
                    got_opp.at[direction, zr, :, cols],
                    s1.at[direction, k],
                    r1.at[direction, k],
                    tp_of(to, z),
                )
            )

    def step2(k, zr, parts):
        for direction, to in ((0, xm), (1, xp)):
            for cols in parts if len(parts) == 1 else [b_cols]:
                land = got_opp.at[direction, zr, :, cols]
                send_to(
                    land, land, s1.at[direction, k], r1.at[direction, k], tp_of(to, z)
                ).wait_recv()
            at = row_ds(to, direction)
            for h, cols in enumerate(parts):
                p[zr, at, cols] = (
                    p[zr, at, cols].astype(jnp.float32)
                    + got_opp[direction, zr, :, cols].astype(jnp.float32)
                ).astype(jnp.bfloat16)
                sends.start(
                    send_to(
                        p.at[zr, row_ds(to), cols],
                        got_x.at[direction, zr, :, cols],
                        s2.at[direction, k, h],
                        r2.at[direction, k, h],
                        tp_of(to, z),
                    )
                )

    def x_sum(k, h, zr, cols):
        for direction, to in ((0, xm), (1, xp)):
            land = got_x.at[direction, zr, :, cols]
            send_to(
                land, land, s2.at[direction, k, h], r2.at[direction, k, h], tp_of(to, z)
            ).wait_recv()
        return (
            p[zr, row_ds(x), cols].astype(jnp.float32)
            + got_x[0, zr, :, cols].astype(jnp.float32)
            + got_x[1, zr, :, cols].astype(jnp.float32)
        )

    def line_b(d, zr, h):
        return got_zb.at[d, zr, h]

    def line_wait_b(d, zr, h):
        land = line_b(d, zr, h)
        send_to(land, land, tzb.at[0, h], uzb.at[d, zr, h], tp_of(xp, z)).wait_recv()

    def line_wait_a(d, zr, h):
        land = got_za.at[d, zr, :, a_parts[h]]
        send_to(land, land, tza.at[0, h], uza.at[d, zr, h], tp_of(xp, z)).wait_recv()

    def step3(k, far):
        zr = zs[k]
        for h, cols in enumerate(b_parts):
            value = x_sum(k, h, zr, cols)
            if far:
                line_wait_b(way(zr), zr, h)
                value = value + got_zb[way(zr), zr, h].astype(jnp.float32)
            p[zr, row_ds(x), cols] = value.astype(jnp.bfloat16)
            sends.start(
                send_to(
                    p.at[zr, row_ds(x), cols], line_b(way(zr), zr, h), tzb.at[k, h],
                    uzb.at[way(zr), zr, h], nearer(zr),
                )
            )

    def add_a(d, zr, h):
        line_wait_a(d, zr, h)
        cols = a_parts[h]
        p[zr, :, cols] = (
            p[zr, :, cols].astype(jnp.float32) + got_za[d, zr, :, cols].astype(jnp.float32)
        ).astype(jnp.bfloat16)

    def line_a(k, far, when=None):
        zr = zs[k]
        for h, cols in enumerate(a_parts):
            if far:
                add_a(way(zr), zr, h)
            sends.start(
                send_to(
                    p.at[zr, :, cols], got_za.at[way(zr), zr, :, cols], tza.at[k, h],
                    uza.at[way(zr), zr, h], nearer(zr),
                ),
                when,
            )

    def finish(sources):
        for h, cols in enumerate(b_parts):
            value = x_sum(3, h, z, cols)
            for d in sources:
                line_wait_b(d, z, h)
                value = value + got_zb[d, z, h].astype(jnp.float32)
            total[:, cols] = value
        total[:, a_cols] = x_sum(4, 0, z, a_cols)
        values = tok[...].astype(jnp.float32)
        inv_rms = lax.rsqrt(jnp.mean(values * values, axis=1, keepdims=True) + EPS)
        upper = total[...] * gain_row()
        xhat = values * inv_rms
        out_ref[...] = (
            inv_rms * (upper - xhat * jnp.mean(upper * xhat, axis=1, keepdims=True))
        ).astype(jnp.bfloat16)
        sends.finish()

    sends = Sends()
    compute(zs[0])
    step1(0, zs[0], b_cols)
    line_a(0, False, is_edge)
    compute(zs[1])
    step1(1, zs[1], b_cols)
    line_a(1, False, is_edge)
    compute(zs[2])
    step1(2, zs[2], b_cols)
    line_a(2, False, is_edge)
    compute(z)
    opening, sends = sends, Sends()

    @pl.when(is_edge)
    def _():
        source = jnp.where(z == 0, 0, 1)
        step2(0, zs[0], b_parts)
        step2(1, zs[1], b_parts)
        step2(2, zs[2], b_parts)
        step1(3, z, b_cols)
        step3(0, False)
        step3(1, False)
        add_a(source, z, 0)
        add_a(source, z, 1)
        step1(4, z, a_cols)
        step3(2, False)
        step2(3, z, b_parts)
        step2(4, z, [a_cols])
        finish([source])

    sends = Sends()

    @pl.when(jnp.logical_not(is_edge))
    def _():
        step2(0, zs[0], b_parts)
        step2(1, zs[1], b_parts)
        step2(2, zs[2], b_parts)
        step1(3, z, b_cols)
        line_a(0, True)
        line_a(1, True)
        line_a(2, True)
        for d in (0, 1):
            for h in (0, 1):
                add_a(d, z, h)
        step1(4, z, a_cols)
        step3(0, True)
        step2(3, z, b_parts)
        step3(1, True)
        step2(4, z, [a_cols])
        step3(2, True)
        finish([0, 1])

    opening.finish()

    @pl.when(s > 0)
    def _():
        for copy in near_back:
            copy.wait_send()

    @pl.when((s > 1) & jnp.logical_not(is_odd))
    def _():
        far_back.wait_send()

    @pl.when(is_odd)
    def _():
        chip_back.wait_send()

    @pl.when(s + 1 < blocks)
    def _():
        for k in range(NZ):
            near_copy(k, zs[NZ - 1 - k]).wait_send()

    @pl.when(s + 2 < blocks)
    def _():
        for k in range(NZ):
            far_copy(k, zs[NZ - 1 - k]).wait_send()


def on_device(tokens, norm_gain, query_weight, key_matrix, value_matrix, output_grad):
    rows, width = tokens.shape
    q_cols, k_cols = query_weight.shape[1], key_matrix.shape[1]
    cols = q_cols + 2 * k_cols
    a_width = B_TILES * 128
    hd = HEAD_SIZE
    any_space = pl.BlockSpec(memory_space=pltpu.HBM)
    dma = pltpu.SemaphoreType.DMA
    low, full = jnp.bfloat16, jnp.float32

    def vmem(kind, *shape):
        return pltpu.VMEM(shape, kind)

    return pl.pallas_call(
        whole,
        out_shape=jax.ShapeDtypeStruct((rows, width), low),
        in_specs=[any_space] * 6,
        out_specs=pl.BlockSpec(memory_space=pltpu.VMEM),
        scratch_shapes=[
            vmem(low, rows, width),
            vmem(full, width // 128, 128),
            vmem(low, width, cols),
            vmem(low, cols, width),
            vmem(low, NZ, NX * rows, width),
            vmem(low, NX, hd, q_cols),
            vmem(low, NX, hd, q_cols),
            vmem(low, 9, hd, 2 * k_cols),
            vmem(low, hd, 9 * hd),
            vmem(full, NX, 6, hd, 2 * hd),
            vmem(full, NX, 6, hd, 2 * hd),
            vmem(full, NX, 6, hd, 2 * hd),
            vmem(low, NX, 6 * hd, 2 * hd),
            vmem(full, NX, hd, 2 * k_cols),
            vmem(low, 5, hd, 2 * k_cols),
            vmem(low, NX, hd, 2 * k_cols),
            vmem(low, hd, 2 * k_cols),
            vmem(low, hd, 2 * k_cols),
            vmem(low, NX, hd, cols),
            vmem(full, rows, width),
            vmem(low, 2, NZ, rows // 2, width),
            vmem(low, 2, NZ, rows, width),
            vmem(low, 2, NZ, NX * rows, a_width),
            vmem(low, 2, NZ, 2, rows, (width - a_width) // 2),
            dma((6,)),
            dma((2, NZ + 1, 3)),
            dma((2, NZ, NX, 2)),
            dma((2, NZ)),
            dma((NZ,)),
            dma((2, NZ, NX)),
            dma((NZ, NX)),
            dma((NZ,)),
            dma((NZ,)),
            dma((NZ,)),
            dma((NZ,)),
            dma((NX,)),
            dma((NX,)),
            dma((1,)),
            dma((1,)),
            dma((1,)),
            dma((1,)),
            dma((2, NZ + 1)),
            dma((2, NZ + 1)),
            dma((2, NZ + 1, 2)),
            dma((2, NZ + 1, 2)),
            dma((NZ, 2)),
            dma((2, NZ, 2)),
            dma((NZ, 2)),
            dma((2, NZ, 2)),
        ],
        compiler_params=pltpu.CompilerParams(
            collective_id=0, has_side_effects=True, vmem_limit_bytes=62 * 1024 * 1024
        ),
    )(
        tokens,
        norm_gain.reshape(-1, 128),
        output_grad.reshape(NX, hd, q_cols),
        query_weight,
        key_matrix,
        value_matrix,
    )


def solution(mesh):
    tp, both = "tp", ("seq", "tp")
    in_specs = (P(both, None), P(), P(None, tp), P(None, tp), P(None, tp), P("seq", tp))
    return jax.shard_map(
        on_device, mesh=mesh, in_specs=in_specs, out_specs=P(both, None), check_vma=False
    )
```

```python
import jax
import jax.numpy as jnp
from jax import lax
from jax.experimental import pallas as pl
from jax.experimental.pallas import tpu as pltpu
from jax.sharding import PartitionSpec as P

HEAD_SIZE = 128
WINDOW = 640
SCALE = 1.0 / 12.0
CAP = 50.0
EPS = 1e-06
MESH = pl.DeviceIdType.MESH
NX = 4
NZ = 4
A_TILES = 5
B_TILES = 8
TURN = 512
TURNS = 9


def place():
    t = lax.axis_index("tp")
    return t // NZ, t % NZ


def near_to_far(z):
    def high(q):
        return (q, 5 - q, jnp.int32(1), jnp.int32(0))

    up = high(z)
    low = high(3 - z)
    return [jnp.where(z >= 2, u, 3 - v) for u, v in zip(up, low)]


def send_to(src, dst, send_sem, recv_sem, tp):
    return pltpu.make_async_remote_copy(
        src_ref=src,
        dst_ref=dst,
        send_sem=send_sem,
        recv_sem=recv_sem,
        device_id={"tp": tp},
        device_id_type=MESH,
    )


def tp_of(x, z):
    return x * NZ + z


def send_along(src, dst, send_sem, recv_sem, seq):
    return pltpu.make_async_remote_copy(
        src_ref=src,
        dst_ref=dst,
        send_sem=send_sem,
        recv_sem=recv_sem,
        device_id={"seq": seq},
        device_id_type=MESH,
    )


def greet(device):
    barrier = pltpu.get_barrier_semaphore()
    pl.semaphore_signal(barrier, inc=1, device_id=device, device_id_type=MESH)


def meet(x, z, s, blocks):
    barrier = pltpu.get_barrier_semaphore()
    early = (s // 2) % 2 == 0
    greet({"tp": tp_of((x + 1) % NX, z)})
    greet({"tp": tp_of((x + 3) % NX, z)})
    pl.when(z > 0)(lambda: greet({"tp": tp_of(x, z - 1)}))
    pl.when(z < NZ - 1)(lambda: greet({"tp": tp_of(x, z + 1)}))
    greet({"seq": s + 1 - 2 * (s % 2)})
    near = jnp.where((z == 0) | (z == NZ - 1), 4, 5)
    others = [s - 2, s + 2, s - 1 + 2 * (s % 2)]
    there = [(o >= 0) & (o < blocks) for o in others]
    far = sum(jnp.where(t, 1, 0) for t in there)

    def first():
        pl.semaphore_wait(barrier, near + jnp.where(early, 0, far))
        for o, t in zip(others, there):
            pl.when(t)(lambda o=o: greet({"seq": o}))

    def second():
        pl.when(early)(lambda: pl.semaphore_wait(barrier, far))

    return first, second


class Sends:
    def __init__(self):
        self.started = []

    def start(self, copy, when=None):
        self.started.append((copy, when))
        if when is None:
            copy.start()
        else:
            pl.when(when)(lambda: copy.start())

    def finish(self):
        for copy, when in self.started:
            if when is None:
                copy.wait_send()
            else:
                pl.when(when)(lambda copy=copy: copy.wait_send())


def whole(
    tokens_ref, gain_ref, grad_ref, wq_ref, wk_ref, wv_ref, out_ref,
    tok, gain, w, wt, g, dout, qb, kv, kt, e_buf, dp_buf, b_buf, dr_buf, acc,
    back_out, back_near, back_far, back_chip, grads, total, got_opp, got_x, got_za, got_zb,
    load_sem, sx, rx, szb, rzb, sza, rza, s_near, r_near, s_far, r_far,
    s_bn, r_bn, s_bf, r_bf, s_bc, r_bc, s1, r1, s2, r2, tza, uza, tzb, uzb,
):
    x, z = place()
    s = lax.axis_index("seq")
    blocks = lax.axis_size("seq")
    rows, width = tok.shape
    half = rows // 2
    a_width = A_TILES * 128
    a_cols = pl.ds(0, a_width)
    b_cols = pl.ds(a_width, width - a_width)
    xp, xm, xo = (x + 1) % NX, (x + 3) % NX, (x + 2) % NX
    zs = near_to_far(z)
    q_cols, k_cols = wq_ref.shape[1], wk_ref.shape[1]
    meet_first, meet_second = meet(x, z, s, blocks)
    loads = [
        pltpu.make_async_copy(tokens_ref, tok, load_sem.at[0]),
        pltpu.make_async_copy(gain_ref, gain, load_sem.at[1]),
        pltpu.make_async_copy(wq_ref, w.at[:, pl.ds(0, q_cols)], load_sem.at[2]),
        pltpu.make_async_copy(wk_ref, w.at[:, pl.ds(q_cols, k_cols)], load_sem.at[3]),
        pltpu.make_async_copy(wv_ref, w.at[:, pl.ds(q_cols + k_cols, k_cols)], load_sem.at[4]),
        pltpu.make_async_copy(grad_ref, dout, load_sem.at[5]),
    ]
    for load in loads:
        load.start()
    loads[0].wait()
    loads[1].wait()

    def gain_row():
        return jnp.concatenate([gain[i : i + 1, :] for i in range(gain.shape[0])], axis=1)

    values = tok[...].astype(jnp.float32)
    inv_rms = lax.rsqrt(jnp.mean(values * values, axis=1, keepdims=True) + EPS)
    g[z, pl.ds(x * rows, rows), :] = (values * inv_rms * gain_row()).astype(jnp.bfloat16)
    meet_first()
    sends = Sends()

    def part(zr, xr, h, cols):
        if h is None:
            return g.at[zr, pl.ds(pl.multiple_of(xr * rows, rows), rows), cols]
        return g.at[zr, pl.ds(pl.multiple_of(xr * rows + h * half, half), half), cols]

    def x_send(k, zr, xr, h, cols, to, direction, slot):
        piece = part(zr, xr, h, cols)
        p = 1 if k == NZ else 0
        sends.start(
            send_to(piece, piece, sx.at[direction, k, slot], rx.at[p, zr, xr, h], tp_of(to, z))
        )

    def x_wait(k, zr, xr, h, cols):
        piece = part(zr, xr, h, cols)
        p = 1 if k == NZ else 0
        send_to(piece, piece, sx.at[0, k, 0], rx.at[p, zr, xr, h], tp_of(xp, z)).wait_recv()

    def x_own(k, zr, cols, first):
        h_right, h_left = (0, 1) if first else (1, 0)
        slot = 0 if first else 1
        x_send(k, zr, x, h_right, cols, xp, 0, slot)
        x_send(k, zr, x, h_left, cols, xm, 1, slot)

    def x_forward(k, zr, cols):
        x_wait(k, zr, xm, 0, cols)
        x_send(k, zr, xm, 0, cols, xp, 0, 2)
        x_wait(k, zr, xp, 1, cols)
        x_send(k, zr, xp, 1, cols, xm, 1, 2)

    def x_rest_near(k, zr, cols):
        x_wait(k, zr, xm, 1, cols)
        x_wait(k, zr, xp, 0, cols)

    def x_rest_opposite(k, zr, cols):
        x_wait(k, zr, xo, 0, cols)
        x_wait(k, zr, xo, 1, cols)

    def x_rest(k, zr, cols):
        x_rest_near(k, zr, cols)
        x_rest_opposite(k, zr, cols)

    def z_send_b(k, zr, way, to):
        piece = part(zr, x, None, b_cols)
        sends.start(send_to(piece, piece, szb.at[way, k], rzb.at[zr], tp_of(x, to)))

    def z_send_a(k, zr, xr, way, to):
        piece = part(zr, xr, None, a_cols)
        sends.start(
            send_to(piece, piece, sza.at[way, k, xr], rza.at[zr, xr], tp_of(x, to))
        )

    def z_wait_b(k):
        piece = part(zs[k], x, None, b_cols)
        send_to(piece, piece, szb.at[0, 0], rzb.at[zs[k]], tp_of(xp, z)).wait_recv()

    def z_wait_a(k):
        for i in range(NX):
            piece = part(zs[k], i, None, a_cols)
            send_to(piece, piece, sza.at[0, 0, i], rza.at[zs[k], i], tp_of(xp, z)).wait_recv()

    def turn(c):
        at = pl.ds(c * TURN, TURN)
        wt[:, at] = w[at, :].T

    def slab(first, count, zr):
        return kv.at[pl.ds(first, count), pl.ds(pl.multiple_of(zr * rows, rows), rows), :]

    def near_copy(k, zr):
        return send_along(
            slab(5, 4, zr), slab(1, 4, zr), s_near.at[k], r_near.at[k],
            jnp.minimum(s + 1, blocks - 1),
        )

    def far_copy(k, zr):
        return send_along(
            slab(8, 1, zr), slab(0, 1, zr), s_far.at[k], r_far.at[k],
            jnp.minimum(s + 2, blocks - 1),
        )

    def project(k):
        zr = zs[k]
        out = jnp.dot(g[zr], w[...], preferred_element_type=jnp.float32).astype(jnp.bfloat16)
        at = pl.ds(pl.multiple_of(zr * rows, rows), rows)
        for i in range(NX):
            kv[5 + i, at, :] = out[i * rows : (i + 1) * rows, q_cols:]
            qb[i, at, :] = out[i * rows : (i + 1) * rows, :q_cols]
        pl.when(s + 2 < blocks)(lambda: far_copy(k, zr).start())
        pl.when(s + 1 < blocks)(lambda: near_copy(k, zr).start())

    is_edge = (z == 0) | (z == NZ - 1)

    def start_gather(neighbours):
        x_own(NZ, z, a_cols, True)
        x_own(NZ, z, a_cols, False)
        for way, to in neighbours:
            z_send_b(0, z, way, to)
        x_own(0, z, b_cols, True)
        x_forward(NZ, z, a_cols)
        x_own(0, z, b_cols, False)
        way, to = neighbours[0]
        x_rest_near(NZ, z, a_cols)
        for i in (x, xm, xp):
            z_send_a(0, z, i, way, to)
        for load in loads[2:]:
            load.wait()
        clear_edges()
        turn(0)
        x_rest_opposite(NZ, z, a_cols)
        z_send_a(0, z, xo, way, to)
        x_forward(0, z, b_cols)
        meet_second()

    def clear_edges():
        @pl.when(s == 0)
        def _():
            kv[0:5] = jnp.zeros_like(kv[0:5])

        @pl.when(s == 1)
        def _():
            kv[0] = jnp.zeros_like(kv[0])

        @pl.when(s == blocks - 1)
        def _():
            back_near[...] = jnp.zeros_like(back_near)

        @pl.when((s >= blocks - 2) | (s % 2 == 1))
        def _():
            back_far[...] = jnp.zeros_like(back_far)

    @pl.when(is_edge)
    def _():
        start_gather([(0, jnp.where(z == 0, 1, NZ - 2))])
        z_wait_b(1)
        x_own(1, zs[1], b_cols, True)
        x_own(1, zs[1], b_cols, False)
        for c in range(1, 5):
            turn(c)
        x_rest(0, z, b_cols)
        project(0)
        x_forward(1, zs[1], b_cols)
        turn(5)
        z_wait_b(2)
        x_own(2, zs[2], b_cols, True)
        x_own(2, zs[2], b_cols, False)
        z_wait_a(1)
        x_rest(1, zs[1], b_cols)
        project(1)
        x_forward(2, zs[2], b_cols)
        z_wait_b(3)
        x_own(3, zs[3], b_cols, True)
        x_own(3, zs[3], b_cols, False)
        for c in range(6, TURNS):
            turn(c)
        z_wait_a(2)
        x_rest(2, zs[2], b_cols)
        project(2)
        x_forward(3, zs[3], b_cols)
        z_wait_a(3)
        x_rest(3, zs[3], b_cols)
        project(3)
        sends.finish()

    sends = Sends()

    @pl.when(jnp.logical_not(is_edge))
    def _():
        outer = jnp.where(z == 1, 0, NZ - 1)
        inner = NZ - 1 - z
        start_gather([(0, outer), (1, inner)])
        z_wait_b(1)
        z_send_b(1, zs[1], 1, inner)
        for i in (x, xm, xp, xo):
            z_send_a(0, z, i, 1, inner)
        x_own(1, zs[1], b_cols, True)
        x_own(1, zs[1], b_cols, False)
        z_wait_b(2)
        z_send_b(2, zs[2], 0, outer)
        x_own(2, zs[2], b_cols, True)
        x_own(2, zs[2], b_cols, False)
        for c in range(1, 4):
            turn(c)
        x_rest(0, z, b_cols)
        project(0)
        z_wait_a(1)
        for i in range(NX):
            z_send_a(1, zs[1], i, 1, inner)
        z_wait_b(3)
        z_send_b(3, zs[3], 0, outer)
        x_forward(1, zs[1], b_cols)
        x_own(3, zs[3], b_cols, True)
        x_own(3, zs[3], b_cols, False)
        for c in range(4, 7):
            turn(c)
        x_forward(2, zs[2], b_cols)
        z_wait_a(2)
        for i in range(NX):
            z_send_a(2, zs[2], i, 0, outer)
        for c in range(7, TURNS):
            turn(c)
        x_rest(1, zs[1], b_cols)
        project(1)
        z_wait_a(3)
        for i in range(NX):
            z_send_a(3, zs[3], i, 0, outer)
        x_forward(3, zs[3], b_cols)
        x_rest(2, zs[2], b_cols)
        project(2)
        x_rest(3, zs[3], b_cols)
        project(3)
        sends.finish()

    hd = HEAD_SIZE
    last = (((1,), (1,)), ((), ()))

    def two_heads(ref, qt):
        return jnp.concatenate([ref[qt, :, 0:hd], ref[qt, :, hd : 2 * hd]], axis=0)

    row_at = lax.broadcasted_iota(jnp.int32, (hd, 2 * hd), 0)
    col_at = lax.broadcasted_iota(jnp.int32, (hd, 2 * hd), 1) % hd

    def scores(qt, c, q2, do2):
        j = qt + c
        raw = lax.dot_general(kv[j, :, 0:hd], q2, last, preferred_element_type=jnp.float32)
        bent = jnp.tanh(raw * (SCALE / CAP))
        expo = jnp.exp(CAP * bent)
        if c == 0:
            expo = jnp.where(row_at > col_at, expo, 0.0)
        if c == 5:
            expo = jnp.where(row_at <= col_at, expo, 0.0)
        if j < 5:
            expo = expo * jnp.where(s >= (1 if j > 0 else 2), 1.0, 0.0)
        d_probs = lax.dot_general(
            kv[j, :, hd : 2 * hd], do2, last, preferred_element_type=jnp.float32
        )
        e_buf[qt, c] = expo
        dp_buf[qt, c] = d_probs
        b_buf[qt, c] = bent
        shape = (hd // 8, 8, 2 * hd)
        return (
            jnp.sum(expo.reshape(shape), axis=0),
            jnp.sum((expo * d_probs).reshape(shape), axis=0),
        )

    def transpose_keys(j):
        kt[:, pl.ds(j * hd, hd)] = kv[j, :, 0:hd].astype(jnp.float32).T.astype(jnp.bfloat16)

    sums = []
    for qt in range(NX):
        q2, do2 = two_heads(qb, qt), two_heads(dout, qt)
        parts = [scores(qt, c, q2, do2) for c in range(5 - qt, 6)]
        sums.append((sum(p[0] for p in parts), sum(p[1] for p in parts)))
    for j in range(5, 9):
        transpose_keys(j)

    @pl.when(s > 0)
    def _():
        for k in range(NZ):
            near_copy(k, zs[k]).wait_recv()

    @pl.when(s > 1)
    def _():
        for k in range(NZ):
            far_copy(k, zs[k]).wait_recv()

    for j in range(5):
        transpose_keys(j)

    rest = []
    for qt in range(NX):
        q2, do2 = two_heads(qb, qt), two_heads(dout, qt)
        parts = [scores(qt, c, q2, do2) for c in range(0, 5 - qt)]
        norm = jnp.sum(sums[qt][0] + sum(p[0] for p in parts), axis=0, keepdims=True)
        inner = jnp.sum(sums[qt][1] + sum(p[1] for p in parts), axis=0, keepdims=True)
        inverse = 1.0 / norm
        rest.append((inverse, inner * inverse))

    def tile_grads(j):
        d_key = d_value = 0.0
        for qt in range(max(0, j - 5), min(NX, j + 1)):
            c = j - qt
            inverse, delta = rest[qt]
            probs = e_buf[qt, c] * inverse
            bent = b_buf[qt, c]
            d_raw = (
                probs * (dp_buf[qt, c] - delta) * (1.0 - bent * bent) * SCALE
            ).astype(jnp.bfloat16)
            dr_buf[qt, pl.ds(c * hd, hd), :] = d_raw
            d_key += jnp.dot(d_raw, two_heads(qb, qt), preferred_element_type=jnp.float32)
            d_value += jnp.dot(
                probs.astype(jnp.bfloat16), two_heads(dout, qt), preferred_element_type=jnp.float32
            )
        return d_key, d_value

    far_back = send_along(
        back_out.at[0], back_far, s_bf.at[0], r_bf.at[0], jnp.maximum(s - 2, 0)
    )
    near_back = [
        send_along(
            back_out.at[j], back_near.at[j - 1], s_bn.at[j - 1], r_bn.at[j - 1],
            jnp.maximum(s - 1, 0),
        )
        for j in range(1, 5)
    ]
    chip_back = send_along(
        back_out.at[0], back_chip, s_bc.at[0], r_bc.at[0], jnp.maximum(s - 1, 0)
    )
    is_odd = s % 2 == 1
    for j in range(5):
        d_key, d_value = tile_grads(j)
        back_out[j, :, 0:hd] = d_key.astype(jnp.bfloat16)
        back_out[j, :, hd : 2 * hd] = d_value.astype(jnp.bfloat16)
        if j == 0:
            pl.when(is_odd)(lambda: chip_back.start())
            pl.when((s > 1) & jnp.logical_not(is_odd))(lambda: far_back.start())
        elif j < 4:
            pl.when(s > 0)(lambda j=j: near_back[j - 1].start())
        else:

            @pl.when(jnp.logical_not(is_odd))
            def _():
                chip_back.wait_recv()
                other = back_chip[...].astype(jnp.float32)
                back_out[j, :, 0:hd] = (d_key + other[:, 0:hd]).astype(jnp.bfloat16)
                back_out[j, :, hd : 2 * hd] = (d_value + other[:, hd : 2 * hd]).astype(
                    jnp.bfloat16
                )

            pl.when(s > 0)(lambda: near_back[3].start())
    for j in range(5, 9):
        d_key, d_value = tile_grads(j)
        acc[j - 5, :, 0:hd] = d_key
        acc[j - 5, :, hd : 2 * hd] = d_value
    for qt in range(NX):
        d_query = jnp.dot(
            kt[:, pl.ds(qt * hd, 6 * hd)], dr_buf[qt], preferred_element_type=jnp.float32
        )
        grads[qt, :, 0:hd] = d_query[:, 0:hd].T.astype(jnp.bfloat16)
        grads[qt, :, hd : 2 * hd] = d_query[:, hd : 2 * hd].T.astype(jnp.bfloat16)

    @pl.when((s < blocks - 2) & jnp.logical_not(is_odd))
    def _():
        far_back.wait_recv()

    @pl.when(s < blocks - 1)
    def _():
        for i in range(NX):
            send_along(
                back_out.at[i + 1], back_near.at[i], s_bn.at[i], r_bn.at[i], s
            ).wait_recv()

    for i in range(NX):
        own = acc[i] + back_near[i].astype(jnp.float32)
        if i == NX - 1:
            own = own + back_far[...].astype(jnp.float32)
        grads[i, :, q_cols:] = own.astype(jnp.bfloat16)

    zs = zs[::-1]
    p = g
    tile = 768
    a_width = B_TILES * 128
    a_cols = pl.ds(0, a_width)
    b_cols = pl.ds(a_width, width - a_width)
    b_half = (width - a_width) // 2
    a_half = a_width // 2
    a_parts = [pl.ds(0, a_half), pl.ds(a_half, a_half)]
    b_parts = [pl.ds(a_width, b_half), pl.ds(a_width + b_half, b_half)]

    def row_ds(xr, h=None):
        if h is None:
            return pl.ds(pl.multiple_of(xr * rows, rows), rows)
        return pl.ds(pl.multiple_of(xr * rows + h * half, half), half)

    def compute(zr):
        lhs = grads[:, pl.ds(pl.multiple_of(zr * rows, rows), rows), :].reshape(NX * rows, -1)

        for j in range(width // tile):
            at = pl.ds(j * tile, tile)
            p[zr, :, at] = jnp.dot(
                lhs, wt[:, at], preferred_element_type=jnp.float32
            ).astype(jnp.bfloat16)

    def way(zr):
        return jnp.where(zr > z, 1, 0)

    def nearer(zr):
        return tp_of(x, jnp.where(zr > z, z + 1, z - 1))

    def step1(k, zr, cols):
        for direction, to in ((0, xm), (1, xp)):
            sends.start(
                send_to(
                    p.at[zr, row_ds(xo, direction), cols],
                    got_opp.at[direction, zr, :, cols],
                    s1.at[direction, k],
                    r1.at[direction, k],
                    tp_of(to, z),
                )
            )

    def step2(k, zr, parts):
        for direction, to in ((0, xm), (1, xp)):
            for cols in parts if len(parts) == 1 else [b_cols]:
                land = got_opp.at[direction, zr, :, cols]
                send_to(
                    land, land, s1.at[direction, k], r1.at[direction, k], tp_of(to, z)
                ).wait_recv()
            at = row_ds(to, direction)
            for h, cols in enumerate(parts):
                p[zr, at, cols] = (
                    p[zr, at, cols].astype(jnp.float32)
                    + got_opp[direction, zr, :, cols].astype(jnp.float32)
                ).astype(jnp.bfloat16)
                sends.start(
                    send_to(
                        p.at[zr, row_ds(to), cols],
                        got_x.at[direction, zr, :, cols],
                        s2.at[direction, k, h],
                        r2.at[direction, k, h],
                        tp_of(to, z),
                    )
                )

    def x_sum(k, h, zr, cols):
        for direction, to in ((0, xm), (1, xp)):
            land = got_x.at[direction, zr, :, cols]
            send_to(
                land, land, s2.at[direction, k, h], r2.at[direction, k, h], tp_of(to, z)
            ).wait_recv()
        return (
            p[zr, row_ds(x), cols].astype(jnp.float32)
            + got_x[0, zr, :, cols].astype(jnp.float32)
            + got_x[1, zr, :, cols].astype(jnp.float32)
        )

    def line_b(d, zr, h):
        return got_zb.at[d, zr, h]

    def line_wait_b(d, zr, h):
        land = line_b(d, zr, h)
        send_to(land, land, tzb.at[0, h], uzb.at[d, zr, h], tp_of(xp, z)).wait_recv()

    def line_wait_a(d, zr, h):
        land = got_za.at[d, zr, :, a_parts[h]]
        send_to(land, land, tza.at[0, h], uza.at[d, zr, h], tp_of(xp, z)).wait_recv()

    def step3(k, far, halves=(0, 1)):
        zr = zs[k]
        for h in halves:
            cols = b_parts[h]
            value = x_sum(k, h, zr, cols)
            if far:
                line_wait_b(way(zr), zr, h)
                value = value + got_zb[way(zr), zr, h].astype(jnp.float32)
            p[zr, row_ds(x), cols] = value.astype(jnp.bfloat16)
            sends.start(
                send_to(
                    p.at[zr, row_ds(x), cols], line_b(way(zr), zr, h), tzb.at[k, h],
                    uzb.at[way(zr), zr, h], nearer(zr),
                )
            )

    def add_a(d, zr, h):
        line_wait_a(d, zr, h)
        cols = a_parts[h]
        p[zr, :, cols] = (
            p[zr, :, cols].astype(jnp.float32) + got_za[d, zr, :, cols].astype(jnp.float32)
        ).astype(jnp.bfloat16)

    def line_a(k, far, when=None):
        zr = zs[k]
        for h, cols in enumerate(a_parts):
            if far:
                add_a(way(zr), zr, h)
            sends.start(
                send_to(
                    p.at[zr, :, cols], got_za.at[way(zr), zr, :, cols], tza.at[k, h],
                    uza.at[way(zr), zr, h], nearer(zr),
                ),
                when,
            )

    def finish(sources):
        for h, cols in enumerate(b_parts):
            value = x_sum(3, h, z, cols)
            for d in sources:
                line_wait_b(d, z, h)
                value = value + got_zb[d, z, h].astype(jnp.float32)
            total[:, cols] = value
        total[:, a_cols] = x_sum(4, 0, z, a_cols)
        values = tok[...].astype(jnp.float32)
        inv_rms = lax.rsqrt(jnp.mean(values * values, axis=1, keepdims=True) + EPS)
        upper = total[...] * gain_row()
        xhat = values * inv_rms
        out_ref[...] = (
            inv_rms * (upper - xhat * jnp.mean(upper * xhat, axis=1, keepdims=True))
        ).astype(jnp.bfloat16)
        sends.finish()

    sends = Sends()
    compute(zs[0])
    step1(0, zs[0], b_cols)
    line_a(0, False, is_edge)
    compute(zs[1])
    step1(1, zs[1], b_cols)
    line_a(1, False, is_edge)
    compute(zs[2])
    step1(2, zs[2], b_cols)
    line_a(2, False, is_edge)
    compute(z)
    opening, sends = sends, Sends()

    @pl.when(is_edge)
    def _():
        source = jnp.where(z == 0, 0, 1)
        step2(0, zs[0], b_parts)
        step2(1, zs[1], b_parts)
        step2(2, zs[2], b_parts)
        step1(3, z, b_cols)
        step3(0, False)
        step3(1, False)
        add_a(source, z, 0)
        add_a(source, z, 1)
        step1(4, z, a_cols)
        step3(2, False)
        step2(3, z, b_parts)
        step2(4, z, [a_cols])
        finish([source])

    sends = Sends()

    @pl.when(jnp.logical_not(is_edge))
    def _():
        step2(0, zs[0], b_parts)
        step2(1, zs[1], b_parts)
        step2(2, zs[2], b_parts)
        step1(3, z, b_cols)
        line_a(0, True)
        line_a(1, True)
        line_a(2, True)
        for d in (0, 1):
            for h in (0, 1):
                add_a(d, z, h)
        step1(4, z, a_cols)
        step3(0, True)
        step2(3, z, b_parts)
        for h in (0, 1):
            step3(2, True, (h,))
            step3(1, True, (h,))
        step2(4, z, [a_cols])
        finish([0, 1])

    opening.finish()

    @pl.when(s > 0)
    def _():
        for copy in near_back:
            copy.wait_send()

    @pl.when((s > 1) & jnp.logical_not(is_odd))
    def _():
        far_back.wait_send()

    @pl.when(is_odd)
    def _():
        chip_back.wait_send()

    @pl.when(s + 1 < blocks)
    def _():
        for k in range(NZ):
            near_copy(k, zs[NZ - 1 - k]).wait_send()

    @pl.when(s + 2 < blocks)
    def _():
        for k in range(NZ):
            far_copy(k, zs[NZ - 1 - k]).wait_send()


def on_device(tokens, norm_gain, query_weight, key_matrix, value_matrix, output_grad):
    rows, width = tokens.shape
    q_cols, k_cols = query_weight.shape[1], key_matrix.shape[1]
    cols = q_cols + 2 * k_cols
    a_width = B_TILES * 128
    hd = HEAD_SIZE
    any_space = pl.BlockSpec(memory_space=pltpu.HBM)
    dma = pltpu.SemaphoreType.DMA
    low, full = jnp.bfloat16, jnp.float32

    def vmem(kind, *shape):
        return pltpu.VMEM(shape, kind)

    return pl.pallas_call(
        whole,
        out_shape=jax.ShapeDtypeStruct((rows, width), low),
        in_specs=[any_space] * 6,
        out_specs=pl.BlockSpec(memory_space=pltpu.VMEM),
        scratch_shapes=[
            vmem(low, rows, width),
            vmem(full, width // 128, 128),
            vmem(low, width, cols),
            vmem(low, cols, width),
            vmem(low, NZ, NX * rows, width),
            vmem(low, NX, hd, q_cols),
            vmem(low, NX, hd, q_cols),
            vmem(low, 9, hd, 2 * k_cols),
            vmem(low, hd, 9 * hd),
            vmem(full, NX, 6, hd, 2 * hd),
            vmem(full, NX, 6, hd, 2 * hd),
            vmem(full, NX, 6, hd, 2 * hd),
            vmem(low, NX, 6 * hd, 2 * hd),
            vmem(full, NX, hd, 2 * k_cols),
            vmem(low, 5, hd, 2 * k_cols),
            vmem(low, NX, hd, 2 * k_cols),
            vmem(low, hd, 2 * k_cols),
            vmem(low, hd, 2 * k_cols),
            vmem(low, NX, hd, cols),
            vmem(full, rows, width),
            vmem(low, 2, NZ, rows // 2, width),
            vmem(low, 2, NZ, rows, width),
            vmem(low, 2, NZ, NX * rows, a_width),
            vmem(low, 2, NZ, 2, rows, (width - a_width) // 2),
            dma((6,)),
            dma((2, NZ + 1, 3)),
            dma((2, NZ, NX, 2)),
            dma((2, NZ)),
            dma((NZ,)),
            dma((2, NZ, NX)),
            dma((NZ, NX)),
            dma((NZ,)),
            dma((NZ,)),
            dma((NZ,)),
            dma((NZ,)),
            dma((NX,)),
            dma((NX,)),
            dma((1,)),
            dma((1,)),
            dma((1,)),
            dma((1,)),
            dma((2, NZ + 1)),
            dma((2, NZ + 1)),
            dma((2, NZ + 1, 2)),
            dma((2, NZ + 1, 2)),
            dma((NZ, 2)),
            dma((2, NZ, 2)),
            dma((NZ, 2)),
            dma((2, NZ, 2)),
        ],
        compiler_params=pltpu.CompilerParams(
            collective_id=0, has_side_effects=True, vmem_limit_bytes=62 * 1024 * 1024
        ),
    )(
        tokens,
        norm_gain.reshape(-1, 128),
        output_grad.reshape(NX, hd, q_cols),
        query_weight,
        key_matrix,
        value_matrix,
    )


def solution(mesh):
    tp, both = "tp", ("seq", "tp")
    in_specs = (P(both, None), P(), P(None, tp), P(None, tp), P(None, tp), P("seq", tp))
    return jax.shard_map(
        on_device, mesh=mesh, in_specs=in_specs, out_specs=P(both, None), check_vma=False
    )
```

```python
import jax
import jax.numpy as jnp
from jax import lax
from jax.experimental import pallas as pl
from jax.experimental.pallas import tpu as pltpu
from jax.sharding import PartitionSpec as P

HEAD_SIZE = 128
WINDOW = 640
SCALE = 1.0 / 12.0
CAP = 50.0
EPS = 1e-06
MESH = pl.DeviceIdType.MESH
NX = 4
NZ = 4
A_TILES = 5
B_TILES = 6
TURN = 512
TURNS = 9


def place():
    t = lax.axis_index("tp")
    return t // NZ, t % NZ


def near_to_far(z):
    def high(q):
        return (q, 5 - q, jnp.int32(1), jnp.int32(0))

    up = high(z)
    low = high(3 - z)
    return [jnp.where(z >= 2, u, 3 - v) for u, v in zip(up, low)]


def send_to(src, dst, send_sem, recv_sem, tp):
    return pltpu.make_async_remote_copy(
        src_ref=src,
        dst_ref=dst,
        send_sem=send_sem,
        recv_sem=recv_sem,
        device_id={"tp": tp},
        device_id_type=MESH,
    )


def tp_of(x, z):
    return x * NZ + z


def send_along(src, dst, send_sem, recv_sem, seq):
    return pltpu.make_async_remote_copy(
        src_ref=src,
        dst_ref=dst,
        send_sem=send_sem,
        recv_sem=recv_sem,
        device_id={"seq": seq},
        device_id_type=MESH,
    )


def greet(device):
    barrier = pltpu.get_barrier_semaphore()
    pl.semaphore_signal(barrier, inc=1, device_id=device, device_id_type=MESH)


def meet(x, z, s, blocks):
    barrier = pltpu.get_barrier_semaphore()
    early = (s // 2) % 2 == 0
    greet({"tp": tp_of((x + 1) % NX, z)})
    greet({"tp": tp_of((x + 3) % NX, z)})
    pl.when(z > 0)(lambda: greet({"tp": tp_of(x, z - 1)}))
    pl.when(z < NZ - 1)(lambda: greet({"tp": tp_of(x, z + 1)}))
    greet({"seq": s + 1 - 2 * (s % 2)})
    near = jnp.where((z == 0) | (z == NZ - 1), 4, 5)
    others = [s - 2, s + 2, s - 1 + 2 * (s % 2)]
    there = [(o >= 0) & (o < blocks) for o in others]
    far = sum(jnp.where(t, 1, 0) for t in there)

    def first():
        pl.semaphore_wait(barrier, near + jnp.where(early, 0, far))
        for o, t in zip(others, there):
            pl.when(t)(lambda o=o: greet({"seq": o}))

    def second():
        pl.when(early)(lambda: pl.semaphore_wait(barrier, far))

    return first, second


class Sends:
    def __init__(self):
        self.started = []

    def start(self, copy, when=None):
        self.started.append((copy, when))
        if when is None:
            copy.start()
        else:
            pl.when(when)(lambda: copy.start())

    def finish(self):
        for copy, when in self.started:
            if when is None:
                copy.wait_send()
            else:
                pl.when(when)(lambda copy=copy: copy.wait_send())


def whole(
    tokens_ref, gain_ref, grad_ref, wq_ref, wk_ref, wv_ref, out_ref,
    tok, gain, w, wt, g, dout, qb, kv, kt, e_buf, dp_buf, b_buf, dr_buf, acc,
    back_out, back_near, back_far, back_chip, grads, total, got_opp, got_x, got_za, got_zb,
    load_sem, sx, rx, szb, rzb, sza, rza, s_near, r_near, s_far, r_far,
    s_bn, r_bn, s_bf, r_bf, s_bc, r_bc, s1, r1, s2, r2, tza, uza, tzb, uzb,
):
    x, z = place()
    s = lax.axis_index("seq")
    blocks = lax.axis_size("seq")
    rows, width = tok.shape
    half = rows // 2
    a_width = A_TILES * 128
    a_cols = pl.ds(0, a_width)
    b_cols = pl.ds(a_width, width - a_width)
    xp, xm, xo = (x + 1) % NX, (x + 3) % NX, (x + 2) % NX
    zs = near_to_far(z)
    q_cols, k_cols = wq_ref.shape[1], wk_ref.shape[1]
    meet_first, meet_second = meet(x, z, s, blocks)
    loads = [
        pltpu.make_async_copy(tokens_ref, tok, load_sem.at[0]),
        pltpu.make_async_copy(gain_ref, gain, load_sem.at[1]),
        pltpu.make_async_copy(wq_ref, w.at[:, pl.ds(0, q_cols)], load_sem.at[2]),
        pltpu.make_async_copy(wk_ref, w.at[:, pl.ds(q_cols, k_cols)], load_sem.at[3]),
        pltpu.make_async_copy(wv_ref, w.at[:, pl.ds(q_cols + k_cols, k_cols)], load_sem.at[4]),
        pltpu.make_async_copy(grad_ref, dout, load_sem.at[5]),
    ]
    for load in loads:
        load.start()
    loads[0].wait()
    loads[1].wait()

    def gain_row():
        return jnp.concatenate([gain[i : i + 1, :] for i in range(gain.shape[0])], axis=1)

    values = tok[...].astype(jnp.float32)
    inv_rms = lax.rsqrt(jnp.mean(values * values, axis=1, keepdims=True) + EPS)
    g[z, pl.ds(x * rows, rows), :] = (values * inv_rms * gain_row()).astype(jnp.bfloat16)
    meet_first()
    sends = Sends()

    def part(zr, xr, h, cols):
        if h is None:
            return g.at[zr, pl.ds(pl.multiple_of(xr * rows, rows), rows), cols]
        return g.at[zr, pl.ds(pl.multiple_of(xr * rows + h * half, half), half), cols]

    def x_send(k, zr, xr, h, cols, to, direction, slot):
        piece = part(zr, xr, h, cols)
        p = 1 if k == NZ else 0
        sends.start(
            send_to(piece, piece, sx.at[direction, k, slot], rx.at[p, zr, xr, h], tp_of(to, z))
        )

    def x_wait(k, zr, xr, h, cols):
        piece = part(zr, xr, h, cols)
        p = 1 if k == NZ else 0
        send_to(piece, piece, sx.at[0, k, 0], rx.at[p, zr, xr, h], tp_of(xp, z)).wait_recv()

    def x_own(k, zr, cols, first):
        h_right, h_left = (0, 1) if first else (1, 0)
        slot = 0 if first else 1
        x_send(k, zr, x, h_right, cols, xp, 0, slot)
        x_send(k, zr, x, h_left, cols, xm, 1, slot)

    def x_forward(k, zr, cols):
        x_wait(k, zr, xm, 0, cols)
        x_send(k, zr, xm, 0, cols, xp, 0, 2)
        x_wait(k, zr, xp, 1, cols)
        x_send(k, zr, xp, 1, cols, xm, 1, 2)

    def x_rest_near(k, zr, cols):
        x_wait(k, zr, xm, 1, cols)
        x_wait(k, zr, xp, 0, cols)

    def x_rest_opposite(k, zr, cols):
        x_wait(k, zr, xo, 0, cols)
        x_wait(k, zr, xo, 1, cols)

    def x_rest(k, zr, cols):
        x_rest_near(k, zr, cols)
        x_rest_opposite(k, zr, cols)

    def z_send_b(k, zr, way, to):
        piece = part(zr, x, None, b_cols)
        sends.start(send_to(piece, piece, szb.at[way, k], rzb.at[zr], tp_of(x, to)))

    def z_send_a(k, zr, xr, way, to):
        piece = part(zr, xr, None, a_cols)
        sends.start(
            send_to(piece, piece, sza.at[way, k, xr], rza.at[zr, xr], tp_of(x, to))
        )

    def z_wait_b(k):
        piece = part(zs[k], x, None, b_cols)
        send_to(piece, piece, szb.at[0, 0], rzb.at[zs[k]], tp_of(xp, z)).wait_recv()

    def z_wait_a(k):
        for i in range(NX):
            piece = part(zs[k], i, None, a_cols)
            send_to(piece, piece, sza.at[0, 0, i], rza.at[zs[k], i], tp_of(xp, z)).wait_recv()

    def turn(c):
        at = pl.ds(c * TURN, TURN)
        wt[:, at] = w[at, :].T

    def slab(first, count, zr):
        return kv.at[pl.ds(first, count), pl.ds(pl.multiple_of(zr * rows, rows), rows), :]

    def near_copy(k, zr):
        return send_along(
            slab(5, 4, zr), slab(1, 4, zr), s_near.at[k], r_near.at[k],
            jnp.minimum(s + 1, blocks - 1),
        )

    def far_copy(k, zr):
        return send_along(
            slab(8, 1, zr), slab(0, 1, zr), s_far.at[k], r_far.at[k],
            jnp.minimum(s + 2, blocks - 1),
        )

    def project(k):
        zr = zs[k]
        out = jnp.dot(g[zr], w[...], preferred_element_type=jnp.float32).astype(jnp.bfloat16)
        at = pl.ds(pl.multiple_of(zr * rows, rows), rows)
        for i in range(NX):
            kv[5 + i, at, :] = out[i * rows : (i + 1) * rows, q_cols:]
            qb[i, at, :] = out[i * rows : (i + 1) * rows, :q_cols]
        pl.when(s + 2 < blocks)(lambda: far_copy(k, zr).start())
        pl.when(s + 1 < blocks)(lambda: near_copy(k, zr).start())

    is_edge = (z == 0) | (z == NZ - 1)

    def start_gather(neighbours):
        x_own(NZ, z, a_cols, True)
        x_own(NZ, z, a_cols, False)
        for way, to in neighbours:
            z_send_b(0, z, way, to)
        x_own(0, z, b_cols, True)
        x_forward(NZ, z, a_cols)
        x_own(0, z, b_cols, False)
        way, to = neighbours[0]
        x_rest_near(NZ, z, a_cols)
        for i in (x, xm, xp):
            z_send_a(0, z, i, way, to)
        for load in loads[2:]:
            load.wait()
        clear_edges()
        turn(0)
        x_rest_opposite(NZ, z, a_cols)
        z_send_a(0, z, xo, way, to)
        x_forward(0, z, b_cols)
        meet_second()

    def clear_edges():
        @pl.when(s == 0)
        def _():
            kv[0:5] = jnp.zeros_like(kv[0:5])

        @pl.when(s == 1)
        def _():
            kv[0] = jnp.zeros_like(kv[0])

        @pl.when(s == blocks - 1)
        def _():
            back_near[...] = jnp.zeros_like(back_near)

        @pl.when((s >= blocks - 2) | (s % 2 == 1))
        def _():
            back_far[...] = jnp.zeros_like(back_far)

    @pl.when(is_edge)
    def _():
        start_gather([(0, jnp.where(z == 0, 1, NZ - 2))])
        z_wait_b(1)
        x_own(1, zs[1], b_cols, True)
        x_own(1, zs[1], b_cols, False)
        for c in range(1, 5):
            turn(c)
        x_rest(0, z, b_cols)
        project(0)
        x_forward(1, zs[1], b_cols)
        turn(5)
        z_wait_b(2)
        x_own(2, zs[2], b_cols, True)
        x_own(2, zs[2], b_cols, False)
        z_wait_a(1)
        x_rest(1, zs[1], b_cols)
        project(1)
        x_forward(2, zs[2], b_cols)
        z_wait_b(3)
        x_own(3, zs[3], b_cols, True)
        x_own(3, zs[3], b_cols, False)
        for c in range(6, TURNS):
            turn(c)
        z_wait_a(2)
        x_rest(2, zs[2], b_cols)
        project(2)
        x_forward(3, zs[3], b_cols)
        z_wait_a(3)
        x_rest(3, zs[3], b_cols)
        project(3)
        sends.finish()

    sends = Sends()

    @pl.when(jnp.logical_not(is_edge))
    def _():
        outer = jnp.where(z == 1, 0, NZ - 1)
        inner = NZ - 1 - z
        start_gather([(0, outer), (1, inner)])
        z_wait_b(1)
        z_send_b(1, zs[1], 1, inner)
        for i in (x, xm, xp, xo):
            z_send_a(0, z, i, 1, inner)
        x_own(1, zs[1], b_cols, True)
        x_own(1, zs[1], b_cols, False)
        z_wait_b(2)
        z_send_b(2, zs[2], 0, outer)
        x_own(2, zs[2], b_cols, True)
        x_own(2, zs[2], b_cols, False)
        for c in range(1, 4):
            turn(c)
        x_rest(0, z, b_cols)
        project(0)
        z_wait_a(1)
        for i in range(NX):
            z_send_a(1, zs[1], i, 1, inner)
        z_wait_b(3)
        z_send_b(3, zs[3], 0, outer)
        x_forward(1, zs[1], b_cols)
        x_own(3, zs[3], b_cols, True)
        x_own(3, zs[3], b_cols, False)
        for c in range(4, 7):
            turn(c)
        x_forward(2, zs[2], b_cols)
        z_wait_a(2)
        for i in range(NX):
            z_send_a(2, zs[2], i, 0, outer)
        for c in range(7, TURNS):
            turn(c)
        x_rest(1, zs[1], b_cols)
        project(1)
        z_wait_a(3)
        for i in range(NX):
            z_send_a(3, zs[3], i, 0, outer)
        x_forward(3, zs[3], b_cols)
        x_rest(2, zs[2], b_cols)
        project(2)
        x_rest(3, zs[3], b_cols)
        project(3)
        sends.finish()

    hd = HEAD_SIZE
    last = (((1,), (1,)), ((), ()))

    def two_heads(ref, qt):
        return jnp.concatenate([ref[qt, :, 0:hd], ref[qt, :, hd : 2 * hd]], axis=0)

    row_at = lax.broadcasted_iota(jnp.int32, (hd, 2 * hd), 0)
    col_at = lax.broadcasted_iota(jnp.int32, (hd, 2 * hd), 1) % hd

    def scores(qt, c, q2, do2):
        j = qt + c
        raw = lax.dot_general(kv[j, :, 0:hd], q2, last, preferred_element_type=jnp.float32)
        bent = jnp.tanh(raw * (SCALE / CAP))
        expo = jnp.exp(CAP * bent)
        if c == 0:
            expo = jnp.where(row_at > col_at, expo, 0.0)
        if c == 5:
            expo = jnp.where(row_at <= col_at, expo, 0.0)
        if j < 5:
            expo = expo * jnp.where(s >= (1 if j > 0 else 2), 1.0, 0.0)
        d_probs = lax.dot_general(
            kv[j, :, hd : 2 * hd], do2, last, preferred_element_type=jnp.float32
        )
        e_buf[qt, c] = expo
        dp_buf[qt, c] = d_probs
        b_buf[qt, c] = bent
        shape = (hd // 8, 8, 2 * hd)
        return (
            jnp.sum(expo.reshape(shape), axis=0),
            jnp.sum((expo * d_probs).reshape(shape), axis=0),
        )

    def transpose_keys(j):
        kt[:, pl.ds(j * hd, hd)] = kv[j, :, 0:hd].astype(jnp.float32).T.astype(jnp.bfloat16)

    sums = []
    for qt in range(NX):
        q2, do2 = two_heads(qb, qt), two_heads(dout, qt)
        parts = [scores(qt, c, q2, do2) for c in range(5 - qt, 6)]
        sums.append((sum(p[0] for p in parts), sum(p[1] for p in parts)))
    for j in range(5, 9):
        transpose_keys(j)

    @pl.when(s > 0)
    def _():
        for k in range(NZ):
            near_copy(k, zs[k]).wait_recv()

    @pl.when(s > 1)
    def _():
        for k in range(NZ):
            far_copy(k, zs[k]).wait_recv()

    for j in range(5):
        transpose_keys(j)

    rest = []
    for qt in range(NX):
        q2, do2 = two_heads(qb, qt), two_heads(dout, qt)
        parts = [scores(qt, c, q2, do2) for c in range(0, 5 - qt)]
        norm = jnp.sum(sums[qt][0] + sum(p[0] for p in parts), axis=0, keepdims=True)
        inner = jnp.sum(sums[qt][1] + sum(p[1] for p in parts), axis=0, keepdims=True)
        inverse = 1.0 / norm
        rest.append((inverse, inner * inverse))

    def tile_grads(j):
        d_key = d_value = 0.0
        for qt in range(max(0, j - 5), min(NX, j + 1)):
            c = j - qt
            inverse, delta = rest[qt]
            probs = e_buf[qt, c] * inverse
            bent = b_buf[qt, c]
            d_raw = (
                probs * (dp_buf[qt, c] - delta) * (1.0 - bent * bent) * SCALE
            ).astype(jnp.bfloat16)
            dr_buf[qt, pl.ds(c * hd, hd), :] = d_raw
            d_key += jnp.dot(d_raw, two_heads(qb, qt), preferred_element_type=jnp.float32)
            d_value += jnp.dot(
                probs.astype(jnp.bfloat16), two_heads(dout, qt), preferred_element_type=jnp.float32
            )
        return d_key, d_value

    far_back = send_along(
        back_out.at[0], back_far, s_bf.at[0], r_bf.at[0], jnp.maximum(s - 2, 0)
    )
    near_back = [
        send_along(
            back_out.at[j], back_near.at[j - 1], s_bn.at[j - 1], r_bn.at[j - 1],
            jnp.maximum(s - 1, 0),
        )
        for j in range(1, 5)
    ]
    chip_back = send_along(
        back_out.at[0], back_chip, s_bc.at[0], r_bc.at[0], jnp.maximum(s - 1, 0)
    )
    is_odd = s % 2 == 1
    for j in range(5):
        d_key, d_value = tile_grads(j)
        back_out[j, :, 0:hd] = d_key.astype(jnp.bfloat16)
        back_out[j, :, hd : 2 * hd] = d_value.astype(jnp.bfloat16)
        if j == 0:
            pl.when(is_odd)(lambda: chip_back.start())
            pl.when((s > 1) & jnp.logical_not(is_odd))(lambda: far_back.start())
        elif j < 4:
            pl.when(s > 0)(lambda j=j: near_back[j - 1].start())
        else:

            @pl.when(jnp.logical_not(is_odd))
            def _():
                chip_back.wait_recv()
                other = back_chip[...].astype(jnp.float32)
                back_out[j, :, 0:hd] = (d_key + other[:, 0:hd]).astype(jnp.bfloat16)
                back_out[j, :, hd : 2 * hd] = (d_value + other[:, hd : 2 * hd]).astype(
                    jnp.bfloat16
                )

            pl.when(s > 0)(lambda: near_back[3].start())
    for j in range(5, 9):
        d_key, d_value = tile_grads(j)
        acc[j - 5, :, 0:hd] = d_key
        acc[j - 5, :, hd : 2 * hd] = d_value
    for qt in range(NX):
        d_query = jnp.dot(
            kt[:, pl.ds(qt * hd, 6 * hd)], dr_buf[qt], preferred_element_type=jnp.float32
        )
        grads[qt, :, 0:hd] = d_query[:, 0:hd].T.astype(jnp.bfloat16)
        grads[qt, :, hd : 2 * hd] = d_query[:, hd : 2 * hd].T.astype(jnp.bfloat16)

    @pl.when((s < blocks - 2) & jnp.logical_not(is_odd))
    def _():
        far_back.wait_recv()

    @pl.when(s < blocks - 1)
    def _():
        for i in range(NX):
            send_along(
                back_out.at[i + 1], back_near.at[i], s_bn.at[i], r_bn.at[i], s
            ).wait_recv()

    for i in range(NX):
        own = acc[i] + back_near[i].astype(jnp.float32)
        if i == NX - 1:
            own = own + back_far[...].astype(jnp.float32)
        grads[i, :, q_cols:] = own.astype(jnp.bfloat16)

    zs = zs[::-1]
    p = g
    tile = 768
    a_width = B_TILES * 128
    a_cols = pl.ds(0, a_width)
    b_cols = pl.ds(a_width, width - a_width)
    b_half = (width - a_width) // 2
    a_half = a_width // 2
    a_parts = [pl.ds(0, a_half), pl.ds(a_half, a_half)]
    b_parts = [pl.ds(a_width, b_half), pl.ds(a_width + b_half, b_half)]

    def row_ds(xr, h=None):
        if h is None:
            return pl.ds(pl.multiple_of(xr * rows, rows), rows)
        return pl.ds(pl.multiple_of(xr * rows + h * half, half), half)

    def compute(zr):
        lhs = grads[:, pl.ds(pl.multiple_of(zr * rows, rows), rows), :].reshape(NX * rows, -1)

        for j in range(width // tile):
            at = pl.ds(j * tile, tile)
            p[zr, :, at] = jnp.dot(
                lhs, wt[:, at], preferred_element_type=jnp.float32
            ).astype(jnp.bfloat16)

    def way(zr):
        return jnp.where(zr > z, 1, 0)

    def nearer(zr):
        return tp_of(x, jnp.where(zr > z, z + 1, z - 1))

    def step1(k, zr, cols):
        for direction, to in ((0, xm), (1, xp)):
            sends.start(
                send_to(
                    p.at[zr, row_ds(xo, direction), cols],
                    got_opp.at[direction, zr, :, cols],
                    s1.at[direction, k],
                    r1.at[direction, k],
                    tp_of(to, z),
                )
            )

    def step2(k, zr, parts):
        for direction, to in ((0, xm), (1, xp)):
            for cols in parts if len(parts) == 1 else [b_cols]:
                land = got_opp.at[direction, zr, :, cols]
                send_to(
                    land, land, s1.at[direction, k], r1.at[direction, k], tp_of(to, z)
                ).wait_recv()
            at = row_ds(to, direction)
            for h, cols in enumerate(parts):
                p[zr, at, cols] = (
                    p[zr, at, cols].astype(jnp.float32)
                    + got_opp[direction, zr, :, cols].astype(jnp.float32)
                ).astype(jnp.bfloat16)
                sends.start(
                    send_to(
                        p.at[zr, row_ds(to), cols],
                        got_x.at[direction, zr, :, cols],
                        s2.at[direction, k, h],
                        r2.at[direction, k, h],
                        tp_of(to, z),
                    )
                )

    def x_sum(k, h, zr, cols):
        for direction, to in ((0, xm), (1, xp)):
            land = got_x.at[direction, zr, :, cols]
            send_to(
                land, land, s2.at[direction, k, h], r2.at[direction, k, h], tp_of(to, z)
            ).wait_recv()
        return (
            p[zr, row_ds(x), cols].astype(jnp.float32)
            + got_x[0, zr, :, cols].astype(jnp.float32)
            + got_x[1, zr, :, cols].astype(jnp.float32)
        )

    def line_b(d, zr, h):
        return got_zb.at[d, zr, h]

    def line_wait_b(d, zr, h):
        land = line_b(d, zr, h)
        send_to(land, land, tzb.at[0, h], uzb.at[d, zr, h], tp_of(xp, z)).wait_recv()

    def line_wait_a(d, zr, h):
        land = got_za.at[d, zr, :, a_parts[h]]
        send_to(land, land, tza.at[0, h], uza.at[d, zr, h], tp_of(xp, z)).wait_recv()

    def step3(k, far, halves=(0, 1)):
        zr = zs[k]
        for h in halves:
            cols = b_parts[h]
            value = x_sum(k, h, zr, cols)
            if far:
                line_wait_b(way(zr), zr, h)
                value = value + got_zb[way(zr), zr, h].astype(jnp.float32)
            p[zr, row_ds(x), cols] = value.astype(jnp.bfloat16)
            sends.start(
                send_to(
                    p.at[zr, row_ds(x), cols], line_b(way(zr), zr, h), tzb.at[k, h],
                    uzb.at[way(zr), zr, h], nearer(zr),
                )
            )

    def add_a(d, zr, h):
        line_wait_a(d, zr, h)
        cols = a_parts[h]
        p[zr, :, cols] = (
            p[zr, :, cols].astype(jnp.float32) + got_za[d, zr, :, cols].astype(jnp.float32)
        ).astype(jnp.bfloat16)

    def line_a(k, far, when=None):
        zr = zs[k]
        for h, cols in enumerate(a_parts):
            if far:
                add_a(way(zr), zr, h)
            sends.start(
                send_to(
                    p.at[zr, :, cols], got_za.at[way(zr), zr, :, cols], tza.at[k, h],
                    uza.at[way(zr), zr, h], nearer(zr),
                ),
                when,
            )

    def finish(sources):
        for h, cols in enumerate(b_parts):
            value = x_sum(3, h, z, cols)
            for d in sources:
                line_wait_b(d, z, h)
                value = value + got_zb[d, z, h].astype(jnp.float32)
            total[:, cols] = value
        total[:, a_cols] = x_sum(4, 0, z, a_cols)
        values = tok[...].astype(jnp.float32)
        inv_rms = lax.rsqrt(jnp.mean(values * values, axis=1, keepdims=True) + EPS)
        upper = total[...] * gain_row()
        xhat = values * inv_rms
        out_ref[...] = (
            inv_rms * (upper - xhat * jnp.mean(upper * xhat, axis=1, keepdims=True))
        ).astype(jnp.bfloat16)
        sends.finish()

    sends = Sends()
    compute(zs[0])
    step1(0, zs[0], b_cols)
    line_a(0, False, is_edge)
    compute(zs[1])
    step1(1, zs[1], b_cols)
    line_a(1, False, is_edge)
    compute(zs[2])
    step1(2, zs[2], b_cols)
    line_a(2, False, is_edge)
    compute(z)
    opening, sends = sends, Sends()

    @pl.when(is_edge)
    def _():
        source = jnp.where(z == 0, 0, 1)
        step2(0, zs[0], b_parts)
        step2(1, zs[1], b_parts)
        step2(2, zs[2], b_parts)
        step1(3, z, b_cols)
        step3(0, False)
        step3(1, False)
        add_a(source, z, 0)
        add_a(source, z, 1)
        step1(4, z, a_cols)
        step3(2, False)
        step2(3, z, b_parts)
        step2(4, z, [a_cols])
        finish([source])

    sends = Sends()

    @pl.when(jnp.logical_not(is_edge))
    def _():
        step2(0, zs[0], b_parts)
        step2(1, zs[1], b_parts)
        step2(2, zs[2], b_parts)
        step1(3, z, b_cols)
        line_a(0, True)
        line_a(1, True)
        line_a(2, True)
        for d in (0, 1):
            for h in (0, 1):
                add_a(d, z, h)
        step1(4, z, a_cols)
        step3(0, True)
        step2(3, z, b_parts)
        for h in (0, 1):
            step3(2, True, (h,))
            step3(1, True, (h,))
        step2(4, z, [a_cols])
        finish([0, 1])

    opening.finish()

    @pl.when(s > 0)
    def _():
        for copy in near_back:
            copy.wait_send()

    @pl.when((s > 1) & jnp.logical_not(is_odd))
    def _():
        far_back.wait_send()

    @pl.when(is_odd)
    def _():
        chip_back.wait_send()

    @pl.when(s + 1 < blocks)
    def _():
        for k in range(NZ):
            near_copy(k, zs[NZ - 1 - k]).wait_send()

    @pl.when(s + 2 < blocks)
    def _():
        for k in range(NZ):
            far_copy(k, zs[NZ - 1 - k]).wait_send()


def on_device(tokens, norm_gain, query_weight, key_matrix, value_matrix, output_grad):
    rows, width = tokens.shape
    q_cols, k_cols = query_weight.shape[1], key_matrix.shape[1]
    cols = q_cols + 2 * k_cols
    a_width = B_TILES * 128
    hd = HEAD_SIZE
    any_space = pl.BlockSpec(memory_space=pltpu.HBM)
    dma = pltpu.SemaphoreType.DMA
    low, full = jnp.bfloat16, jnp.float32

    def vmem(kind, *shape):
        return pltpu.VMEM(shape, kind)

    return pl.pallas_call(
        whole,
        out_shape=jax.ShapeDtypeStruct((rows, width), low),
        in_specs=[any_space] * 6,
        out_specs=pl.BlockSpec(memory_space=pltpu.VMEM),
        scratch_shapes=[
            vmem(low, rows, width),
            vmem(full, width // 128, 128),
            vmem(low, width, cols),
            vmem(low, cols, width),
            vmem(low, NZ, NX * rows, width),
            vmem(low, NX, hd, q_cols),
            vmem(low, NX, hd, q_cols),
            vmem(low, 9, hd, 2 * k_cols),
            vmem(low, hd, 9 * hd),
            vmem(full, NX, 6, hd, 2 * hd),
            vmem(full, NX, 6, hd, 2 * hd),
            vmem(full, NX, 6, hd, 2 * hd),
            vmem(low, NX, 6 * hd, 2 * hd),
            vmem(full, NX, hd, 2 * k_cols),
            vmem(low, 5, hd, 2 * k_cols),
            vmem(low, NX, hd, 2 * k_cols),
            vmem(low, hd, 2 * k_cols),
            vmem(low, hd, 2 * k_cols),
            vmem(low, NX, hd, cols),
            vmem(full, rows, width),
            vmem(low, 2, NZ, rows // 2, width),
            vmem(low, 2, NZ, rows, width),
            vmem(low, 2, NZ, NX * rows, a_width),
            vmem(low, 2, NZ, 2, rows, (width - a_width) // 2),
            dma((6,)),
            dma((2, NZ + 1, 3)),
            dma((2, NZ, NX, 2)),
            dma((2, NZ)),
            dma((NZ,)),
            dma((2, NZ, NX)),
            dma((NZ, NX)),
            dma((NZ,)),
            dma((NZ,)),
            dma((NZ,)),
            dma((NZ,)),
            dma((NX,)),
            dma((NX,)),
            dma((1,)),
            dma((1,)),
            dma((1,)),
            dma((1,)),
            dma((2, NZ + 1)),
            dma((2, NZ + 1)),
            dma((2, NZ + 1, 2)),
            dma((2, NZ + 1, 2)),
            dma((NZ, 2)),
            dma((2, NZ, 2)),
            dma((NZ, 2)),
            dma((2, NZ, 2)),
        ],
        compiler_params=pltpu.CompilerParams(
            collective_id=0, has_side_effects=True, vmem_limit_bytes=62 * 1024 * 1024
        ),
    )(
        tokens,
        norm_gain.reshape(-1, 128),
        output_grad.reshape(NX, hd, q_cols),
        query_weight,
        key_matrix,
        value_matrix,
    )


def solution(mesh):
    tp, both = "tp", ("seq", "tp")
    in_specs = (P(both, None), P(), P(None, tp), P(None, tp), P(None, tp), P("seq", tp))
    return jax.shard_map(
        on_device, mesh=mesh, in_specs=in_specs, out_specs=P(both, None), check_vma=False
    )
```
